512 devices in a mesh: row: 16 (over y, core), col: 32 (over z, x).
Axes of the slice: x: 4, y: 8, z: 8, core: 2. Of those that a mesh axis runs over, the one named last changes fastest.
Arguments:
- singles: bfloat16 [1536, 384], P(('row', 'col')), may hold values from -6 to 6
- pair: float32 [1536, 1536, 128], P('row', 'col'), may hold values from -48 to 48
- frames: float32 [1536, 12], P(('row', 'col')), may hold values from -9 to 9, as said below
- w_query: bfloat16 [384, 336], replicated, may hold values from -0.3125 to 0.3125
- w_keyval: bfloat16 [384, 816], replicated, may hold values from -0.3125 to 0.3125
- w_bias: float32 [128, 12], replicated, may hold values from -1 to 1
- head_weights: float32 [12], replicated, may hold values from -2 to 1
- w_out: bfloat16 [2112, 384], replicated, may hold values from -0.125 to 0.125
Outputs:
- update: float32 [1536, 384], P(('row', 'col'))
The draws below stay inside these ranges and needn't reach their ends.
Inputs may be any that keep to these rules, and one draw needn't show every extreme that they name: `frames`: the first nine entries of a row are a rotation matrix in row-major order, the last three a translation.
All inputs are finite; a program needn't handle non-finite values.
Results may differ from the reference program's by a relative error of at most 0.0029.
Values sent between devices are 32-bit elements; how exact they have to be, the bound alone decides.
A program may use at most 64 MiB of HBM per device.

```python
import math
import jax
import jax.numpy as jnp
from jax import lax

CS = 384
CZ = 128
H = 12
CH = 16
PQ = 4
PV = 8
RESIDUES = 1536


def sign_vector(key):
    coin_flips = jax.random.bernoulli(jax.random.fold_in(key, 101), 0.5, (CZ,))
    return jnp.where(coin_flips, 1.0, -1.0).astype(jnp.float32)


def draw_pair(key, part):
    base_key = jax.random.fold_in(key, 202)
    shape_all = (RESIDUES, RESIDUES, CZ)
    values = jnp.clip(jax.random.normal(base_key, shape_all, jnp.float32), -6.0, 6.0)
    return values.astype(jnp.float32)


def draw_w_bias(key, part):
    signs_cz = sign_vector(key)
    normal_part = jax.random.normal(jax.random.fold_in(key, 404), (CZ, H), jnp.float32)
    magnitude = jnp.minimum(jnp.abs(normal_part), 4.0)
    return (signs_cz[:, None] * magnitude / jnp.sqrt(jnp.float32(CZ))).astype(jnp.float32)


def draw_frames(key, part):
    quaternion = jax.random.normal(jax.random.fold_in(key, 505), (RESIDUES, 4), jnp.float32)
    comp_w = jnp.abs(quaternion[:, 0]) + 1.0
    comp_x = quaternion[:, 1]
    comp_y = quaternion[:, 2]
    comp_z = quaternion[:, 3]
    norm_sq = comp_w * comp_w + comp_x * comp_x + comp_y * comp_y + comp_z * comp_z
    scale_inv = 1.0 / jnp.sqrt(norm_sq)
    comp_w = comp_w * scale_inv
    comp_x = comp_x * scale_inv
    comp_y = comp_y * scale_inv
    comp_z = comp_z * scale_inv
    rotation = jnp.stack([1.0 - 2.0 * (comp_y * comp_y + comp_z * comp_z), 2.0 * (comp_x * comp_y - comp_w * comp_z), 2.0 * (comp_x * comp_z + comp_w * comp_y), 2.0 * (comp_x * comp_y + comp_w * comp_z), 1.0 - 2.0 * (comp_x * comp_x + comp_z * comp_z), 2.0 * (comp_y * comp_z - comp_w * comp_x), 2.0 * (comp_x * comp_z - comp_w * comp_y), 2.0 * (comp_y * comp_z + comp_w * comp_x), 1.0 - 2.0 * (comp_x * comp_x + comp_y * comp_y)], axis=1)
    trans_key = jax.random.fold_in(key, 606)
    shift = jnp.clip(1.5 * jax.random.normal(trans_key, (RESIDUES, 3), jnp.float32), -9.0, 9.0)
    return jnp.concatenate([rotation, shift], 1).astype(jnp.float32)


def shard_levels(own_key, extent, cuts, smallest, top_value):
    gain = 1.0
    for dim, parts in cuts:
        steps = jax.random.uniform(jax.random.fold_in(jax.random.fold_in(own_key, 6), dim), (parts,), jnp.float32, smallest / len(cuts), top_value / len(cuts))
        gain = gain * jnp.repeat(jnp.exp(steps), extent[dim] // parts).reshape((-1,) + (1,) * (len(extent) - 1 - dim))
    return gain


def normal_values(key, extent, deviation, reach, pieces=(), dtype=jnp.bfloat16):
    gain = shard_levels(key, extent, pieces, -0.22, 0.18) if pieces else 1.0
    result = jax.random.normal(key, extent, jnp.float32) * deviation * gain
    return jnp.minimum(jnp.maximum(result, -reach), reach).astype(dtype)


def setup_inputs(seed: int = 0) -> dict:
    streams_of = jax.random.split(jax.random.key(seed), 9)
    singles = normal_values(streams_of[0], (RESIDUES, CS), 1.0, 6.0, ((0, 512),))
    pair = draw_pair(jax.random.fold_in(streams_of[8], 71), 0)
    frames = draw_frames(jax.random.fold_in(streams_of[8], 71), 0)
    w_query = normal_values(streams_of[3], (CS, H * CH + 3 * H * PQ), CS ** -0.5, 0.3125)
    w_keyval = normal_values(streams_of[4], (CS, 2 * H * CH + 3 * H * (PQ + PV)), CS ** -0.5, 0.3125)
    w_bias = draw_w_bias(jax.random.fold_in(streams_of[8], 71), 0)
    head_weights = jnp.clip(jax.random.uniform(streams_of[6], (H,), jnp.float32, -2.0, 1.0), -2.0, 1.0)
    w_out = normal_values(streams_of[7], (H * (CH + 4 * PV + CZ), CS), (H * (CH + 4 * PV + CZ)) ** -0.5, 0.125)
    return dict(singles=singles, pair=pair, frames=frames, w_query=w_query, w_keyval=w_keyval, w_bias=w_bias, head_weights=head_weights, w_out=w_out)


HIGHEST = lax.Precision.HIGHEST

def rigid_apply(frames, points):
    rotation = frames[:, :9].reshape(frames.shape[0], 3, 3)
    moved = jnp.einsum('nab,nbm->nam', rotation, points, precision=HIGHEST)
    return moved + frames[:, 9:12, None]

def query_side(singles, frames, w_query):
    row_count = singles.shape[0]
    scalar_width = H * CH
    projected = jnp.dot(singles, w_query, preferred_element_type=jnp.float32)
    points = rigid_apply(frames, projected[:, scalar_width:].reshape(row_count, 3, H * PQ))
    return jnp.concatenate([projected[:, :scalar_width], points.reshape(row_count, 3 * H * PQ)], 1)

def key_side(singles, frames, w_keyval):
    row_count = singles.shape[0]
    scalar_width = 2 * H * CH
    point_end = scalar_width + 3 * H * PQ
    projected = jnp.dot(singles, w_keyval, preferred_element_type=jnp.float32)
    key_points = rigid_apply(frames, projected[:, scalar_width:point_end].reshape(row_count, 3, H * PQ))
    value_points = rigid_apply(frames, projected[:, point_end:].reshape(row_count, 3, H * PV))
    return jnp.concatenate([projected[:, :scalar_width], key_points.reshape(row_count, 3 * H * PQ), value_points.reshape(row_count, 3 * H * PV)], 1)

def logits_of(query_feat, key_feat, pair_block, w_bias, head_weights):
    query_rows = query_feat.shape[0]
    key_rows = key_feat.shape[0]
    scalar_width = H * CH
    query_vec = query_feat[:, :scalar_width].reshape(query_rows, H, CH)
    query_points = query_feat[:, scalar_width:].reshape(query_rows, 3, H, PQ)
    key_vec = key_feat[:, :scalar_width].reshape(key_rows, H, CH)
    key_points = key_feat[:, 2 * scalar_width:2 * scalar_width + 3 * H * PQ].reshape(key_rows, 3, H, PQ)
    scalar = jnp.einsum('ihc,jhc->ihj', query_vec, key_vec, precision=HIGHEST) / math.sqrt(CH)
    pair_bias = jnp.einsum('ijc,ch->ihj', pair_block, w_bias, precision=HIGHEST)
    cross_term = jnp.einsum('iahp,jahp->ihj', query_points, key_points, precision=HIGHEST)
    query_square = lax.optimization_barrier(jnp.sum(query_points * query_points, axis=(1, 3)))
    key_square = lax.optimization_barrier(jnp.sum(key_points * key_points, axis=(1, 3)))
    distance = query_square[:, :, None] + key_square.T[None, :, :] - 2.0 * cross_term
    weight = jax.nn.softplus(head_weights) * (math.sqrt(2.0 / (9.0 * PQ)) / 2.0)
    return math.sqrt(1.0 / 3.0) * (scalar + pair_bias - weight[None, :, None] * distance)

def weighted(exponent, key_feat, pair_block):
    key_rows = key_feat.shape[0]
    scalar_width = H * CH
    value_vec = key_feat[:, scalar_width:2 * scalar_width].reshape(key_rows, H, CH)
    value_points = key_feat[:, 2 * scalar_width + 3 * H * PQ:].reshape(key_rows, 3, H, PV)
    weight_sum = lax.optimization_barrier(jnp.sum(exponent, axis=2))
    scalar = jnp.einsum('ihj,jhc->ihc', exponent, value_vec, precision=HIGHEST)
    points = jnp.einsum('ihj,jahp->iahp', exponent, value_points, precision=HIGHEST)
    paired = jnp.einsum('ihj,ijc->ihc', exponent, pair_block, precision=HIGHEST)
    return (weight_sum, scalar, points, paired)

def finish_rest(scalar, points, frames, w_out):
    row_count = scalar.shape[0]
    rotation = frames[:, :9].reshape(row_count, 3, 3)
    relative = points - frames[:, 9:12, None, None]
    local_points = jnp.einsum('nba,nbhp->nahp', rotation, relative, precision=HIGHEST)
    length = jnp.sqrt(lax.optimization_barrier(jnp.sum(local_points * local_points, axis=1)) + 1.0)
    features = jnp.concatenate([scalar.reshape(row_count, H * CH), local_points.reshape(row_count, 3 * H * PV), length.reshape(row_count, H * PV)], 1)
    features = features.astype(jnp.bfloat16)
    return jnp.dot(features, w_out[:H * (CH + 4 * PV)], preferred_element_type=jnp.float32)

def paired_term(paired, w_out):
    row_count = paired.shape[0]
    pair_rows = w_out[H * (CH + 4 * PV):].astype(jnp.float32)
    return jnp.dot(paired.reshape(row_count, H * CZ), pair_rows, precision=HIGHEST)

def finish(weight_sum, scalar, points, paired, frames, w_out):
    scalar = scalar / weight_sum[:, :, None]
    points = points / weight_sum[:, None, :, None]
    paired = paired / weight_sum[:, :, None]
    return finish_rest(scalar, points, frames, w_out) + paired_term(paired, w_out)

def reference(singles, pair, frames, w_query, w_keyval, w_bias, head_weights, w_out):
    query_feat = query_side(singles, frames, w_query)
    key_feat = key_side(singles, frames, w_keyval)
    residues = singles.shape[0]
    block_rows = 128 if residues % 128 == 0 else residues

    def one_block(first_row):
        query_part = lax.dynamic_slice_in_dim(query_feat, first_row, block_rows, 0)
        pair_part = lax.dynamic_slice_in_dim(pair, first_row, block_rows, 0)
        frame_part = lax.dynamic_slice_in_dim(frames, first_row, block_rows, 0)
        logits = logits_of(query_part, key_feat, pair_part, w_bias, head_weights)
        exponent = jnp.exp(logits - lax.optimization_barrier(jnp.max(logits, axis=2, keepdims=True)))
        weight_sum, scalar, points, paired = weighted(exponent, key_feat, pair_part)
        return finish(weight_sum, scalar, points, paired, frame_part, w_out)
    starts = (jnp.arange(residues // block_rows) * block_rows).astype(jnp.int32)
    blocks = lax.map(one_block, starts)
    return blocks.reshape(residues, CS)
```

```python
import functools
import math

import jax
import jax.numpy as jnp
from jax import lax
from jax.experimental import pallas as pl
from jax.experimental.pallas import tpu as pltpu
from jax.sharding import PartitionSpec as P

CS = 384
CZ = 128
H = 12
CH = 16
PQ = 4
PV = 8

HP = 16
LANES = 128
SCALAR = H * CH
VALUE = SCALAR + 3 * H * PV
SPLIT = H * (CH + 4 * PV)
GROUP = 32
FEAT = H * GROUP
SCALE = math.sqrt(1.0 / 3.0)
MESH = pl.DeviceIdType.MESH
NT = (((1,), (1,)), ((), ()))
NN = (((1,), (0,)), ((), ()))
F32 = jnp.float32
BF16 = jnp.bfloat16


def dot(left, right, dims):
    return lax.dot_general(left, right, dims, preferred_element_type=F32)


def pieces(value, count):
    result = []
    for _ in range(count):
        piece = value.astype(BF16).astype(F32)
        result.append(piece)
        value = value - piece
    return result


def iota(shape, dim):
    return lax.broadcasted_iota(jnp.int32, shape, dim)


def moved_points(frame, local, width):
    parts = [local[:, b * width : (b + 1) * width] for b in range(3)]
    return [
        frame[:, 3 * a : 3 * a + 1] * parts[0]
        + frame[:, 3 * a + 1 : 3 * a + 2] * parts[1]
        + frame[:, 3 * a + 2 : 3 * a + 3] * parts[2]
        + frame[:, 9 + a : 10 + a]
        for a in range(3)
    ]


def value_head(lane):
    points = lax.rem(lane - SCALAR, H * PV) // PV
    head = jnp.where(lane < SCALAR, lane // CH, points)
    return jnp.where(lane < VALUE, head, -1)


def kernel(
    sizes,
    singles_ref,
    frames_ref,
    w_bias_ref,
    heads_ref,
    pair_hbm,
    w_query_hbm,
    w_keyval_hbm,
    w_out_hbm,
    out_ref,
    pair_ref,
    pair_hi,
    pair_lo,
    w_query_ref,
    w_keyval_ref,
    w_out_ref,
    q_all,
    k_own,
    v_own,
    k_all,
    v_all,
    bias_ref,
    attn_ref,
    pooled_ref,
    lse_all,
    point_own,
    point_all,
    part_own,
    part_all,
    load_sem,
    q_send,
    q_recv,
    k_send,
    k_recv,
    v_send,
    v_recv,
    l_send,
    l_recv,
    o_send,
    o_recv,
    p_send,
    p_recv,
):
    row_devs, col_devs = sizes
    rows = singles_ref.shape[0]
    queries, keys = pair_ref.shape[0], pair_ref.shape[1]
    owners = keys // rows
    row = lax.axis_index("row")
    col = lax.axis_index("col")

    loads = [
        pltpu.make_async_copy(w_query_hbm, w_query_ref, load_sem.at[0]),
        pltpu.make_async_copy(w_keyval_hbm, w_keyval_ref, load_sem.at[1]),
        pltpu.make_async_copy(pair_hbm, pair_ref, load_sem.at[2]),
        pltpu.make_async_copy(w_out_hbm, w_out_ref, load_sem.at[3]),
    ]
    for load in loads:
        load.start()

    me = row * col_devs + col
    key_col = me // owners
    key_slot = lax.rem(me, owners)
    own_keys = key_col == col

    def source_of(slot):
        index = col * owners + slot
        return (index // col_devs, lax.rem(index, col_devs))

    barrier = pltpu.get_barrier_semaphore()

    def greet(peer):
        pl.semaphore_signal(barrier, inc=1, device_id=peer, device_id_type=MESH)

    def greet_source(step, carry):
        slot = lax.rem(key_slot + step, owners)

        @pl.when(jnp.logical_not(jnp.logical_and(own_keys, slot == key_slot)))
        def _():
            greet(source_of(slot))

        return carry

    def greet_row(step, carry):
        greet((row, lax.rem(col + step, col_devs)))
        return carry

    lax.fori_loop(0, owners, greet_source, 0)
    lax.fori_loop(1, col_devs, greet_row, 0)

    single = singles_ref[...]
    frame = frames_ref[...]
    loads[0].wait()
    query_proj = dot(single, w_query_ref[...], NT)
    loads[1].wait()
    key_proj = dot(single, w_keyval_ref[...], NT)

    lane = iota((1, FEAT), 1)
    lane_head = lane // GROUP
    within = lax.rem(lane, GROUP)
    is_scalar = within < CH
    axis = (within - CH) // PQ
    is_point = jnp.logical_and(within >= CH, within < CH + 3 * PQ)
    point = lax.rem(within - CH, PQ)
    targets = [jnp.where(is_scalar, lane_head * CH + within, -1)]
    for b in range(3):
        column = SCALAR + b * H * PQ + lane_head * PQ + point
        targets.append(jnp.where(is_point, column, -1))
    target = jnp.concatenate(targets, 1)
    width = SCALAR + 3 * H * PQ
    place = jnp.where(iota((width, 4 * FEAT), 0) == target, 1.0, 0.0).astype(BF16)
    key_part = jnp.concatenate(
        [key_proj[:, :SCALAR], key_proj[:, 2 * SCALAR : 2 * SCALAR + 3 * H * PQ]], 1
    )
    both = jnp.concatenate(
        [query_proj, key_part, jnp.zeros((8 - 2 * rows, width), F32)], 0
    )
    placed = dot(jnp.concatenate(pieces(both, 3), 0).astype(BF16), place, NN)
    placed = placed[0:8] + placed[8:16] + placed[16:24]
    frame8 = jnp.concatenate([frame, frame, jnp.zeros((8 - 2 * rows, 12), F32)], 0)

    def by_axis(first, stride):
        return jnp.where(
            axis == 0,
            frame8[:, first : first + 1],
            jnp.where(
                axis == 1,
                frame8[:, first + stride : first + stride + 1],
                frame8[:, first + 2 * stride : first + 2 * stride + 1],
            ),
        )

    moved = by_axis(9, 1)
    for b in range(3):
        moved = moved + by_axis(b, 3) * placed[:, (b + 1) * FEAT : (b + 2) * FEAT]
    moved = jnp.where(is_point, moved, 0.0)
    same_head = iota((FEAT, FEAT), 0) // GROUP == iota((FEAT, FEAT), 1) // GROUP
    same_head = jnp.where(same_head, 1.0, 0.0).astype(BF16)
    squares = jnp.concatenate(pieces(moved * moved, 3), 0).astype(BF16)
    squares = dot(squares, same_head, NN)
    squares = squares[0:8] + squares[8:16] + squares[16:24]

    raw = heads_ref[...]
    gamma = jnp.maximum(raw, 0.0) + jnp.log(1.0 + jnp.exp(-jnp.abs(raw)))
    weight = jnp.zeros((1, FEAT), F32)
    for h in range(H):
        weight = jnp.where(lane_head == h, gamma[:, h : h + 1], weight)
    weight = weight * (SCALE * math.sqrt(2.0 / (9.0 * PQ)) / 2.0)
    scalars = placed[:, :FEAT]
    first_extra = within == CH + 3 * PQ
    second_extra = within == CH + 3 * PQ + 1
    zero = jnp.zeros((8, FEAT), F32)
    q_feat = jnp.where(is_scalar, scalars * (SCALE / math.sqrt(CH)), moved * (2.0 * weight))
    q_feat = jnp.where(first_extra, -weight * squares, q_feat)
    q_feat = jnp.where(second_extra, weight + zero, q_feat)
    k_feat = jnp.where(is_scalar, scalars, moved)
    k_feat = jnp.where(first_extra, 1.0, k_feat)
    k_feat = jnp.where(second_extra, -squares, k_feat)
    v_points = moved_points(frame, key_proj[:, 2 * SCALAR + 3 * H * PQ :], H * PV)
    v_feat = jnp.concatenate(
        [key_proj[:, SCALAR : 2 * SCALAR]]
        + v_points
        + [jnp.zeros((rows, 4 * LANES - VALUE), F32)],
        1,
    )

    own_rows = pl.ds(col * rows, rows)
    key_rows = pl.ds(key_slot * rows, rows)
    for t in range(FEAT // LANES):
        part = slice(t * LANES, (t + 1) * LANES)
        q_all[own_rows, t, :] = q_feat[0:rows, part]
        k_own[:, t, :] = k_feat[rows : 2 * rows, part]
    for t in range(4):
        v_own[:, t, :] = v_feat[:, t * LANES : (t + 1) * LANES]

    @pl.when(own_keys)
    def _():
        for t in range(FEAT // LANES):
            k_all[key_rows, t, :] = k_feat[rows : 2 * rows, t * LANES : (t + 1) * LANES]
        for t in range(4):
            v_all[key_rows, t, :] = v_feat[:, t * LANES : (t + 1) * LANES]

    pl.semaphore_wait(barrier, owners + col_devs - 1 - own_keys.astype(jnp.int32))

    def key_copy(src, dst, peer, slot, send, recv, index):
        return pltpu.make_async_remote_copy(
            src_ref=src,
            dst_ref=dst.at[pl.ds(slot * rows, rows)],
            send_sem=send.at[index],
            recv_sem=recv.at[slot],
            device_id=peer,
            device_id_type=MESH,
        )

    def k_copy(peer, slot, index):
        return key_copy(k_own, k_all, peer, slot, k_send, k_recv, index)

    def v_copy(peer, slot, index):
        return key_copy(v_own, v_all, peer, slot, v_send, v_recv, index)

    def each_key_peer(act):
        def body(step, carry):
            peer_row = lax.rem(row + step, row_devs)

            @pl.when(jnp.logical_not(jnp.logical_and(own_keys, peer_row == row)))
            def _():
                act((peer_row, key_col), step)

            return carry

        lax.fori_loop(0, row_devs, body, 0)

    def each_source(act):
        def body(slot, carry):
            @pl.when(jnp.logical_not(jnp.logical_and(own_keys, slot == key_slot)))
            def _():
                act(source_of(slot), slot)

            return carry

        lax.fori_loop(0, owners, body, 0)

    def each_row_peer(act):
        def body(step, carry):
            act(lax.rem(col + step, col_devs), step)
            return carry

        lax.fori_loop(1, col_devs, body, 0)

    def row_copy(src, dst, peer, source, send, recv, index):
        return pltpu.make_async_remote_copy(
            src_ref=src,
            dst_ref=dst,
            send_sem=send.at[index],
            recv_sem=recv.at[source],
            device_id=(row, peer),
            device_id_type=MESH,
        )

    def q_copy(peer, source, index):
        at = pl.ds(source * rows, rows)
        return row_copy(q_all.at[at], q_all.at[at], peer, source, q_send, q_recv, index)

    def l_copy(peer, source, index):
        return row_copy(
            lse_all.at[source], lse_all.at[source], peer, source, l_send, l_recv, index
        )

    def o_copy(peer, source, index):
        return row_copy(
            point_own.at[pl.ds(peer * rows, rows)],
            point_all.at[source],
            peer,
            source,
            o_send,
            o_recv,
            index,
        )

    def p_copy(peer, source, index):
        return row_copy(
            part_own.at[pl.ds(peer * rows, rows)],
            part_all.at[source],
            peer,
            source,
            p_send,
            p_recv,
            index,
        )

    each_key_peer(lambda peer, step: k_copy(peer, key_slot, step).start())
    each_row_peer(lambda peer, step: q_copy(peer, col, step).start())
    each_key_peer(lambda peer, step: v_copy(peer, key_slot, step).start())

    bias_rows = jnp.concatenate([w_bias_ref[...] * SCALE, jnp.zeros((HP - H, CZ), F32)], 0)
    bias_pieces = jnp.concatenate(pieces(bias_rows, 3), 0).astype(BF16)
    loads[2].wait()

    @pl.loop(0, queries // 4)
    def _(block):
        for u in range(4):
            i = block * 4 + u
            high, middle, low = [piece.astype(BF16) for piece in pieces(pair_ref[i], 3)]
            pair_hi[i] = high
            pair_lo[i] = middle
            first = dot(bias_pieces, high, NT)
            second = dot(bias_pieces[0 : 2 * HP], middle, NT)
            third = dot(bias_pieces[0:HP], low, NT)
            small = first[2 * HP :] + second[HP:] + third
            bias_ref[i] = first[0:HP] + (first[HP : 2 * HP] + second[0:HP] + small)

    each_source(lambda peer, slot: k_copy(peer, slot, slot).wait_recv())
    each_row_peer(lambda peer, step: q_copy(peer, peer, step).wait_recv())

    lse_lane = VALUE % LANES
    lane128 = iota((1, LANES), 1)
    lse = jnp.zeros((queries, LANES), F32)
    for t in range(FEAT // LANES):
        q1, q2, q3 = [piece.astype(BF16) for piece in pieces(q_all[:, t, :], 3)]
        k1, k2, k3 = [piece.astype(BF16) for piece in pieces(k_all[:, t, :], 3)]
        left = jnp.concatenate([q1, q1, q2, q1, q2, q3], 1)
        right = jnp.concatenate([k1, k2, k1, k3, k2, k1], 1)
        tile_head = lax.rem(iota((1, 6 * LANES), 1), LANES) // GROUP
        for g in range(LANES // GROUP):
            h = t * (LANES // GROUP) + g
            mask = jnp.where(tile_head == g, 1.0, 0.0).astype(BF16)
            logits = dot(left, right * mask, NT) + bias_ref[:, h, :]
            top = jnp.max(logits, axis=1, keepdims=True)
            exponent = jnp.exp(logits - top)
            total = jnp.sum(exponent, axis=1, keepdims=True)
            attn_ref[:, h, :] = exponent * (1.0 / total)
            lse = jnp.where(lane128 == lse_lane + h, top + jnp.log(total), lse)

    turned = jnp.concatenate([lse, jnp.zeros((LANES - queries, LANES), F32)], 0).T
    own_lse = turned[lse_lane : lse_lane + HP]
    lse_all[col] = own_lse
    each_row_peer(lambda peer, step: l_copy(peer, col, step).start())

    each_source(lambda peer, slot: v_copy(peer, slot, slot).wait_recv())
    values = jnp.concatenate([v_all[:, t, :] for t in range(4)], 1)
    v1, v2 = [piece.astype(BF16) for piece in pieces(values, 2)]
    lane_of = value_head(iota((1, 4 * LANES), 1))
    gathered = jnp.zeros((queries, 4 * LANES), F32)
    for h in range(H):
        mask = jnp.where(lane_of == h, 1.0, 0.0).astype(BF16)
        a1, a2 = [piece.astype(BF16) for piece in pieces(attn_ref[:, h, :], 2)]
        left = jnp.concatenate([a1, a2], 0)
        high = dot(left, v1 * mask, NN)
        low = dot(a1, v2 * mask, NN)
        gathered = gathered + (high[0:queries] + (high[queries:] + low))
    for t in range(4):
        tile = gathered[:, t * LANES : (t + 1) * LANES]
        if t == 3:
            tile = jnp.where(lane128 >= lse_lane, lse, tile)
        point_own[:, t, :] = tile
    for i in range(rows):
        point_all[col, i] = point_own[col * rows + i]
    each_row_peer(lambda peer, step: o_copy(peer, col, step).start())

    @pl.loop(0, queries // 4)
    def _(block):
        for u in range(4):
            i = block * 4 + u
            stacked = jnp.concatenate(pieces(attn_ref[i], 2), 0).astype(BF16)
            high = dot(stacked, pair_hi[i], NN)
            low = dot(stacked[0:HP], pair_lo[i], NN)
            pooled_ref[i] = high[0:HP] + (high[HP:] + low)

    loads[3].wait()
    each_row_peer(lambda peer, step: l_copy(peer, peer, step).wait_recv())
    everyone = lse_all[...]
    top = jnp.max(everyone, axis=0)
    whole = top + jnp.log(jnp.sum(jnp.exp(everyone - top[None]), axis=0))
    factor = jnp.exp(own_lse - whole)
    factor = jnp.concatenate([factor, jnp.zeros((LANES - HP, LANES), F32)], 0).T
    projected = jnp.zeros((queries, CS), F32)
    for h in range(0, H, 2):
        scaled = jnp.concatenate(
            [pooled_ref[:, g, :] * factor[0:queries, g : g + 1] for g in (h, h + 1)], 1
        )
        stacked = jnp.concatenate(pieces(scaled, 2), 0).astype(BF16)
        share = dot(stacked, w_out_ref[SPLIT + h * CZ : SPLIT + (h + 2) * CZ, :], NN)
        projected = projected + (share[0:queries] + share[queries:])
    for t in range(CS // LANES):
        part_own[:, t, :] = projected[:, t * LANES : (t + 1) * LANES]
    for i in range(rows):
        part_all[col, i] = part_own[col * rows + i]
    each_row_peer(lambda peer, step: p_copy(peer, col, step).start())

    each_row_peer(lambda peer, step: o_copy(peer, peer, step).wait_recv())
    shares = []
    for i in range(rows):
        sums = point_all[:, i, 3, :]
        share = jnp.exp(sums - jnp.max(sums, axis=0, keepdims=True))
        share = share / jnp.sum(share, axis=0, keepdims=True)
        shares.append(share)
    shares = jnp.concatenate(pieces(jnp.concatenate(shares, 0), 2), 0).astype(BF16)
    spread = iota((LANES, 4 * LANES), 0) - lse_lane == value_head(
        iota((LANES, 4 * LANES), 1)
    )
    spread = jnp.logical_and(spread, iota((LANES, 4 * LANES), 0) >= lse_lane)
    wide = dot(shares, jnp.where(spread, 1.0, 0.0).astype(BF16), NN)
    count = rows * col_devs
    wide = wide[0:count] + wide[count:]
    kept = jnp.concatenate(
        [
            jnp.concatenate(
                [
                    jnp.sum(
                        point_all[:, i, t, :]
                        * wide[
                            i * col_devs : (i + 1) * col_devs, t * LANES : (t + 1) * LANES
                        ],
                        axis=0,
                        keepdims=True,
                    )
                    for t in range(4)
                ],
                1,
            )
            for i in range(rows)
        ],
        0,
    )
    wide = H * PV
    relative = [
        kept[:, SCALAR + b * wide : SCALAR + (b + 1) * wide] - frame[:, 9 + b : 10 + b]
        for b in range(3)
    ]
    local = [
        frame[:, a : a + 1] * relative[0]
        + frame[:, 3 + a : 4 + a] * relative[1]
        + frame[:, 6 + a : 7 + a] * relative[2]
        for a in range(3)
    ]
    length = jnp.sqrt(local[0] ** 2 + local[1] ** 2 + local[2] ** 2 + 1.0)
    features = jnp.concatenate([kept[:, :SCALAR]] + local + [length], 1).astype(BF16)
    update = dot(features, w_out_ref[0:SPLIT, :], NN)

    each_row_peer(lambda peer, step: p_copy(peer, peer, step).wait_recv())
    for t in range(CS // LANES):
        part = slice(t * LANES, (t + 1) * LANES)
        terms = [
            jnp.sum(part_all[:, i, t, :], axis=0, keepdims=True) for i in range(rows)
        ]
        out_ref[:, part] = update[:, part] + jnp.concatenate(terms, 0)

    each_key_peer(lambda peer, step: k_copy(peer, key_slot, step).wait_send())
    each_key_peer(lambda peer, step: v_copy(peer, key_slot, step).wait_send())
    each_row_peer(lambda peer, step: q_copy(peer, col, step).wait_send())
    each_row_peer(lambda peer, step: l_copy(peer, col, step).wait_send())
    each_row_peer(lambda peer, step: o_copy(peer, col, step).wait_send())
    each_row_peer(lambda peer, step: p_copy(peer, col, step).wait_send())


def solution(mesh):
    sizes = (mesh.shape["row"], mesh.shape["col"])

    def body(singles, pair, frames, w_query, w_keyval, w_bias, head_weights, w_out):
        rows = singles.shape[0]
        queries, keys = pair.shape[0], pair.shape[1]
        owners = keys // rows
        vmem = pl.BlockSpec(memory_space=pltpu.VMEM)
        hbm = pl.BlockSpec(memory_space=pl.ANY)
        dma = pltpu.SemaphoreType.DMA
        return pl.pallas_call(
            functools.partial(kernel, sizes),
            out_shape=jax.ShapeDtypeStruct((rows, w_out.shape[1]), F32),
            in_specs=[vmem] * 4 + [hbm] * 4,
            out_specs=vmem,
            scratch_shapes=[
                pltpu.VMEM(pair.shape, F32),
                pltpu.VMEM(pair.shape, BF16),
                pltpu.VMEM(pair.shape, BF16),
                pltpu.VMEM(w_query.shape[::-1], w_query.dtype),
                pltpu.VMEM(w_keyval.shape[::-1], w_keyval.dtype),
                pltpu.VMEM(w_out.shape, w_out.dtype),
                pltpu.VMEM((queries, FEAT // LANES, LANES), F32),
                pltpu.VMEM((rows, FEAT // LANES, LANES), F32),
                pltpu.VMEM((rows, 4, LANES), F32),
                pltpu.VMEM((keys, FEAT // LANES, LANES), F32),
                pltpu.VMEM((keys, 4, LANES), F32),
                pltpu.VMEM((queries, HP, keys), F32),
                pltpu.VMEM((queries, HP, keys), F32),
                pltpu.VMEM((queries, HP, CZ), F32),
                pltpu.VMEM((sizes[1], HP, LANES), F32),
                pltpu.VMEM((queries, 4, LANES), F32),
                pltpu.VMEM((sizes[1], rows, 4, LANES), F32),
                pltpu.VMEM((queries, CS // LANES, LANES), F32),
                pltpu.VMEM((sizes[1], rows, CS // LANES, LANES), F32),
                dma((4,)),
                dma((sizes[1],)),
                dma((sizes[1],)),
                dma((sizes[0],)),
                dma((owners,)),
                dma((sizes[0],)),
                dma((owners,)),
                dma((sizes[1],)),
                dma((sizes[1],)),
                dma((sizes[1],)),
                dma((sizes[1],)),
                dma((sizes[1],)),
                dma((sizes[1],)),
            ],
            compiler_params=pltpu.CompilerParams(
                collective_id=0, has_side_effects=True, vmem_limit_bytes=60 * 2**20
            ),
        )(
            singles,
            frames,
            w_bias.T,
            head_weights.reshape(1, H),
            pair,
            w_query.T,
            w_keyval.T,
            w_out,
        )

    return jax.shard_map(
        body,
        mesh=mesh,
        in_specs=(
            P(("row", "col"), None),
            P("row", "col", None),
            P(("row", "col"), None),
            P(),
            P(),
            P(),
            P(),
            P(),
        ),
        out_specs=P(("row", "col"), None),
        check_vma=False,
    )
```

```python
import functools
import math

import jax
import jax.numpy as jnp
from jax import lax
from jax.experimental import pallas as pl
from jax.experimental.pallas import tpu as pltpu
from jax.sharding import PartitionSpec as P

CS = 384
CZ = 128
H = 12
CH = 16
PQ = 4
PV = 8

HP = 16
LANES = 128
SCALAR = H * CH
VALUE = SCALAR + 3 * H * PV
SPLIT = H * (CH + 4 * PV)
GROUP = 32
INNER = 4
FEAT = H * GROUP
SCALE = math.sqrt(1.0 / 3.0)
MESH = pl.DeviceIdType.MESH
NT = (((1,), (1,)), ((), ()))
NN = (((1,), (0,)), ((), ()))
F32 = jnp.float32
BF16 = jnp.bfloat16


def dot(left, right, dims):
    return lax.dot_general(left, right, dims, preferred_element_type=F32)


def pieces(value, count):
    result = []
    for _ in range(count):
        piece = value.astype(BF16).astype(F32)
        result.append(piece)
        value = value - piece
    return result


def iota(shape, dim):
    return lax.broadcasted_iota(jnp.int32, shape, dim)


def moved_points(frame, local, width):
    parts = [local[:, b * width : (b + 1) * width] for b in range(3)]
    return [
        frame[:, 3 * a : 3 * a + 1] * parts[0]
        + frame[:, 3 * a + 1 : 3 * a + 2] * parts[1]
        + frame[:, 3 * a + 2 : 3 * a + 3] * parts[2]
        + frame[:, 9 + a : 10 + a]
        for a in range(3)
    ]


def merged(sums):
    top = jnp.max(sums, axis=0)
    return top + jnp.log(jnp.sum(jnp.exp(sums - top[None]), axis=0))


def value_head(lane):
    points = lax.rem(lane - SCALAR, H * PV) // PV
    head = jnp.where(lane < SCALAR, lane // CH, points)
    return jnp.where(lane < VALUE, head, -1)


def kernel(
    sizes,
    singles_hbm,
    frames_hbm,
    w_bias_hbm,
    heads_hbm,
    pair_hbm,
    w_query_hbm,
    w_keyval_hbm,
    w_out_hbm,
    out_ref,
    singles_ref,
    frames_ref,
    w_bias_ref,
    heads_ref,
    pair_ref,
    pair_hi,
    pair_lo,
    w_query_ref,
    w_keyval_ref,
    w_out_ref,
    q_all,
    k_own,
    v_own,
    k_all,
    v_all,
    bias_ref,
    attn_ref,
    pooled_ref,
    lse_inner,
    lse_outer,
    point_own,
    point_all,
    part_own,
    part_all,
    load_sem,
    send_sem,
    recv_sem,
):
    row_devs, col_devs = sizes
    rows = singles_ref.shape[0]
    queries, keys = pair_ref.shape[0], pair_ref.shape[1]
    owners = keys // rows
    row = lax.axis_index("row")
    col = lax.axis_index("col")

    me = row * col_devs + col
    key_col = me // owners
    key_slot = lax.rem(me, owners)
    own_keys = key_col == col
    core = lax.rem(row, 2)
    partner = (row + 1 - 2 * core, col)
    inner_devs = INNER
    outer_devs = col_devs // INNER
    inner = lax.rem(col, INNER)
    outer = col // INNER

    def source_of(slot):
        index = col * owners + slot
        return (index // col_devs, lax.rem(index, col_devs))

    barrier = pltpu.get_barrier_semaphore()

    def greet(peer):
        pl.semaphore_signal(barrier, inc=1, device_id=peer, device_id_type=MESH)

    def greet_source(step, carry):
        slot = lax.rem(key_slot + step, owners)

        @pl.when(jnp.logical_not(jnp.logical_and(own_keys, slot == key_slot)))
        def _():
            greet(source_of(slot))

        return carry

    def greet_row(step, carry):
        greet((row, lax.rem(col + step, col_devs)))
        return carry

    lax.fori_loop(0, owners, greet_source, 0)
    lax.fori_loop(1, col_devs, greet_row, 0)
    greet(partner)

    moves = [
        (singles_hbm, singles_ref),
        (w_query_hbm, w_query_ref),
        (w_keyval_hbm, w_keyval_ref),
        (frames_hbm, frames_ref),
        (heads_hbm, heads_ref),
        (w_bias_hbm, w_bias_ref),
        (pair_hbm, pair_ref),
        (w_out_hbm, w_out_ref),
    ]
    loads = [
        pltpu.make_async_copy(src, dst, load_sem.at[n]) for n, (src, dst) in enumerate(moves)
    ]
    for load in loads:
        load.start()

    loads[0].wait()
    single = singles_ref[...]
    loads[1].wait()
    query_proj = dot(single, w_query_ref[...], NT)
    loads[2].wait()
    key_proj = dot(single, w_keyval_ref[...], NT)
    loads[3].wait()
    frame = frames_ref[...]

    lane = iota((1, FEAT), 1)
    lane_head = lane // GROUP
    within = lax.rem(lane, GROUP)
    is_scalar = within < CH
    axis = (within - CH) // PQ
    is_point = jnp.logical_and(within >= CH, within < CH + 3 * PQ)
    point = lax.rem(within - CH, PQ)
    targets = [jnp.where(is_scalar, lane_head * CH + within, -1)]
    for b in range(3):
        column = SCALAR + b * H * PQ + lane_head * PQ + point
        targets.append(jnp.where(is_point, column, -1))
    target = jnp.concatenate(targets, 1)
    width = SCALAR + 3 * H * PQ
    place = jnp.where(iota((width, 4 * FEAT), 0) == target, 1.0, 0.0).astype(BF16)
    key_part = jnp.concatenate(
        [key_proj[:, :SCALAR], key_proj[:, 2 * SCALAR : 2 * SCALAR + 3 * H * PQ]], 1
    )
    both = jnp.concatenate(
        [query_proj, key_part, jnp.zeros((8 - 2 * rows, width), F32)], 0
    )
    placed = dot(jnp.concatenate(pieces(both, 3), 0).astype(BF16), place, NN)
    placed = placed[0:8] + placed[8:16] + placed[16:24]
    frame8 = jnp.concatenate([frame, frame, jnp.zeros((8 - 2 * rows, 12), F32)], 0)

    def by_axis(first, stride):
        return jnp.where(
            axis == 0,
            frame8[:, first : first + 1],
            jnp.where(
                axis == 1,
                frame8[:, first + stride : first + stride + 1],
                frame8[:, first + 2 * stride : first + 2 * stride + 1],
            ),
        )

    moved = by_axis(9, 1)
    for b in range(3):
        moved = moved + by_axis(b, 3) * placed[:, (b + 1) * FEAT : (b + 2) * FEAT]
    moved = jnp.where(is_point, moved, 0.0)
    same_head = iota((FEAT, FEAT), 0) // GROUP == iota((FEAT, FEAT), 1) // GROUP
    same_head = jnp.where(same_head, 1.0, 0.0).astype(BF16)
    squares = jnp.concatenate(pieces(moved * moved, 3), 0).astype(BF16)
    squares = dot(squares, same_head, NN)
    squares = squares[0:8] + squares[8:16] + squares[16:24]

    loads[4].wait()
    raw = heads_ref[...]
    gamma = jnp.maximum(raw, 0.0) + jnp.log(1.0 + jnp.exp(-jnp.abs(raw)))
    weight = jnp.zeros((1, FEAT), F32)
    for h in range(H):
        weight = jnp.where(lane_head == h, gamma[:, h : h + 1], weight)
    weight = weight * (SCALE * math.sqrt(2.0 / (9.0 * PQ)) / 2.0)
    scalars = placed[:, :FEAT]
    first_extra = within == CH + 3 * PQ
    second_extra = within == CH + 3 * PQ + 1
    zero = jnp.zeros((8, FEAT), F32)
    q_feat = jnp.where(is_scalar, scalars * (SCALE / math.sqrt(CH)), moved * (2.0 * weight))
    q_feat = jnp.where(first_extra, -weight * squares, q_feat)
    q_feat = jnp.where(second_extra, weight + zero, q_feat)
    k_feat = jnp.where(is_scalar, scalars, moved)
    k_feat = jnp.where(first_extra, 1.0, k_feat)
    k_feat = jnp.where(second_extra, -squares, k_feat)
    v_points = moved_points(frame, key_proj[:, 2 * SCALAR + 3 * H * PQ :], H * PV)
    v_feat = jnp.concatenate(
        [key_proj[:, SCALAR : 2 * SCALAR]]
        + v_points
        + [jnp.zeros((rows, 4 * LANES - VALUE), F32)],
        1,
    )

    own_rows = pl.ds(col * rows, rows)
    key_rows = pl.ds(key_slot * rows, rows)
    for t in range(FEAT // LANES):
        part = slice(t * LANES, (t + 1) * LANES)
        q_all[own_rows, t, :] = q_feat[0:rows, part]
        k_own[:, t, :] = k_feat[rows : 2 * rows, part]
    for t in range(4):
        v_own[:, t, :] = v_feat[:, t * LANES : (t + 1) * LANES]

    @pl.when(own_keys)
    def _():
        for t in range(FEAT // LANES):
            k_all[key_rows, t, :] = k_feat[rows : 2 * rows, t * LANES : (t + 1) * LANES]
        for t in range(4):
            v_all[key_rows, t, :] = v_feat[:, t * LANES : (t + 1) * LANES]

    pl.semaphore_wait(barrier, owners + col_devs - own_keys.astype(jnp.int32))

    def remote(src, dst, peer, kind):
        return pltpu.make_async_remote_copy(
            src_ref=src,
            dst_ref=dst,
            send_sem=send_sem.at[kind],
            recv_sem=recv_sem.at[kind],
            device_id=peer,
            device_id_type=MESH,
        )

    def sent(ref, kind):
        remote(ref, ref, partner, kind).wait_send()

    def received(ref, kind):
        remote(ref, ref, partner, kind).wait_recv()

    def of_others(act, ref, count, kind):
        @pl.when(own_keys)
        def _():
            act(ref.at[pl.ds(0, (count - 1) * rows)], kind)

        @pl.when(jnp.logical_not(own_keys))
        def _():
            act(ref.at[pl.ds(0, count * rows)], kind)

    K, Q, V, RELAY, LSE_INNER, LSE_OUTER, POINT, PART = range(8)

    def each_key_peer(first, step, act):
        def body(n, carry):
            peer_row = lax.rem(row + n * step + first, row_devs)

            @pl.when(jnp.logical_not(jnp.logical_and(own_keys, peer_row == row)))
            def _():
                act((peer_row, key_col))

            return carry

        lax.fori_loop(0, row_devs // step, body, 0)

    def each_row_peer(act):
        def body(step, carry):
            act(lax.rem(col + step, col_devs))
            return carry

        lax.fori_loop(1, col_devs, body, 0)

    key_rows = pl.ds(key_slot * rows, rows)
    peers = col_devs - 1
    each_key_peer(0, 1, lambda peer: remote(k_own, k_all.at[key_rows], peer, K).start())
    each_row_peer(
        lambda peer: remote(q_all.at[own_rows], q_all.at[own_rows], (row, peer), Q).start()
    )

    loads[5].wait()
    bias_rows = jnp.concatenate([w_bias_ref[...] * SCALE, jnp.zeros((HP - H, CZ), F32)], 0)
    bias_pieces = jnp.concatenate(pieces(bias_rows, 3), 0).astype(BF16)
    loads[6].wait()

    def bias_block(block):
        for u in range(8):
            i = block * 8 + u
            high, middle, low = [piece.astype(BF16) for piece in pieces(pair_ref[i], 3)]
            pair_hi[i] = high
            pair_lo[i] = middle
            first = dot(bias_pieces, high, NT)
            second = dot(bias_pieces[0 : 2 * HP], middle, NT)
            third = dot(bias_pieces[0:HP], low, NT)
            small = first[2 * HP :] + second[HP:] + third
            bias_ref[i] = first[0:HP] + (first[HP : 2 * HP] + second[0:HP] + small)

    blocks = queries // 8
    pl.loop(0, blocks // 2)(bias_block)
    each_key_peer(0, 2, lambda peer: remote(v_own, v_all.at[key_rows], peer, V).start())
    pl.loop(blocks // 2, blocks)(bias_block)

    of_others(received, k_all, owners, K)
    received(q_all.at[pl.ds(0, peers * rows)], Q)

    lse_lane = VALUE % LANES
    lane128 = iota((1, LANES), 1)
    lse = jnp.zeros((queries, LANES), F32)
    for t in range(FEAT // LANES):
        q1, q2, q3 = [piece.astype(BF16) for piece in pieces(q_all[:, t, :], 3)]
        k1, k2, k3 = [piece.astype(BF16) for piece in pieces(k_all[:, t, :], 3)]
        left = jnp.concatenate([q1, q1, q2, q1, q2, q3], 1)
        right = jnp.concatenate([k1, k2, k1, k3, k2, k1], 1)
        tile_head = lax.rem(iota((1, 6 * LANES), 1), LANES) // GROUP
        for g in range(LANES // GROUP):
            h = t * (LANES // GROUP) + g
            mask = jnp.where(tile_head == g, 1.0, 0.0).astype(BF16)
            logits = dot(left, right * mask, NT) + bias_ref[:, h, :]
            top = jnp.max(logits, axis=1, keepdims=True)
            exponent = jnp.exp(logits - top)
            total = jnp.sum(exponent, axis=1, keepdims=True)
            attn_ref[:, h, :] = exponent * (1.0 / total)
            lse = jnp.where(lane128 == lse_lane + h, top + jnp.log(total), lse)

    turned = jnp.concatenate([lse, jnp.zeros((LANES - queries, LANES), F32)], 0).T
    own_lse = turned[lse_lane : lse_lane + HP]
    lse_inner[inner] = own_lse
    for step in range(1, inner_devs):
        peer = outer * inner_devs + lax.rem(inner + step, inner_devs)
        slot = lse_inner.at[inner]
        remote(slot, slot, (row, peer), LSE_INNER).start()

    direct = lax.rem(col // 2, 2) == core

    @pl.when(direct)
    def _():
        of_others(received, v_all, owners, V)
        remote(v_all, v_all, partner, RELAY).start()

    @pl.when(jnp.logical_not(direct))
    def _():
        received(v_all, RELAY)

    values = jnp.concatenate([v_all[:, t, :] for t in range(4)], 1)
    v1, v2 = [piece.astype(BF16) for piece in pieces(values, 2)]
    lane_of = value_head(iota((1, 4 * LANES), 1))
    gathered = jnp.zeros((queries, 4 * LANES), F32)
    for h in range(H):
        mask = jnp.where(lane_of == h, 1.0, 0.0).astype(BF16)
        a1, a2 = [piece.astype(BF16) for piece in pieces(attn_ref[:, h, :], 2)]
        left = jnp.concatenate([a1, a2], 0)
        high = dot(left, v1 * mask, NN)
        low = dot(a1, v2 * mask, NN)
        gathered = gathered + (high[0:queries] + (high[queries:] + low))
    for t in range(4):
        tile = gathered[:, t * LANES : (t + 1) * LANES]
        if t == 3:
            tile = jnp.where(lane128 >= lse_lane, lse, tile)
        point_own[:, t, :] = tile
    for i in range(rows):
        point_all[col, i] = point_own[col * rows + i]

    received(lse_inner.at[pl.ds(0, inner_devs - 1)], LSE_INNER)
    lse_outer[outer] = merged(lse_inner[...])
    for step in range(1, outer_devs):
        peer = lax.rem(outer + step, outer_devs) * inner_devs + inner
        slot = lse_outer.at[outer]
        remote(slot, slot, (row, peer), LSE_OUTER).start()

    def send_points(peer):
        theirs = point_own.at[pl.ds(peer * rows, rows)]
        remote(theirs, point_all.at[col], (row, peer), POINT).start()

    each_row_peer(send_points)

    @pl.loop(0, queries // 8)
    def _(block):
        for u in range(8):
            i = block * 8 + u
            stacked = jnp.concatenate(pieces(attn_ref[i], 2), 0).astype(BF16)
            high = dot(stacked, pair_hi[i], NN)
            low = dot(stacked[0:HP], pair_lo[i], NN)
            pooled_ref[i] = high[0:HP] + (high[HP:] + low)

    loads[7].wait()
    received(lse_outer.at[pl.ds(0, outer_devs - 1)], LSE_OUTER)
    factor = jnp.exp(own_lse - merged(lse_outer[...]))
    factor = jnp.concatenate([factor, jnp.zeros((LANES - HP, LANES), F32)], 0).T
    projected = jnp.zeros((queries, CS), F32)
    for h in range(0, H, 2):
        scaled = jnp.concatenate(
            [pooled_ref[:, g, :] * factor[0:queries, g : g + 1] for g in (h, h + 1)], 1
        )
        stacked = jnp.concatenate(pieces(scaled, 2), 0).astype(BF16)
        share = dot(stacked, w_out_ref[SPLIT + h * CZ : SPLIT + (h + 2) * CZ, :], NN)
        projected = projected + (share[0:queries] + share[queries:])
    for t in range(CS // LANES):
        part_own[:, t, :] = projected[:, t * LANES : (t + 1) * LANES]
    for i in range(rows):
        part_all[col, i] = part_own[col * rows + i]

    def send_part(peer):
        theirs = part_own.at[pl.ds(peer * rows, rows)]
        remote(theirs, part_all.at[col], (row, peer), PART).start()

    each_row_peer(send_part)

    received(point_all.at[pl.ds(0, peers)], POINT)
    shares = []
    for i in range(rows):
        sums = point_all[:, i, 3, :]
        share = jnp.exp(sums - jnp.max(sums, axis=0, keepdims=True))
        share = share / jnp.sum(share, axis=0, keepdims=True)
        shares.append(share)
    shares = jnp.concatenate(pieces(jnp.concatenate(shares, 0), 2), 0).astype(BF16)
    spread = iota((LANES, 4 * LANES), 0) - lse_lane == value_head(
        iota((LANES, 4 * LANES), 1)
    )
    spread = jnp.logical_and(spread, iota((LANES, 4 * LANES), 0) >= lse_lane)
    wide = dot(shares, jnp.where(spread, 1.0, 0.0).astype(BF16), NN)
    count = rows * col_devs
    wide = wide[0:count] + wide[count:]
    kept = jnp.concatenate(
        [
            jnp.concatenate(
                [
                    jnp.sum(
                        point_all[:, i, t, :]
                        * wide[
                            i * col_devs : (i + 1) * col_devs, t * LANES : (t + 1) * LANES
                        ],
                        axis=0,
                        keepdims=True,
                    )
                    for t in range(4)
                ],
                1,
            )
            for i in range(rows)
        ],
        0,
    )
    wide = H * PV
    relative = [
        kept[:, SCALAR + b * wide : SCALAR + (b + 1) * wide] - frame[:, 9 + b : 10 + b]
        for b in range(3)
    ]
    local = [
        frame[:, a : a + 1] * relative[0]
        + frame[:, 3 + a : 4 + a] * relative[1]
        + frame[:, 6 + a : 7 + a] * relative[2]
        for a in range(3)
    ]
    length = jnp.sqrt(local[0] ** 2 + local[1] ** 2 + local[2] ** 2 + 1.0)
    features = jnp.concatenate([kept[:, :SCALAR]] + local + [length], 1).astype(BF16)
    update = dot(features, w_out_ref[0:SPLIT, :], NN)

    received(part_all.at[pl.ds(0, peers)], PART)
    for t in range(CS // LANES):
        part = slice(t * LANES, (t + 1) * LANES)
        terms = [
            jnp.sum(part_all[:, i, t, :], axis=0, keepdims=True) for i in range(rows)
        ]
        out_ref[:, part] = update[:, part] + jnp.concatenate(terms, 0)

    of_others(sent, k_all, row_devs, K)
    of_others(sent, v_all, row_devs // 2, V)

    @pl.when(direct)
    def _():
        sent(v_all, RELAY)

    sent(q_all.at[pl.ds(0, peers * rows)], Q)
    sent(lse_inner.at[pl.ds(0, inner_devs - 1)], LSE_INNER)
    sent(lse_outer.at[pl.ds(0, outer_devs - 1)], LSE_OUTER)
    sent(point_own.at[pl.ds(0, peers * rows)], POINT)
    sent(part_own.at[pl.ds(0, peers * rows)], PART)


def solution(mesh):
    sizes = (mesh.shape["row"], mesh.shape["col"])

    def body(singles, pair, frames, w_query, w_keyval, w_bias, head_weights, w_out):
        rows = singles.shape[0]
        queries, keys = pair.shape[0], pair.shape[1]
        owners = keys // rows
        vmem = pl.BlockSpec(memory_space=pltpu.VMEM)
        hbm = pl.BlockSpec(memory_space=pl.ANY)
        dma = pltpu.SemaphoreType.DMA
        return pl.pallas_call(
            functools.partial(kernel, sizes),
            out_shape=jax.ShapeDtypeStruct((rows, w_out.shape[1]), F32),
            in_specs=[hbm] * 8,
            out_specs=vmem,
            scratch_shapes=[
                pltpu.VMEM(singles.shape, singles.dtype),
                pltpu.VMEM(frames.shape, F32),
                pltpu.VMEM(w_bias.shape[::-1], F32),
                pltpu.VMEM((1, H), F32),
                pltpu.VMEM(pair.shape, F32),
                pltpu.VMEM(pair.shape, BF16),
                pltpu.VMEM(pair.shape, BF16),
                pltpu.VMEM(w_query.shape[::-1], w_query.dtype),
                pltpu.VMEM(w_keyval.shape[::-1], w_keyval.dtype),
                pltpu.VMEM(w_out.shape, w_out.dtype),
                pltpu.VMEM((queries, FEAT // LANES, LANES), F32),
                pltpu.VMEM((rows, FEAT // LANES, LANES), F32),
                pltpu.VMEM((rows, 4, LANES), F32),
                pltpu.VMEM((keys, FEAT // LANES, LANES), F32),
                pltpu.VMEM((keys, 4, LANES), F32),
                pltpu.VMEM((queries, HP, keys), F32),
                pltpu.VMEM((queries, HP, keys), F32),
                pltpu.VMEM((queries, HP, CZ), F32),
                pltpu.VMEM((INNER, HP, LANES), F32),
                pltpu.VMEM((sizes[1] // INNER, HP, LANES), F32),
                pltpu.VMEM((queries, 4, LANES), F32),
                pltpu.VMEM((sizes[1], rows, 4, LANES), F32),
                pltpu.VMEM((queries, CS // LANES, LANES), F32),
                pltpu.VMEM((sizes[1], rows, CS // LANES, LANES), F32),
                dma((8,)),
                dma((8,)),
                dma((8,)),
            ],
            compiler_params=pltpu.CompilerParams(
                collective_id=0, has_side_effects=True, vmem_limit_bytes=60 * 2**20
            ),
        )(
            singles,
            frames,
            w_bias.T,
            head_weights.reshape(1, H),
            pair,
            w_query.T,
            w_keyval.T,
            w_out,
        )

    return jax.shard_map(
        body,
        mesh=mesh,
        in_specs=(
            P(("row", "col"), None),
            P("row", "col", None),
            P(("row", "col"), None),
            P(),
            P(),
            P(),
            P(),
            P(),
        ),
        out_specs=P(("row", "col"), None),
        check_vma=False,
    )
```

```python
import functools
import math

import jax
import jax.numpy as jnp
from jax import lax
from jax.experimental import pallas as pl
from jax.experimental.pallas import tpu as pltpu
from jax.sharding import PartitionSpec as P

CS = 384
CZ = 128
H = 12
CH = 16
PQ = 4
PV = 8

HP = 16
LANES = 128
SCALAR = H * CH
VALUE = SCALAR + 3 * H * PV
SPLIT = H * (CH + 4 * PV)
GROUP = 32
INNER = 4
EARLY = 5
FEAT = H * GROUP
SCALE = math.sqrt(1.0 / 3.0)
MESH = pl.DeviceIdType.MESH
NT = (((1,), (1,)), ((), ()))
NN = (((1,), (0,)), ((), ()))
F32 = jnp.float32
BF16 = jnp.bfloat16


def dot(left, right, dims):
    return lax.dot_general(left, right, dims, preferred_element_type=F32)


def pieces(value, count):
    result = []
    for _ in range(count):
        piece = value.astype(BF16).astype(F32)
        result.append(piece)
        value = value - piece
    return result


def iota(shape, dim):
    return lax.broadcasted_iota(jnp.int32, shape, dim)


def moved_points(frame, local, width):
    parts = [local[:, b * width : (b + 1) * width] for b in range(3)]
    return [
        frame[:, 3 * a : 3 * a + 1] * parts[0]
        + frame[:, 3 * a + 1 : 3 * a + 2] * parts[1]
        + frame[:, 3 * a + 2 : 3 * a + 3] * parts[2]
        + frame[:, 9 + a : 10 + a]
        for a in range(3)
    ]


def merged(sums):
    top = jnp.max(sums, axis=0)
    return top + jnp.log(jnp.sum(jnp.exp(sums - top[None]), axis=0))


def value_head(lane):
    points = lax.rem(lane - SCALAR, H * PV) // PV
    head = jnp.where(lane < SCALAR, lane // CH, points)
    return jnp.where(lane < VALUE, head, -1)


def kernel(
    sizes,
    singles_hbm,
    frames_hbm,
    w_bias_hbm,
    heads_hbm,
    pair_hbm,
    w_query_hbm,
    w_keyval_hbm,
    w_out_hbm,
    out_ref,
    singles_ref,
    frames_ref,
    w_bias_ref,
    heads_ref,
    pair_ref,
    pair_hi,
    pair_lo,
    w_query_ref,
    w_keyval_ref,
    w_out_ref,
    q_all,
    k_own,
    v_own,
    k_all,
    v_all,
    bias_ref,
    attn_ref,
    pooled_ref,
    lse_inner,
    lse_outer,
    point_own,
    point_inner,
    point_mid,
    point_outer,
    part_own,
    part_all,
    load_sem,
    send_sem,
    recv_sem,
    ready_sem,
):
    row_devs, col_devs = sizes
    rows = singles_ref.shape[0]
    queries, keys = pair_ref.shape[0], pair_ref.shape[1]
    owners = keys // rows
    row = lax.axis_index("row")
    col = lax.axis_index("col")

    me = row * col_devs + col
    key_col = me // owners
    key_slot = lax.rem(me, owners)
    own_keys = key_col == col
    core = lax.rem(row, 2)
    partner = (row + 1 - 2 * core, col)
    inner_devs = INNER
    outer_devs = col_devs // INNER
    inner = lax.rem(col, INNER)
    outer = col // INNER

    def source_of(slot):
        index = col * owners + slot
        return (index // col_devs, lax.rem(index, col_devs))

    level = outer
    key_level = key_col // inner_devs
    source_level = lax.rem(col * owners, col_devs) // inner_devs
    lower_sources = jnp.clip((level - source_level) * inner_devs, 0, owners)
    barrier = pltpu.get_barrier_semaphore()

    def each(first, last, act):
        def body(n, carry):
            act(n)
            return carry

        lax.fori_loop(first, last, body, 0)

    def greet(peer):
        pl.semaphore_signal(barrier, inc=1, device_id=peer, device_id_type=MESH)

    def tell(peer):
        pl.semaphore_signal(
            ready_sem.at[level], inc=1, device_id=peer, device_id_type=MESH
        )

    def greet_row(peer):
        @pl.when(peer != col)
        def _():
            greet((row, peer))

    def greet_source(slot):
        @pl.when(jnp.logical_not(jnp.logical_and(own_keys, slot == key_slot)))
        def _():
            greet(source_of(slot))

    each(level * inner_devs, col_devs, greet_row)
    each(lower_sources, owners, greet_source)

    @pl.when(key_level > level)
    def _():
        each(0, row_devs, lambda peer_row: greet((peer_row, key_col)))

    greet(partner)

    moves = [
        (singles_hbm, singles_ref),
        (w_query_hbm, w_query_ref),
        (w_keyval_hbm, w_keyval_ref),
        (frames_hbm, frames_ref),
        (heads_hbm, heads_ref),
        (w_bias_hbm, w_bias_ref),
        (pair_hbm, pair_ref),
        (w_out_hbm, w_out_ref),
    ]
    loads = [
        pltpu.make_async_copy(src, dst, load_sem.at[n]) for n, (src, dst) in enumerate(moves)
    ]
    for load in loads:
        load.start()

    near_keys = jnp.where(key_level <= level, row_devs - own_keys.astype(jnp.int32), 0)
    pl.semaphore_wait(barrier, (level + 1) * inner_devs + near_keys + lower_sources)
    each(0, level * inner_devs, lambda peer: tell((row, peer)))
    each(0, lower_sources, lambda slot: tell(source_of(slot)))

    loads[0].wait()
    single = singles_ref[...]
    loads[1].wait()
    query_proj = dot(single, w_query_ref[...], NT)
    loads[2].wait()
    key_proj = dot(single, w_keyval_ref[...], NT)
    loads[3].wait()
    frame = frames_ref[...]

    lane = iota((1, FEAT), 1)
    lane_head = lane // GROUP
    within = lax.rem(lane, GROUP)
    is_scalar = within < CH
    axis = (within - CH) // PQ
    is_point = jnp.logical_and(within >= CH, within < CH + 3 * PQ)
    point = lax.rem(within - CH, PQ)
    targets = [jnp.where(is_scalar, lane_head * CH + within, -1)]
    for b in range(3):
        column = SCALAR + b * H * PQ + lane_head * PQ + point
        targets.append(jnp.where(is_point, column, -1))
    target = jnp.concatenate(targets, 1)
    width = SCALAR + 3 * H * PQ
    place = jnp.where(iota((width, 4 * FEAT), 0) == target, 1.0, 0.0).astype(BF16)
    key_part = jnp.concatenate(
        [key_proj[:, :SCALAR], key_proj[:, 2 * SCALAR : 2 * SCALAR + 3 * H * PQ]], 1
    )
    both = jnp.concatenate(
        [query_proj, key_part, jnp.zeros((8 - 2 * rows, width), F32)], 0
    )
    placed = dot(jnp.concatenate(pieces(both, 3), 0).astype(BF16), place, NN)
    placed = placed[0:8] + placed[8:16] + placed[16:24]
    frame8 = jnp.concatenate([frame, frame, jnp.zeros((8 - 2 * rows, 12), F32)], 0)

    def by_axis(first, stride):
        return jnp.where(
            axis == 0,
            frame8[:, first : first + 1],
            jnp.where(
                axis == 1,
                frame8[:, first + stride : first + stride + 1],
                frame8[:, first + 2 * stride : first + 2 * stride + 1],
            ),
        )

    moved = by_axis(9, 1)
    for b in range(3):
        moved = moved + by_axis(b, 3) * placed[:, (b + 1) * FEAT : (b + 2) * FEAT]
    moved = jnp.where(is_point, moved, 0.0)
    same_head = iota((FEAT, FEAT), 0) // GROUP == iota((FEAT, FEAT), 1) // GROUP
    same_head = jnp.where(same_head, 1.0, 0.0).astype(BF16)
    squares = jnp.concatenate(pieces(moved * moved, 3), 0).astype(BF16)
    squares = dot(squares, same_head, NN)
    squares = squares[0:8] + squares[8:16] + squares[16:24]

    loads[4].wait()
    raw = heads_ref[...]
    gamma = jnp.maximum(raw, 0.0) + jnp.log(1.0 + jnp.exp(-jnp.abs(raw)))
    weight = jnp.zeros((1, FEAT), F32)
    for h in range(H):
        weight = jnp.where(lane_head == h, gamma[:, h : h + 1], weight)
    weight = weight * (SCALE * math.sqrt(2.0 / (9.0 * PQ)) / 2.0)
    scalars = placed[:, :FEAT]
    first_extra = within == CH + 3 * PQ
    second_extra = within == CH + 3 * PQ + 1
    zero = jnp.zeros((8, FEAT), F32)
    q_feat = jnp.where(is_scalar, scalars * (SCALE / math.sqrt(CH)), moved * (2.0 * weight))
    q_feat = jnp.where(first_extra, -weight * squares, q_feat)
    q_feat = jnp.where(second_extra, weight + zero, q_feat)
    k_feat = jnp.where(is_scalar, scalars, moved)
    k_feat = jnp.where(first_extra, 1.0, k_feat)
    k_feat = jnp.where(second_extra, -squares, k_feat)
    v_points = moved_points(frame, key_proj[:, 2 * SCALAR + 3 * H * PQ :], H * PV)
    v_feat = jnp.concatenate(
        [key_proj[:, SCALAR : 2 * SCALAR]]
        + v_points
        + [jnp.zeros((rows, 4 * LANES - VALUE), F32)],
        1,
    )

    own_rows = pl.ds(col * rows, rows)
    key_rows = pl.ds(key_slot * rows, rows)
    for t in range(FEAT // LANES):
        part = slice(t * LANES, (t + 1) * LANES)
        q_all[own_rows, t, :] = q_feat[0:rows, part]
        k_own[:, t, :] = k_feat[rows : 2 * rows, part]
    for t in range(4):
        v_own[:, t, :] = v_feat[:, t * LANES : (t + 1) * LANES]

    @pl.when(own_keys)
    def _():
        for t in range(FEAT // LANES):
            k_all[key_rows, t, :] = k_feat[rows : 2 * rows, t * LANES : (t + 1) * LANES]
        for t in range(4):
            v_all[key_rows, t, :] = v_feat[:, t * LANES : (t + 1) * LANES]

    def remote(src, dst, peer, kind):
        return pltpu.make_async_remote_copy(
            src_ref=src,
            dst_ref=dst,
            send_sem=send_sem.at[kind],
            recv_sem=recv_sem.at[kind],
            device_id=peer,
            device_id_type=MESH,
        )

    def sent(ref, kind):
        remote(ref, ref, partner, kind).wait_send()

    def received(ref, kind):
        remote(ref, ref, partner, kind).wait_recv()

    def of_others(act, ref, count, kind):
        @pl.when(own_keys)
        def _():
            act(ref.at[pl.ds(0, (count - 1) * rows)], kind)

        @pl.when(jnp.logical_not(own_keys))
        def _():
            act(ref.at[pl.ds(0, count * rows)], kind)

    K, Q, V, RELAY, LSE_INNER, LSE_OUTER, POINT_INNER, POINT_OUTER, PART = range(9)

    def each_key_peer(first, step, act):
        def body(n, carry):
            peer_row = lax.rem(row + n * step + first, row_devs)

            @pl.when(jnp.logical_not(jnp.logical_and(own_keys, peer_row == row)))
            def _():
                act((peer_row, key_col))

            return carry

        lax.fori_loop(0, row_devs // step, body, 0)

    def each_row_peer(act):
        def body(step, carry):
            act(lax.rem(col + step, col_devs))
            return carry

        lax.fori_loop(1, col_devs, body, 0)

    key_rows = pl.ds(key_slot * rows, rows)
    peers = col_devs - 1

    def send_keys():
        each_key_peer(
            0, 1, lambda peer: remote(k_own, k_all.at[key_rows], peer, K).start()
        )

    def send_query(peer):
        @pl.when(peer != col)
        def _():
            mine = q_all.at[own_rows]
            remote(mine, mine, (row, peer), Q).start()

    pl.when(key_level <= level)(send_keys)
    each(0, (level + 1) * inner_devs, send_query)

    loads[5].wait()
    bias_rows = jnp.concatenate([w_bias_ref[...] * SCALE, jnp.zeros((HP - H, CZ), F32)], 0)
    bias_pieces = jnp.concatenate(pieces(bias_rows, 3), 0).astype(BF16)
    loads[6].wait()

    def bias_block(block):
        for u in range(8):
            i = block * 8 + u
            high, middle, low = [piece.astype(BF16) for piece in pieces(pair_ref[i], 3)]
            pair_hi[i] = high
            pair_lo[i] = middle
            first = dot(bias_pieces, high, NT)
            second = dot(bias_pieces[0 : 2 * HP], middle, NT)
            third = dot(bias_pieces[0:HP], low, NT)
            small = first[2 * HP :] + second[HP:] + third
            bias_ref[i] = first[0:HP] + (first[HP : 2 * HP] + second[0:HP] + small)

    def next_level(above):
        far_keys = key_level == above
        pl.semaphore_wait(
            ready_sem.at[above], inner_devs + jnp.where(far_keys, row_devs, 0)
        )
        pl.when(far_keys)(send_keys)
        each(above * inner_devs, (above + 1) * inner_devs, send_query)

    blocks = queries // 8
    early = jnp.where(level < EARLY, blocks, 0)
    pl.loop(0, early)(bias_block)
    each(level + 1, outer_devs, next_level)
    pl.loop(early, blocks)(bias_block)
    each_key_peer(0, 2, lambda peer: remote(v_own, v_all.at[key_rows], peer, V).start())

    of_others(received, k_all, owners, K)
    received(q_all.at[pl.ds(0, peers * rows)], Q)

    lse_lane = VALUE % LANES
    lane128 = iota((1, LANES), 1)
    lse = jnp.zeros((queries, LANES), F32)
    for t in range(FEAT // LANES):
        q1, q2, q3 = [piece.astype(BF16) for piece in pieces(q_all[:, t, :], 3)]
        k1, k2, k3 = [piece.astype(BF16) for piece in pieces(k_all[:, t, :], 3)]
        left = jnp.concatenate([q1, q1, q2, q1, q2, q3], 1)
        right = jnp.concatenate([k1, k2, k1, k3, k2, k1], 1)
        tile_head = lax.rem(iota((1, 6 * LANES), 1), LANES) // GROUP
        for g in range(LANES // GROUP):
            h = t * (LANES // GROUP) + g
            mask = jnp.where(tile_head == g, 1.0, 0.0).astype(BF16)
            logits = dot(left, right * mask, NT) + bias_ref[:, h, :]
            top = jnp.max(logits, axis=1, keepdims=True)
            exponent = jnp.exp(logits - top)
            total = jnp.sum(exponent, axis=1, keepdims=True)
            attn_ref[:, h, :] = exponent * (1.0 / total)
            lse = jnp.where(lane128 == lse_lane + h, top + jnp.log(total), lse)

    turned = jnp.concatenate([lse, jnp.zeros((LANES - queries, LANES), F32)], 0).T
    own_lse = turned[lse_lane : lse_lane + HP]
    lse_inner[inner] = own_lse
    for step in range(1, inner_devs):
        peer = outer * inner_devs + lax.rem(inner + step, inner_devs)
        slot = lse_inner.at[inner]
        remote(slot, slot, (row, peer), LSE_INNER).start()

    @pl.loop(0, queries // 8)
    def _(block):
        for u in range(8):
            i = block * 8 + u
            stacked = jnp.concatenate(pieces(attn_ref[i], 2), 0).astype(BF16)
            high = dot(stacked, pair_hi[i], NN)
            low = dot(stacked[0:HP], pair_lo[i], NN)
            pooled_ref[i] = high[0:HP] + (high[HP:] + low)

    received(lse_inner.at[pl.ds(0, inner_devs - 1)], LSE_INNER)
    lse_outer[outer] = merged(lse_inner[...])
    for step in range(1, outer_devs):
        peer = lax.rem(outer + step, outer_devs) * inner_devs + inner
        slot = lse_outer.at[outer]
        remote(slot, slot, (row, peer), LSE_OUTER).start()

    direct = lax.rem(col // 2, 2) == core

    @pl.when(direct)
    def _():
        of_others(received, v_all, owners, V)
        remote(v_all, v_all, partner, RELAY).start()

    @pl.when(jnp.logical_not(direct))
    def _():
        received(v_all, RELAY)

    values = jnp.concatenate([v_all[:, t, :] for t in range(4)], 1)
    v1, v2 = [piece.astype(BF16) for piece in pieces(values, 2)]
    lane_of = value_head(iota((1, 4 * LANES), 1))
    gathered = jnp.zeros((queries, 4 * LANES), F32)
    for h in range(H):
        mask = jnp.where(lane_of == h, 1.0, 0.0).astype(BF16)
        a1, a2 = [piece.astype(BF16) for piece in pieces(attn_ref[:, h, :], 2)]
        left = jnp.concatenate([a1, a2], 0)
        high = dot(left, v1 * mask, NN)
        low = dot(a1, v2 * mask, NN)
        gathered = gathered + (high[0:queries] + (high[queries:] + low))
    for t in range(4):
        tile = gathered[:, t * LANES : (t + 1) * LANES]
        if t == 3:
            tile = jnp.where(lane128 >= lse_lane, lse, tile)
        point_own[:, t, :] = tile
    for z in range(outer_devs):
        for i in range(rows):
            point_inner[inner, z * rows + i] = point_own[
                (z * inner_devs + inner) * rows + i
            ]
    for step in range(1, inner_devs):
        theirs = lax.rem(inner + step, inner_devs)
        for z in range(outer_devs):
            sent_rows = pl.ds((z * inner_devs + theirs) * rows, rows)
            remote(
                point_own.at[sent_rows],
                point_inner.at[inner, pl.ds(z * rows, rows)],
                (row, outer * inner_devs + theirs),
                POINT_INNER,
            ).start()

    loads[7].wait()
    received(lse_outer.at[pl.ds(0, outer_devs - 1)], LSE_OUTER)
    factor = jnp.exp(own_lse - merged(lse_outer[...]))
    factor = jnp.concatenate([factor, jnp.zeros((LANES - HP, LANES), F32)], 0).T
    projected = jnp.zeros((queries, CS), F32)
    for h in range(0, H, 2):
        scaled = jnp.concatenate(
            [pooled_ref[:, g, :] * factor[0:queries, g : g + 1] for g in (h, h + 1)], 1
        )
        stacked = jnp.concatenate(pieces(scaled, 2), 0).astype(BF16)
        share = dot(stacked, w_out_ref[SPLIT + h * CZ : SPLIT + (h + 2) * CZ, :], NN)
        projected = projected + (share[0:queries] + share[queries:])
    for t in range(CS // LANES):
        part_own[:, t, :] = projected[:, t * LANES : (t + 1) * LANES]
    for i in range(rows):
        part_all[col, i] = part_own[col * rows + i]

    def send_part(peer):
        theirs = part_own.at[pl.ds(peer * rows, rows)]
        remote(theirs, part_all.at[col], (row, peer), PART).start()

    each_row_peer(send_part)

    spread = iota((LANES, 4 * LANES), 0) - lse_lane == value_head(
        iota((LANES, 4 * LANES), 1)
    )
    spread = jnp.logical_and(spread, iota((LANES, 4 * LANES), 0) >= lse_lane)
    spread = jnp.where(spread, 1.0, 0.0).astype(BF16)

    def spread_heads(shares):
        wide = dot(jnp.concatenate(pieces(shares, 2), 0).astype(BF16), spread, NN)
        return wide[0 : shares.shape[0]] + wide[shares.shape[0] :]

    received(point_inner.at[pl.ds(0, inner_devs - 1)], POINT_INNER)
    count = outer_devs * rows
    sums = [point_inner[d, :, 3, :] for d in range(inner_devs)]
    top = functools.reduce(jnp.maximum, sums)
    shares = [jnp.exp(value - top) for value in sums]
    total = sum(shares)
    wide = spread_heads(jnp.concatenate([share / total for share in shares], 0))
    for t in range(4):
        tile = sum(
            point_inner[d, :, t, :]
            * wide[d * count : (d + 1) * count, t * LANES : (t + 1) * LANES]
            for d in range(inner_devs)
        )
        if t == 3:
            tile = jnp.where(lane128 >= lse_lane, top + jnp.log(total), tile)
        point_mid[:, t, :] = tile
    for i in range(rows):
        point_outer[outer, i] = point_mid[outer * rows + i]
    for step in range(1, outer_devs):
        theirs = lax.rem(outer + step, outer_devs)
        remote(
            point_mid.at[pl.ds(theirs * rows, rows)],
            point_outer.at[outer],
            (row, theirs * inner_devs + inner),
            POINT_OUTER,
        ).start()

    received(point_outer.at[pl.ds(0, outer_devs - 1)], POINT_OUTER)
    shares = []
    for i in range(rows):
        sums = point_outer[:, i, 3, :]
        share = jnp.exp(sums - jnp.max(sums, axis=0, keepdims=True))
        shares.append(share / jnp.sum(share, axis=0, keepdims=True))
    wide = spread_heads(jnp.concatenate(shares, 0))
    kept = jnp.concatenate(
        [
            jnp.concatenate(
                [
                    jnp.sum(
                        point_outer[:, i, t, :]
                        * wide[
                            i * outer_devs : (i + 1) * outer_devs,
                            t * LANES : (t + 1) * LANES,
                        ],
                        axis=0,
                        keepdims=True,
                    )
                    for t in range(4)
                ],
                1,
            )
            for i in range(rows)
        ],
        0,
    )
    wide = H * PV
    relative = [
        kept[:, SCALAR + b * wide : SCALAR + (b + 1) * wide] - frame[:, 9 + b : 10 + b]
        for b in range(3)
    ]
    local = [
        frame[:, a : a + 1] * relative[0]
        + frame[:, 3 + a : 4 + a] * relative[1]
        + frame[:, 6 + a : 7 + a] * relative[2]
        for a in range(3)
    ]
    length = jnp.sqrt(local[0] ** 2 + local[1] ** 2 + local[2] ** 2 + 1.0)
    features = jnp.concatenate([kept[:, :SCALAR]] + local + [length], 1).astype(BF16)
    update = dot(features, w_out_ref[0:SPLIT, :], NN)

    received(part_all.at[pl.ds(0, peers)], PART)
    for t in range(CS // LANES):
        part = slice(t * LANES, (t + 1) * LANES)
        terms = [
            jnp.sum(part_all[:, i, t, :], axis=0, keepdims=True) for i in range(rows)
        ]
        out_ref[:, part] = update[:, part] + jnp.concatenate(terms, 0)

    of_others(sent, k_all, row_devs, K)
    of_others(sent, v_all, row_devs // 2, V)

    @pl.when(direct)
    def _():
        sent(v_all, RELAY)

    sent(q_all.at[pl.ds(0, peers * rows)], Q)
    sent(lse_inner.at[pl.ds(0, inner_devs - 1)], LSE_INNER)
    sent(lse_outer.at[pl.ds(0, outer_devs - 1)], LSE_OUTER)
    sent(point_inner.at[pl.ds(0, inner_devs - 1)], POINT_INNER)
    sent(point_outer.at[pl.ds(0, outer_devs - 1)], POINT_OUTER)
    sent(part_own.at[pl.ds(0, peers * rows)], PART)


def solution(mesh):
    sizes = (mesh.shape["row"], mesh.shape["col"])

    def body(singles, pair, frames, w_query, w_keyval, w_bias, head_weights, w_out):
        rows = singles.shape[0]
        queries, keys = pair.shape[0], pair.shape[1]
        owners = keys // rows
        vmem = pl.BlockSpec(memory_space=pltpu.VMEM)
        hbm = pl.BlockSpec(memory_space=pl.ANY)
        dma = pltpu.SemaphoreType.DMA
        return pl.pallas_call(
            functools.partial(kernel, sizes),
            out_shape=jax.ShapeDtypeStruct((rows, w_out.shape[1]), F32),
            in_specs=[hbm] * 8,
            out_specs=vmem,
            scratch_shapes=[
                pltpu.VMEM(singles.shape, singles.dtype),
                pltpu.VMEM(frames.shape, F32),
                pltpu.VMEM(w_bias.shape[::-1], F32),
                pltpu.VMEM((1, H), F32),
                pltpu.VMEM(pair.shape, F32),
                pltpu.VMEM(pair.shape, BF16),
                pltpu.VMEM(pair.shape, BF16),
                pltpu.VMEM(w_query.shape[::-1], w_query.dtype),
                pltpu.VMEM(w_keyval.shape[::-1], w_keyval.dtype),
                pltpu.VMEM(w_out.shape, w_out.dtype),
                pltpu.VMEM((queries, FEAT // LANES, LANES), F32),
                pltpu.VMEM((rows, FEAT // LANES, LANES), F32),
                pltpu.VMEM((rows, 4, LANES), F32),
                pltpu.VMEM((keys, FEAT // LANES, LANES), F32),
                pltpu.VMEM((keys, 4, LANES), F32),
                pltpu.VMEM((queries, HP, keys), F32),
                pltpu.VMEM((queries, HP, keys), F32),
                pltpu.VMEM((queries, HP, CZ), F32),
                pltpu.VMEM((INNER, HP, LANES), F32),
                pltpu.VMEM((sizes[1] // INNER, HP, LANES), F32),
                pltpu.VMEM((queries, 4, LANES), F32),
                pltpu.VMEM((INNER, sizes[1] // INNER * rows, 4, LANES), F32),
                pltpu.VMEM((sizes[1] // INNER * rows, 4, LANES), F32),
                pltpu.VMEM((sizes[1] // INNER, rows, 4, LANES), F32),
                pltpu.VMEM((queries, CS // LANES, LANES), F32),
                pltpu.VMEM((sizes[1], rows, CS // LANES, LANES), F32),
                dma((8,)),
                dma((9,)),
                dma((9,)),
                pltpu.SemaphoreType.REGULAR((sizes[1] // INNER,)),
            ],
            compiler_params=pltpu.CompilerParams(
                collective_id=0, has_side_effects=True, vmem_limit_bytes=60 * 2**20
            ),
        )(
            singles,
            frames,
            w_bias.T,
            head_weights.reshape(1, H),
            pair,
            w_query.T,
            w_keyval.T,
            w_out,
        )

    return jax.shard_map(
        body,
        mesh=mesh,
        in_specs=(
            P(("row", "col"), None),
            P("row", "col", None),
            P(("row", "col"), None),
            P(),
            P(),
            P(),
            P(),
            P(),
        ),
        out_specs=P(("row", "col"), None),
        check_vma=False,
    )
```

```python
import functools
import math

import jax
import jax.numpy as jnp
from jax import lax
from jax.experimental import pallas as pl
from jax.experimental.pallas import tpu as pltpu
from jax.sharding import PartitionSpec as P

CS = 384
CZ = 128
H = 12
CH = 16
PQ = 4
PV = 8

HP = 16
LANES = 128
SCALAR = H * CH
VALUE = SCALAR + 3 * H * PV
SPLIT = H * (CH + 4 * PV)
GROUP = 32
INNER = 4
FEAT = H * GROUP
SCALE = math.sqrt(1.0 / 3.0)
MESH = pl.DeviceIdType.MESH
NT = (((1,), (1,)), ((), ()))
NN = (((1,), (0,)), ((), ()))
F32 = jnp.float32
BF16 = jnp.bfloat16


def dot(left, right, dims):
    return lax.dot_general(left, right, dims, preferred_element_type=F32)


def pieces(value, count):
    result = []
    for _ in range(count):
        piece = value.astype(BF16).astype(F32)
        result.append(piece)
        value = value - piece
    return result


def iota(shape, dim):
    return lax.broadcasted_iota(jnp.int32, shape, dim)


def moved_points(frame, local, width):
    parts = [local[:, b * width : (b + 1) * width] for b in range(3)]
    return [
        frame[:, 3 * a : 3 * a + 1] * parts[0]
        + frame[:, 3 * a + 1 : 3 * a + 2] * parts[1]
        + frame[:, 3 * a + 2 : 3 * a + 3] * parts[2]
        + frame[:, 9 + a : 10 + a]
        for a in range(3)
    ]


def merged(sums):
    top = jnp.max(sums, axis=0)
    return top + jnp.log(jnp.sum(jnp.exp(sums - top[None]), axis=0))


def value_head(lane):
    points = lax.rem(lane - SCALAR, H * PV) // PV
    head = jnp.where(lane < SCALAR, lane // CH, points)
    return jnp.where(lane < VALUE, head, -1)


def kernel(
    sizes,
    singles_hbm,
    frames_hbm,
    w_bias_hbm,
    heads_hbm,
    pair_hbm,
    w_query_hbm,
    w_keyval_hbm,
    w_out_hbm,
    out_ref,
    singles_ref,
    frames_ref,
    w_bias_ref,
    heads_ref,
    pair_ref,
    pair_hi,
    pair_lo,
    w_query_ref,
    w_keyval_ref,
    w_out_ref,
    q_all,
    k_chunk,
    v_chunk,
    k_all,
    v_all,
    bias_ref,
    attn_ref,
    pooled_ref,
    lse_inner,
    lse_outer,
    point_own,
    point_inner,
    point_mid,
    point_outer,
    part_own,
    part_all,
    load_sem,
    send_sem,
    recv_sem,
):
    row_devs, col_devs = sizes
    rows = singles_ref.shape[0]
    queries, keys = pair_ref.shape[0], pair_ref.shape[1]
    owners = keys // rows
    row = lax.axis_index("row")
    col = lax.axis_index("col")

    core = lax.rem(row, 2)
    y = row // 2
    y_devs = row_devs // 2
    partner = (row + 1 - 2 * core, col)
    inner_devs = INNER
    outer_devs = col_devs // INNER
    inner = lax.rem(col, INNER)
    outer = col // INNER
    key_slot = lax.rem(col, owners)

    def key_col_of(source_y):
        return ((2 * source_y + core) * col_devs + col) // owners

    direct = lax.rem(col * owners // col_devs, 2) == core
    own_source_y = (col * owners) // (2 * col_devs)
    own_keys = key_col_of(own_source_y) == col

    barrier = pltpu.get_barrier_semaphore()

    def greet(peer):
        pl.semaphore_signal(barrier, inc=1, device_id=peer, device_id_type=MESH)

    def row_peers():
        half = col_devs // 2
        steps = sorted(range(1, col_devs), key=lambda step: abs(step - half))
        return [lax.rem(col + step, col_devs) for step in steps]

    def y_peers():
        half = y_devs // 2
        steps = sorted(range(1, y_devs), key=lambda step: abs(step - half))
        return [(2 * lax.rem(y + step, y_devs) + core, col) for step in steps]

    for peer in row_peers():
        greet((row, peer))
    for peer in y_peers():
        greet(peer)
    greet(partner)

    moves = [
        (singles_hbm, singles_ref),
        (w_query_hbm, w_query_ref),
        (w_keyval_hbm, w_keyval_ref),
        (frames_hbm, frames_ref),
        (heads_hbm, heads_ref),
        (w_bias_hbm, w_bias_ref),
        (pair_hbm, pair_ref),
        (w_out_hbm, w_out_ref),
    ]
    loads = [
        pltpu.make_async_copy(src, dst, load_sem.at[n]) for n, (src, dst) in enumerate(moves)
    ]
    for load in loads:
        load.start()

    loads[0].wait()
    single = singles_ref[...]
    loads[1].wait()
    query_proj = dot(single, w_query_ref[...], NT)
    loads[2].wait()
    key_proj = dot(single, w_keyval_ref[...], NT)
    loads[3].wait()
    frame = frames_ref[...]

    lane = iota((1, FEAT), 1)
    lane_head = lane // GROUP
    within = lax.rem(lane, GROUP)
    is_scalar = within < CH
    axis = (within - CH) // PQ
    is_point = jnp.logical_and(within >= CH, within < CH + 3 * PQ)
    point = lax.rem(within - CH, PQ)
    targets = [jnp.where(is_scalar, lane_head * CH + within, -1)]
    for b in range(3):
        column = SCALAR + b * H * PQ + lane_head * PQ + point
        targets.append(jnp.where(is_point, column, -1))
    target = jnp.concatenate(targets, 1)
    width = SCALAR + 3 * H * PQ
    place = jnp.where(iota((width, 4 * FEAT), 0) == target, 1.0, 0.0).astype(BF16)
    key_part = jnp.concatenate(
        [key_proj[:, :SCALAR], key_proj[:, 2 * SCALAR : 2 * SCALAR + 3 * H * PQ]], 1
    )
    both = jnp.concatenate(
        [query_proj, key_part, jnp.zeros((8 - 2 * rows, width), F32)], 0
    )
    placed = dot(jnp.concatenate(pieces(both, 3), 0).astype(BF16), place, NN)
    placed = placed[0:8] + placed[8:16] + placed[16:24]
    frame8 = jnp.concatenate([frame, frame, jnp.zeros((8 - 2 * rows, 12), F32)], 0)

    def by_axis(first, stride):
        return jnp.where(
            axis == 0,
            frame8[:, first : first + 1],
            jnp.where(
                axis == 1,
                frame8[:, first + stride : first + stride + 1],
                frame8[:, first + 2 * stride : first + 2 * stride + 1],
            ),
        )

    moved = by_axis(9, 1)
    for b in range(3):
        moved = moved + by_axis(b, 3) * placed[:, (b + 1) * FEAT : (b + 2) * FEAT]
    moved = jnp.where(is_point, moved, 0.0)
    same_head = iota((FEAT, FEAT), 0) // GROUP == iota((FEAT, FEAT), 1) // GROUP
    same_head = jnp.where(same_head, 1.0, 0.0).astype(BF16)
    squares = jnp.concatenate(pieces(moved * moved, 3), 0).astype(BF16)
    squares = dot(squares, same_head, NN)
    squares = squares[0:8] + squares[8:16] + squares[16:24]

    loads[4].wait()
    raw = heads_ref[...]
    gamma = jnp.maximum(raw, 0.0) + jnp.log(1.0 + jnp.exp(-jnp.abs(raw)))
    weight = jnp.zeros((1, FEAT), F32)
    for h in range(H):
        weight = jnp.where(lane_head == h, gamma[:, h : h + 1], weight)
    weight = weight * (SCALE * math.sqrt(2.0 / (9.0 * PQ)) / 2.0)
    scalars = placed[:, :FEAT]
    first_extra = within == CH + 3 * PQ
    second_extra = within == CH + 3 * PQ + 1
    zero = jnp.zeros((8, FEAT), F32)
    q_feat = jnp.where(is_scalar, scalars * (SCALE / math.sqrt(CH)), moved * (2.0 * weight))
    q_feat = jnp.where(first_extra, -weight * squares, q_feat)
    q_feat = jnp.where(second_extra, weight + zero, q_feat)
    k_feat = jnp.where(is_scalar, scalars, moved)
    k_feat = jnp.where(first_extra, 1.0, k_feat)
    k_feat = jnp.where(second_extra, -squares, k_feat)
    v_points = moved_points(frame, key_proj[:, 2 * SCALAR + 3 * H * PQ :], H * PV)
    v_feat = jnp.concatenate(
        [key_proj[:, SCALAR : 2 * SCALAR]]
        + v_points
        + [jnp.zeros((rows, 4 * LANES - VALUE), F32)],
        1,
    )

    own_rows = pl.ds(col * rows, rows)
    key_rows = pl.ds(key_slot * rows, rows)
    for t in range(FEAT // LANES):
        part = slice(t * LANES, (t + 1) * LANES)
        q_all[own_rows, t, :] = q_feat[0:rows, part]
        k_chunk[y, :, t, :] = k_feat[rows : 2 * rows, part]
    for t in range(4):
        v_chunk[y, :, t, :] = v_feat[:, t * LANES : (t + 1) * LANES]

    pl.semaphore_wait(barrier, col_devs + y_devs - 1)

    def remote(src, dst, peer, kind):
        return pltpu.make_async_remote_copy(
            src_ref=src,
            dst_ref=dst,
            send_sem=send_sem.at[kind],
            recv_sem=recv_sem.at[kind],
            device_id=peer,
            device_id_type=MESH,
        )

    def sent(ref, kind):
        remote(ref, ref, partner, kind).wait_send()

    def received(ref, kind):
        remote(ref, ref, partner, kind).wait_recv()

    KY, VY, K, V, Q, KR, VR, LSE_INNER, LSE_OUTER, POINT_INNER, POINT_OUTER, PART = range(12)
    key_rows = pl.ds(key_slot * rows, rows)
    peers = col_devs - 1
    for peer in y_peers():
        remote(k_chunk.at[y], k_chunk.at[y], peer, KY).start()
    for peer in row_peers():
        remote(q_all.at[own_rows], q_all.at[own_rows], (row, peer), Q).start()
    for peer in y_peers():
        remote(v_chunk.at[y], v_chunk.at[y], peer, VY).start()

    def forward(chunk, whole, kind):
        def body(step, carry):
            source_y = lax.rem(outer + step, y_devs)
            peer = key_col_of(source_y)

            @pl.when(peer != col)
            def _():
                remote(chunk.at[source_y], whole.at[key_rows], (row, peer), kind).start()

            return carry

        lax.fori_loop(0, y_devs, body, 0)

        @pl.when(own_keys)
        def _():
            for i in range(rows):
                whole[key_slot * rows + i] = chunk[own_source_y, i]

    def of_sources(act, whole, count, kind):
        @pl.when(own_keys)
        def _():
            act(whole.at[pl.ds(0, (count - 1) * rows)], kind)

        @pl.when(jnp.logical_not(own_keys))
        def _():
            act(whole.at[pl.ds(0, count * rows)], kind)

    loads[5].wait()
    bias_rows = jnp.concatenate([w_bias_ref[...] * SCALE, jnp.zeros((HP - H, CZ), F32)], 0)
    bias_pieces = jnp.concatenate(pieces(bias_rows, 3), 0).astype(BF16)
    loads[6].wait()

    def bias_block(block):
        for u in range(8):
            i = block * 8 + u
            high, middle, low = [piece.astype(BF16) for piece in pieces(pair_ref[i], 3)]
            pair_hi[i] = high
            pair_lo[i] = middle
            first = dot(bias_pieces, high, NT)
            second = dot(bias_pieces[0 : 2 * HP], middle, NT)
            third = dot(bias_pieces[0:HP], low, NT)
            small = first[2 * HP :] + second[HP:] + third
            bias_ref[i] = first[0:HP] + (first[HP : 2 * HP] + second[0:HP] + small)

    blocks = queries // 8
    pl.loop(0, blocks // 2)(bias_block)
    received(k_chunk.at[pl.ds(0, y_devs - 1)], KY)
    forward(k_chunk, k_all, K)
    received(v_chunk.at[pl.ds(0, y_devs - 1)], VY)
    forward(v_chunk, v_all, V)
    pl.loop(blocks // 2, blocks)(bias_block)

    @pl.when(direct)
    def _():
        of_sources(received, k_all, owners, K)
        remote(k_all, k_all, partner, KR).start()

    received(q_all.at[pl.ds(0, peers * rows)], Q)

    @pl.when(direct)
    def _():
        of_sources(received, v_all, owners, V)
        remote(v_all, v_all, partner, VR).start()

    @pl.when(jnp.logical_not(direct))
    def _():
        received(k_all, KR)

    lse_lane = VALUE % LANES
    lane128 = iota((1, LANES), 1)
    lse = jnp.zeros((queries, LANES), F32)
    for t in range(FEAT // LANES):
        q1, q2, q3 = [piece.astype(BF16) for piece in pieces(q_all[:, t, :], 3)]
        k1, k2, k3 = [piece.astype(BF16) for piece in pieces(k_all[:, t, :], 3)]
        left = jnp.concatenate([q1, q1, q2, q1, q2, q3], 1)
        right = jnp.concatenate([k1, k2, k1, k3, k2, k1], 1)
        tile_head = lax.rem(iota((1, 6 * LANES), 1), LANES) // GROUP
        for g in range(LANES // GROUP):
            h = t * (LANES // GROUP) + g
            mask = jnp.where(tile_head == g, 1.0, 0.0).astype(BF16)
            logits = dot(left, right * mask, NT) + bias_ref[:, h, :]
            top = jnp.max(logits, axis=1, keepdims=True)
            exponent = jnp.exp(logits - top)
            total = jnp.sum(exponent, axis=1, keepdims=True)
            attn_ref[:, h, :] = exponent * (1.0 / total)
            lse = jnp.where(lane128 == lse_lane + h, top + jnp.log(total), lse)

    turned = jnp.concatenate([lse, jnp.zeros((LANES - queries, LANES), F32)], 0).T
    own_lse = turned[lse_lane : lse_lane + HP]
    lse_inner[inner] = own_lse
    for step in range(1, inner_devs):
        peer = outer * inner_devs + lax.rem(inner + step, inner_devs)
        slot = lse_inner.at[inner]
        remote(slot, slot, (row, peer), LSE_INNER).start()

    @pl.when(jnp.logical_not(direct))
    def _():
        received(v_all, VR)

    values = jnp.concatenate([v_all[:, t, :] for t in range(4)], 1)
    v1, v2 = [piece.astype(BF16) for piece in pieces(values, 2)]
    lane_of = value_head(iota((1, 4 * LANES), 1))
    gathered = jnp.zeros((queries, 4 * LANES), F32)
    for h in range(H):
        mask = jnp.where(lane_of == h, 1.0, 0.0).astype(BF16)
        a1, a2 = [piece.astype(BF16) for piece in pieces(attn_ref[:, h, :], 2)]
        left = jnp.concatenate([a1, a2], 0)
        high = dot(left, v1 * mask, NN)
        low = dot(a1, v2 * mask, NN)
        gathered = gathered + (high[0:queries] + (high[queries:] + low))
    for t in range(4):
        tile = gathered[:, t * LANES : (t + 1) * LANES]
        if t == 3:
            tile = jnp.where(lane128 >= lse_lane, lse, tile)
        point_own[:, t, :] = tile
    for z in range(outer_devs):
        for i in range(rows):
            point_inner[inner, z * rows + i] = point_own[
                (z * inner_devs + inner) * rows + i
            ]
    for step in range(1, inner_devs):
        theirs = lax.rem(inner + step, inner_devs)
        for z in range(outer_devs):
            sent_rows = pl.ds((z * inner_devs + theirs) * rows, rows)
            remote(
                point_own.at[sent_rows],
                point_inner.at[inner, pl.ds(z * rows, rows)],
                (row, outer * inner_devs + theirs),
                POINT_INNER,
            ).start()

    received(lse_inner.at[pl.ds(0, inner_devs - 1)], LSE_INNER)
    lse_outer[outer] = merged(lse_inner[...])
    for step in range(1, outer_devs):
        peer = lax.rem(outer + step, outer_devs) * inner_devs + inner
        slot = lse_outer.at[outer]
        remote(slot, slot, (row, peer), LSE_OUTER).start()

    @pl.loop(0, queries // 8)
    def _(block):
        for u in range(8):
            i = block * 8 + u
            stacked = jnp.concatenate(pieces(attn_ref[i], 2), 0).astype(BF16)
            high = dot(stacked, pair_hi[i], NN)
            low = dot(stacked[0:HP], pair_lo[i], NN)
            pooled_ref[i] = high[0:HP] + (high[HP:] + low)

    spread = iota((LANES, 4 * LANES), 0) - lse_lane == value_head(
        iota((LANES, 4 * LANES), 1)
    )
    spread = jnp.logical_and(spread, iota((LANES, 4 * LANES), 0) >= lse_lane)
    spread = jnp.where(spread, 1.0, 0.0).astype(BF16)

    def spread_heads(shares):
        wide = dot(jnp.concatenate(pieces(shares, 2), 0).astype(BF16), spread, NN)
        return wide[0 : shares.shape[0]] + wide[shares.shape[0] :]

    received(point_inner.at[pl.ds(0, inner_devs - 1)], POINT_INNER)
    count = outer_devs * rows
    sums = [point_inner[d, :, 3, :] for d in range(inner_devs)]
    top = functools.reduce(jnp.maximum, sums)
    shares = [jnp.exp(value - top) for value in sums]
    total = sum(shares)
    wide = spread_heads(jnp.concatenate([share / total for share in shares], 0))
    for t in range(4):
        tile = sum(
            point_inner[d, :, t, :]
            * wide[d * count : (d + 1) * count, t * LANES : (t + 1) * LANES]
            for d in range(inner_devs)
        )
        if t == 3:
            tile = jnp.where(lane128 >= lse_lane, top + jnp.log(total), tile)
        point_mid[:, t, :] = tile
    for i in range(rows):
        point_outer[outer, i] = point_mid[outer * rows + i]
    for step in range(1, outer_devs):
        theirs = lax.rem(outer + step, outer_devs)
        remote(
            point_mid.at[pl.ds(theirs * rows, rows)],
            point_outer.at[outer],
            (row, theirs * inner_devs + inner),
            POINT_OUTER,
        ).start()

    loads[7].wait()
    received(lse_outer.at[pl.ds(0, outer_devs - 1)], LSE_OUTER)
    factor = jnp.exp(own_lse - merged(lse_outer[...]))
    factor = jnp.concatenate([factor, jnp.zeros((LANES - HP, LANES), F32)], 0).T
    projected = jnp.zeros((queries, CS), F32)
    for h in range(0, H, 2):
        scaled = jnp.concatenate(
            [pooled_ref[:, g, :] * factor[0:queries, g : g + 1] for g in (h, h + 1)], 1
        )
        stacked = jnp.concatenate(pieces(scaled, 2), 0).astype(BF16)
        share = dot(stacked, w_out_ref[SPLIT + h * CZ : SPLIT + (h + 2) * CZ, :], NN)
        projected = projected + (share[0:queries] + share[queries:])
    for t in range(CS // LANES):
        part_own[:, t, :] = projected[:, t * LANES : (t + 1) * LANES]
    for i in range(rows):
        part_all[col, i] = part_own[col * rows + i]
    for peer in row_peers():
        theirs = part_own.at[pl.ds(peer * rows, rows)]
        remote(theirs, part_all.at[col], (row, peer), PART).start()

    received(point_outer.at[pl.ds(0, outer_devs - 1)], POINT_OUTER)
    shares = []
    for i in range(rows):
        sums = point_outer[:, i, 3, :]
        share = jnp.exp(sums - jnp.max(sums, axis=0, keepdims=True))
        shares.append(share / jnp.sum(share, axis=0, keepdims=True))
    wide = spread_heads(jnp.concatenate(shares, 0))
    kept = jnp.concatenate(
        [
            jnp.concatenate(
                [
                    jnp.sum(
                        point_outer[:, i, t, :]
                        * wide[
                            i * outer_devs : (i + 1) * outer_devs,
                            t * LANES : (t + 1) * LANES,
                        ],
                        axis=0,
                        keepdims=True,
                    )
                    for t in range(4)
                ],
                1,
            )
            for i in range(rows)
        ],
        0,
    )
    wide = H * PV
    relative = [
        kept[:, SCALAR + b * wide : SCALAR + (b + 1) * wide] - frame[:, 9 + b : 10 + b]
        for b in range(3)
    ]
    local = [
        frame[:, a : a + 1] * relative[0]
        + frame[:, 3 + a : 4 + a] * relative[1]
        + frame[:, 6 + a : 7 + a] * relative[2]
        for a in range(3)
    ]
    length = jnp.sqrt(local[0] ** 2 + local[1] ** 2 + local[2] ** 2 + 1.0)
    features = jnp.concatenate([kept[:, :SCALAR]] + local + [length], 1).astype(BF16)
    update = dot(features, w_out_ref[0:SPLIT, :], NN)

    received(part_all.at[pl.ds(0, peers)], PART)
    for t in range(CS // LANES):
        part = slice(t * LANES, (t + 1) * LANES)
        terms = [
            jnp.sum(part_all[:, i, t, :], axis=0, keepdims=True) for i in range(rows)
        ]
        out_ref[:, part] = update[:, part] + jnp.concatenate(terms, 0)

    sent(k_chunk.at[pl.ds(0, y_devs - 1)], KY)
    sent(v_chunk.at[pl.ds(0, y_devs - 1)], VY)
    of_sources(sent, k_all, y_devs, K)
    of_sources(sent, v_all, y_devs, V)

    @pl.when(direct)
    def _():
        sent(k_all, KR)
        sent(v_all, VR)

    sent(q_all.at[pl.ds(0, peers * rows)], Q)
    sent(lse_inner.at[pl.ds(0, inner_devs - 1)], LSE_INNER)
    sent(lse_outer.at[pl.ds(0, outer_devs - 1)], LSE_OUTER)
    sent(point_inner.at[pl.ds(0, inner_devs - 1)], POINT_INNER)
    sent(point_outer.at[pl.ds(0, outer_devs - 1)], POINT_OUTER)
    sent(part_own.at[pl.ds(0, peers * rows)], PART)


def solution(mesh):
    sizes = (mesh.shape["row"], mesh.shape["col"])

    def body(singles, pair, frames, w_query, w_keyval, w_bias, head_weights, w_out):
        rows = singles.shape[0]
        queries, keys = pair.shape[0], pair.shape[1]
        vmem = pl.BlockSpec(memory_space=pltpu.VMEM)
        hbm = pl.BlockSpec(memory_space=pl.ANY)
        dma = pltpu.SemaphoreType.DMA
        return pl.pallas_call(
            functools.partial(kernel, sizes),
            out_shape=jax.ShapeDtypeStruct((rows, w_out.shape[1]), F32),
            in_specs=[hbm] * 8,
            out_specs=vmem,
            scratch_shapes=[
                pltpu.VMEM(singles.shape, singles.dtype),
                pltpu.VMEM(frames.shape, F32),
                pltpu.VMEM(w_bias.shape[::-1], F32),
                pltpu.VMEM((1, H), F32),
                pltpu.VMEM(pair.shape, F32),
                pltpu.VMEM(pair.shape, BF16),
                pltpu.VMEM(pair.shape, BF16),
                pltpu.VMEM(w_query.shape[::-1], w_query.dtype),
                pltpu.VMEM(w_keyval.shape[::-1], w_keyval.dtype),
                pltpu.VMEM(w_out.shape, w_out.dtype),
                pltpu.VMEM((queries, FEAT // LANES, LANES), F32),
                pltpu.VMEM((sizes[0] // 2, rows, FEAT // LANES, LANES), F32),
                pltpu.VMEM((sizes[0] // 2, rows, 4, LANES), F32),
                pltpu.VMEM((keys, FEAT // LANES, LANES), F32),
                pltpu.VMEM((keys, 4, LANES), F32),
                pltpu.VMEM((queries, HP, keys), F32),
                pltpu.VMEM((queries, HP, keys), F32),
                pltpu.VMEM((queries, HP, CZ), F32),
                pltpu.VMEM((INNER, HP, LANES), F32),
                pltpu.VMEM((sizes[1] // INNER, HP, LANES), F32),
                pltpu.VMEM((queries, 4, LANES), F32),
                pltpu.VMEM((INNER, sizes[1] // INNER * rows, 4, LANES), F32),
                pltpu.VMEM((sizes[1] // INNER * rows, 4, LANES), F32),
                pltpu.VMEM((sizes[1] // INNER, rows, 4, LANES), F32),
                pltpu.VMEM((queries, CS // LANES, LANES), F32),
                pltpu.VMEM((sizes[1], rows, CS // LANES, LANES), F32),
                dma((8,)),
                dma((12,)),
                dma((12,)),
            ],
            compiler_params=pltpu.CompilerParams(
                collective_id=0, has_side_effects=True, vmem_limit_bytes=60 * 2**20
            ),
        )(
            singles,
            frames,
            w_bias.T,
            head_weights.reshape(1, H),
            pair,
            w_query.T,
            w_keyval.T,
            w_out,
        )

    return jax.shard_map(
        body,
        mesh=mesh,
        in_specs=(
            P(("row", "col"), None),
            P("row", "col", None),
            P(("row", "col"), None),
            P(),
            P(),
            P(),
            P(),
            P(),
        ),
        out_specs=P(("row", "col"), None),
        check_vma=False,
    )
```

```python
import functools
import math

import jax
import jax.numpy as jnp
from jax import lax
from jax.experimental import pallas as pl
from jax.experimental.pallas import tpu as pltpu
from jax.sharding import PartitionSpec as P

CS = 384
CZ = 128
H = 12
CH = 16
PQ = 4
PV = 8

HP = 16
LANES = 128
SCALAR = H * CH
VALUE = SCALAR + 3 * H * PV
SPLIT = H * (CH + 4 * PV)
GROUP = 32
FEAT = H * GROUP
SCALE = math.sqrt(1.0 / 3.0)
MESH = pl.DeviceIdType.MESH
NT = (((1,), (1,)), ((), ()))
NN = (((1,), (0,)), ((), ()))
F32 = jnp.float32
BF16 = jnp.bfloat16


def dot(left, right, dims):
    return lax.dot_general(left, right, dims, preferred_element_type=F32)


def pieces(value, count):
    result = []
    for _ in range(count):
        piece = value.astype(BF16).astype(F32)
        result.append(piece)
        value = value - piece
    return result


def iota(shape, dim):
    return lax.broadcasted_iota(jnp.int32, shape, dim)


def moved_points(frame, local, width):
    parts = [local[:, b * width : (b + 1) * width] for b in range(3)]
    return [
        frame[:, 3 * a : 3 * a + 1] * parts[0]
        + frame[:, 3 * a + 1 : 3 * a + 2] * parts[1]
        + frame[:, 3 * a + 2 : 3 * a + 3] * parts[2]
        + frame[:, 9 + a : 10 + a]
        for a in range(3)
    ]


def value_head(lane):
    points = lax.rem(lane - SCALAR, H * PV) // PV
    head = jnp.where(lane < SCALAR, lane // CH, points)
    return jnp.where(lane < VALUE, head, -1)


def kernel(
    sizes,
    singles_hbm,
    frames_hbm,
    w_bias_hbm,
    heads_hbm,
    pair_hbm,
    w_query_hbm,
    w_keyval_hbm,
    w_out_hbm,
    out_ref,
    singles_ref,
    frames_ref,
    w_bias_ref,
    heads_ref,
    pair_ref,
    pair_hi,
    pair_lo,
    w_query_ref,
    w_keyval_ref,
    w_out_ref,
    q_all,
    k_own,
    v_own,
    k_all,
    v_all,
    bias_ref,
    attn_ref,
    part_own,
    part_all,
    load_sem,
    send_sem,
    recv_sem,
):
    row_devs, col_devs = sizes
    rows = singles_ref.shape[0]
    queries, keys = pair_ref.shape[0], pair_ref.shape[1]
    owners = keys // rows
    row = lax.axis_index("row")
    col = lax.axis_index("col")

    me = row * col_devs + col
    key_col = me // owners
    key_slot = lax.rem(me, owners)
    own_keys = key_col == col

    def source_of(slot):
        index = col * owners + slot
        return (index // col_devs, lax.rem(index, col_devs))

    def far_first(count):
        return sorted(range(1, count), key=lambda step: abs(step - count // 2))

    row_peers = [lax.rem(col + step, col_devs) for step in far_first(col_devs)]
    barrier = pltpu.get_barrier_semaphore()

    def greet(peer):
        pl.semaphore_signal(barrier, inc=1, device_id=peer, device_id_type=MESH)

    def greet_source(step, carry):
        slot = lax.rem(key_slot + step, owners)

        @pl.when(jnp.logical_not(jnp.logical_and(own_keys, slot == key_slot)))
        def _():
            greet(source_of(slot))

        return carry

    lax.fori_loop(0, owners, greet_source, 0)
    for peer in row_peers:
        greet((row, peer))

    moves = [
        (singles_hbm, singles_ref),
        (w_query_hbm, w_query_ref),
        (w_keyval_hbm, w_keyval_ref),
        (frames_hbm, frames_ref),
        (heads_hbm, heads_ref),
        (w_bias_hbm, w_bias_ref),
        (pair_hbm, pair_ref),
        (w_out_hbm, w_out_ref),
    ]
    loads = [
        pltpu.make_async_copy(src, dst, load_sem.at[n]) for n, (src, dst) in enumerate(moves)
    ]
    for load in loads:
        load.start()

    loads[0].wait()
    single = singles_ref[...]
    loads[1].wait()
    query_proj = dot(single, w_query_ref[...], NT)
    loads[2].wait()
    key_proj = dot(single, w_keyval_ref[...], NT)
    loads[3].wait()
    frame = frames_ref[...]

    lane = iota((1, FEAT), 1)
    lane_head = lane // GROUP
    within = lax.rem(lane, GROUP)
    is_scalar = within < CH
    axis = (within - CH) // PQ
    is_point = jnp.logical_and(within >= CH, within < CH + 3 * PQ)
    point = lax.rem(within - CH, PQ)
    targets = [jnp.where(is_scalar, lane_head * CH + within, -1)]
    for b in range(3):
        column = SCALAR + b * H * PQ + lane_head * PQ + point
        targets.append(jnp.where(is_point, column, -1))
    target = jnp.concatenate(targets, 1)
    width = SCALAR + 3 * H * PQ
    place = jnp.where(iota((width, 4 * FEAT), 0) == target, 1.0, 0.0).astype(BF16)
    key_part = jnp.concatenate(
        [key_proj[:, :SCALAR], key_proj[:, 2 * SCALAR : 2 * SCALAR + 3 * H * PQ]], 1
    )
    both = jnp.concatenate(
        [query_proj, key_part, jnp.zeros((8 - 2 * rows, width), F32)], 0
    )
    placed = dot(jnp.concatenate(pieces(both, 3), 0).astype(BF16), place, NN)
    placed = placed[0:8] + placed[8:16] + placed[16:24]
    frame8 = jnp.concatenate([frame, frame, jnp.zeros((8 - 2 * rows, 12), F32)], 0)

    def by_axis(first, stride):
        return jnp.where(
            axis == 0,
            frame8[:, first : first + 1],
            jnp.where(
                axis == 1,
                frame8[:, first + stride : first + stride + 1],
                frame8[:, first + 2 * stride : first + 2 * stride + 1],
            ),
        )

    moved = by_axis(9, 1)
    for b in range(3):
        moved = moved + by_axis(b, 3) * placed[:, (b + 1) * FEAT : (b + 2) * FEAT]
    moved = jnp.where(is_point, moved, 0.0)
    same_head = iota((FEAT, FEAT), 0) // GROUP == iota((FEAT, FEAT), 1) // GROUP
    same_head = jnp.where(same_head, 1.0, 0.0).astype(BF16)
    squares = jnp.concatenate(pieces(moved * moved, 3), 0).astype(BF16)
    squares = dot(squares, same_head, NN)
    squares = squares[0:8] + squares[8:16] + squares[16:24]

    loads[4].wait()
    raw = heads_ref[...]
    gamma = jnp.maximum(raw, 0.0) + jnp.log(1.0 + jnp.exp(-jnp.abs(raw)))
    weight = jnp.zeros((1, FEAT), F32)
    for h in range(H):
        weight = jnp.where(lane_head == h, gamma[:, h : h + 1], weight)
    weight = weight * (SCALE * math.sqrt(2.0 / (9.0 * PQ)) / 2.0)
    scalars = placed[:, :FEAT]
    first_extra = within == CH + 3 * PQ
    second_extra = within == CH + 3 * PQ + 1
    zero = jnp.zeros((8, FEAT), F32)
    q_feat = jnp.where(is_scalar, scalars * (SCALE / math.sqrt(CH)), moved * (2.0 * weight))
    q_feat = jnp.where(first_extra, -weight * squares, q_feat)
    q_feat = jnp.where(second_extra, weight + zero, q_feat)
    k_feat = jnp.where(is_scalar, scalars, moved)
    k_feat = jnp.where(first_extra, 1.0, k_feat)
    k_feat = jnp.where(second_extra, -squares, k_feat)
    v_points = moved_points(frame, key_proj[:, 2 * SCALAR + 3 * H * PQ :], H * PV)
    v_feat = jnp.concatenate(
        [key_proj[:, SCALAR : 2 * SCALAR]]
        + v_points
        + [jnp.zeros((rows, 4 * LANES - VALUE), F32)],
        1,
    )

    own_rows = pl.ds(col * rows, rows)
    key_rows = pl.ds(key_slot * rows, rows)
    for t in range(FEAT // LANES):
        part = slice(t * LANES, (t + 1) * LANES)
        q_all[own_rows, t, :] = q_feat[0:rows, part]
        k_own[:, t, :] = k_feat[rows : 2 * rows, part]
    for t in range(4):
        v_own[:, t, :] = v_feat[:, t * LANES : (t + 1) * LANES]

    key_rows = pl.ds(key_slot * rows, rows)

    @pl.when(own_keys)
    def _():
        for t in range(FEAT // LANES):
            k_all[key_rows, t, :] = k_feat[rows : 2 * rows, t * LANES : (t + 1) * LANES]
        for t in range(4):
            v_all[key_rows, t, :] = v_feat[:, t * LANES : (t + 1) * LANES]

    pl.semaphore_wait(barrier, owners + col_devs - 1 - own_keys.astype(jnp.int32))

    def remote(src, dst, peer, kind):
        return pltpu.make_async_remote_copy(
            src_ref=src,
            dst_ref=dst,
            send_sem=send_sem.at[kind],
            recv_sem=recv_sem.at[kind],
            device_id=peer,
            device_id_type=MESH,
        )

    def sent(ref, kind):
        remote(ref, ref, (row, row_peers[0]), kind).wait_send()

    def received(ref, kind):
        remote(ref, ref, (row, row_peers[0]), kind).wait_recv()

    K, Q, V, PART = range(4)
    peers = col_devs - 1

    def send_keys(src, dst, kind):
        def body(step, carry):
            peer_row = lax.rem(row + row_devs // 2 + step, row_devs)

            @pl.when(jnp.logical_not(jnp.logical_and(own_keys, peer_row == row)))
            def _():
                remote(src, dst.at[key_rows], (peer_row, key_col), kind).start()

            return carry

        lax.fori_loop(0, row_devs, body, 0)

    def of_others(act, ref, count, kind):
        @pl.when(own_keys)
        def _():
            act(ref.at[pl.ds(0, (count - 1) * rows)], kind)

        @pl.when(jnp.logical_not(own_keys))
        def _():
            act(ref.at[pl.ds(0, count * rows)], kind)

    send_keys(k_own, k_all, K)
    for peer in row_peers:
        remote(q_all.at[own_rows], q_all.at[own_rows], (row, peer), Q).start()

    loads[5].wait()
    bias_rows = jnp.concatenate([w_bias_ref[...] * SCALE, jnp.zeros((HP - H, CZ), F32)], 0)
    bias_pieces = jnp.concatenate(pieces(bias_rows, 3), 0).astype(BF16)
    loads[6].wait()

    def bias_block(block):
        for u in range(8):
            i = block * 8 + u
            high, middle, low = [piece.astype(BF16) for piece in pieces(pair_ref[i], 3)]
            pair_hi[i] = high
            pair_lo[i] = middle
            first = dot(bias_pieces, high, NT)
            second = dot(bias_pieces[0 : 2 * HP], middle, NT)
            third = dot(bias_pieces[0:HP], low, NT)
            small = first[2 * HP :] + second[HP:] + third
            bias_ref[i] = first[0:HP] + (first[HP : 2 * HP] + second[0:HP] + small)

    blocks = queries // 8
    pl.loop(0, blocks // 2)(bias_block)
    send_keys(v_own, v_all, V)
    pl.loop(blocks // 2, blocks)(bias_block)

    of_others(received, k_all, owners, K)
    received(q_all.at[pl.ds(0, peers * rows)], Q)

    lse_lane = VALUE % LANES
    lane128 = iota((1, LANES), 1)
    lse = jnp.zeros((queries, LANES), F32)
    for t in range(FEAT // LANES):
        q1, q2, q3 = [piece.astype(BF16) for piece in pieces(q_all[:, t, :], 3)]
        k1, k2, k3 = [piece.astype(BF16) for piece in pieces(k_all[:, t, :], 3)]
        left = jnp.concatenate([q1, q1, q2, q1, q2, q3], 1)
        right = jnp.concatenate([k1, k2, k1, k3, k2, k1], 1)
        tile_head = lax.rem(iota((1, 6 * LANES), 1), LANES) // GROUP
        for g in range(LANES // GROUP):
            h = t * (LANES // GROUP) + g
            mask = jnp.where(tile_head == g, 1.0, 0.0).astype(BF16)
            logits = dot(left, right * mask, NT) + bias_ref[:, h, :]
            top = jnp.max(logits, axis=1, keepdims=True)
            exponent = jnp.exp(logits - top)
            total = jnp.sum(exponent, axis=1, keepdims=True)
            attn_ref[:, h, :] = exponent * (1.0 / total)
            lse = jnp.where(lane128 == lse_lane + h, top + jnp.log(total), lse)

    of_others(received, v_all, owners, V)
    values = jnp.concatenate([v_all[:, t, :] for t in range(4)], 1)
    v1, v2 = [piece.astype(BF16) for piece in pieces(values, 2)]
    lane_of = value_head(iota((1, 4 * LANES), 1))
    gathered = jnp.zeros((queries, 4 * LANES), F32)
    for h in range(H):
        mask = jnp.where(lane_of == h, 1.0, 0.0).astype(BF16)
        a1, a2 = [piece.astype(BF16) for piece in pieces(attn_ref[:, h, :], 2)]
        left = jnp.concatenate([a1, a2], 0)
        high = dot(left, v1 * mask, NN)
        low = dot(a1, v2 * mask, NN)
        gathered = gathered + (high[0:queries] + (high[queries:] + low))
    for t in range(4):
        tile = gathered[:, t * LANES : (t + 1) * LANES]
        if t == 3:
            tile = jnp.where(lane128 >= lse_lane, lse, tile)
        part_own[:, HP - 4 + t, :] = tile

    def pool(n, carry):
        half = col_devs // 2
        steps = [half + 2 * n, half - 1 - 2 * n, half + 2 * n + 1, half - 2 - 2 * n]
        to = [lax.rem(col + step, col_devs) for step in steps]
        for owner in to:
            for i in range(rows):
                at = owner * rows + i
                stacked = jnp.concatenate(pieces(attn_ref[at], 2), 0).astype(BF16)
                high = dot(stacked, pair_hi[at], NN)
                low = dot(stacked[0:HP], pair_lo[at], NN)
                part_own[at, 0:H, :] = (high[0:HP] + (high[HP:] + low))[0:H]
        for owner in to:

            @pl.when(owner != col)
            def _():
                theirs = part_own.at[pl.ds(owner * rows, rows)]
                remote(theirs, part_all.at[col], (row, owner), PART).start()

        return carry

    lax.fori_loop(0, col_devs // 4, pool, 0)
    for i in range(rows):
        part_all[col, i] = part_own[col * rows + i]

    spread = iota((LANES, 4 * LANES), 0) - lse_lane == value_head(
        iota((LANES, 4 * LANES), 1)
    )
    spread = jnp.logical_and(spread, iota((LANES, 4 * LANES), 0) >= lse_lane)
    spread = jnp.where(spread, 1.0, 0.0).astype(BF16)
    loads[7].wait()
    received(part_all.at[pl.ds(0, peers)], PART)
    shares = []
    for i in range(rows):
        sums = part_all[:, i, HP - 1, :]
        share = jnp.exp(sums - jnp.max(sums, axis=0, keepdims=True))
        shares.append(share / jnp.sum(share, axis=0, keepdims=True))
    count = rows * col_devs
    wide = dot(jnp.concatenate(pieces(jnp.concatenate(shares, 0), 2), 0).astype(BF16), spread, NN)
    wide = wide[0:count] + wide[count:]

    def over_devices(tiles):
        return jnp.concatenate([jnp.sum(tile, axis=0, keepdims=True) for tile in tiles], 0)

    kept = jnp.concatenate(
        [
            over_devices(
                part_all[:, i, HP - 4 + t, :]
                * wide[i * col_devs : (i + 1) * col_devs, t * LANES : (t + 1) * LANES]
                for i in range(rows)
            )
            for t in range(4)
        ],
        1,
    )
    pooled = jnp.concatenate(
        [
            over_devices(
                part_all[:, i, h, :] * shares[i][:, lse_lane + h : lse_lane + h + 1]
                for i in range(rows)
            )
            for h in range(H)
        ],
        1,
    )
    pooled = jnp.concatenate([pooled, jnp.zeros((8 - rows, H * CZ), F32)], 0)
    pooled = jnp.concatenate(pieces(pooled, 2), 0).astype(BF16)
    projected = dot(pooled, w_out_ref[SPLIT:, :], NN)
    projected = projected[0:rows] + projected[8 : 8 + rows]
    wide = H * PV
    relative = [
        kept[:, SCALAR + b * wide : SCALAR + (b + 1) * wide] - frame[:, 9 + b : 10 + b]
        for b in range(3)
    ]
    local = [
        frame[:, a : a + 1] * relative[0]
        + frame[:, 3 + a : 4 + a] * relative[1]
        + frame[:, 6 + a : 7 + a] * relative[2]
        for a in range(3)
    ]
    length = jnp.sqrt(local[0] ** 2 + local[1] ** 2 + local[2] ** 2 + 1.0)
    features = jnp.concatenate([kept[:, :SCALAR]] + local + [length], 1).astype(BF16)
    out_ref[...] = dot(features, w_out_ref[0:SPLIT, :], NN) + projected

    of_others(sent, k_all, row_devs, K)
    of_others(sent, v_all, row_devs, V)
    sent(q_all.at[pl.ds(0, peers * rows)], Q)
    sent(part_all.at[pl.ds(0, peers)], PART)


def solution(mesh):
    sizes = (mesh.shape["row"], mesh.shape["col"])

    def body(singles, pair, frames, w_query, w_keyval, w_bias, head_weights, w_out):
        rows = singles.shape[0]
        queries, keys = pair.shape[0], pair.shape[1]
        vmem = pl.BlockSpec(memory_space=pltpu.VMEM)
        hbm = pl.BlockSpec(memory_space=pl.ANY)
        dma = pltpu.SemaphoreType.DMA
        return pl.pallas_call(
            functools.partial(kernel, sizes),
            out_shape=jax.ShapeDtypeStruct((rows, w_out.shape[1]), F32),
            in_specs=[hbm] * 8,
            out_specs=vmem,
            scratch_shapes=[
                pltpu.VMEM(singles.shape, singles.dtype),
                pltpu.VMEM(frames.shape, F32),
                pltpu.VMEM(w_bias.shape[::-1], F32),
                pltpu.VMEM((1, H), F32),
                pltpu.VMEM(pair.shape, F32),
                pltpu.VMEM(pair.shape, BF16),
                pltpu.VMEM(pair.shape, BF16),
                pltpu.VMEM(w_query.shape[::-1], w_query.dtype),
                pltpu.VMEM(w_keyval.shape[::-1], w_keyval.dtype),
                pltpu.VMEM(w_out.shape, w_out.dtype),
                pltpu.VMEM((queries, FEAT // LANES, LANES), F32),
                pltpu.VMEM((rows, FEAT // LANES, LANES), F32),
                pltpu.VMEM((rows, 4, LANES), F32),
                pltpu.VMEM((keys, FEAT // LANES, LANES), F32),
                pltpu.VMEM((keys, 4, LANES), F32),
                pltpu.VMEM((queries, HP, keys), F32),
                pltpu.VMEM((queries, HP, keys), F32),
                pltpu.VMEM((queries, HP, LANES), F32),
                pltpu.VMEM((sizes[1], rows, HP, LANES), F32),
                dma((8,)),
                dma((4,)),
                dma((4,)),
            ],
            compiler_params=pltpu.CompilerParams(
                collective_id=0, has_side_effects=True, vmem_limit_bytes=60 * 2**20
            ),
        )(
            singles,
            frames,
            w_bias.T,
            head_weights.reshape(1, H),
            pair,
            w_query.T,
            w_keyval.T,
            w_out,
        )

    return jax.shard_map(
        body,
        mesh=mesh,
        in_specs=(
            P(("row", "col"), None),
            P("row", "col", None),
            P(("row", "col"), None),
            P(),
            P(),
            P(),
            P(),
            P(),
        ),
        out_specs=P(("row", "col"), None),
        check_vma=False,
    )
```

```python
import functools
import math

import jax
import jax.numpy as jnp
from jax import lax
from jax.experimental import pallas as pl
from jax.experimental.pallas import tpu as pltpu
from jax.sharding import PartitionSpec as P

CS = 384
CZ = 128
H = 12
CH = 16
PQ = 4
PV = 8

HP = 16
LANES = 128
SCALAR = H * CH
VALUE = SCALAR + 3 * H * PV
SPLIT = H * (CH + 4 * PV)
GROUP = 32
FEAT = H * GROUP
SCALE = math.sqrt(1.0 / 3.0)
MESH = pl.DeviceIdType.MESH
NT = (((1,), (1,)), ((), ()))
NN = (((1,), (0,)), ((), ()))
F32 = jnp.float32
BF16 = jnp.bfloat16


def dot(left, right, dims):
    return lax.dot_general(left, right, dims, preferred_element_type=F32)


def pieces(value, count):
    result = []
    for _ in range(count):
        piece = value.astype(BF16).astype(F32)
        result.append(piece)
        value = value - piece
    return result


def iota(shape, dim):
    return lax.broadcasted_iota(jnp.int32, shape, dim)


def moved_points(frame, local, width):
    parts = [local[:, b * width : (b + 1) * width] for b in range(3)]
    return [
        frame[:, 3 * a : 3 * a + 1] * parts[0]
        + frame[:, 3 * a + 1 : 3 * a + 2] * parts[1]
        + frame[:, 3 * a + 2 : 3 * a + 3] * parts[2]
        + frame[:, 9 + a : 10 + a]
        for a in range(3)
    ]


def value_head(lane):
    points = lax.rem(lane - SCALAR, H * PV) // PV
    head = jnp.where(lane < SCALAR, lane // CH, points)
    return jnp.where(lane < VALUE, head, -1)


def kernel(
    sizes,
    singles_hbm,
    frames_hbm,
    w_bias_hbm,
    heads_hbm,
    pair_hbm,
    w_query_hbm,
    w_keyval_hbm,
    w_out_hbm,
    out_ref,
    singles_ref,
    frames_ref,
    w_bias_ref,
    heads_ref,
    pair_ref,
    pair_hi,
    pair_lo,
    w_query_ref,
    w_keyval_ref,
    w_out_ref,
    q_all,
    k_own,
    v_own,
    k_all,
    v_all,
    bias_ref,
    attn_ref,
    pooled_ref,
    lse_all,
    point_own,
    point_all,
    part_own,
    part_all,
    load_sem,
    send_sem,
    recv_sem,
):
    row_devs, col_devs = sizes
    rows = singles_ref.shape[0]
    queries, keys = pair_ref.shape[0], pair_ref.shape[1]
    owners = keys // rows
    row = lax.axis_index("row")
    col = lax.axis_index("col")

    core = lax.rem(row, 2)
    partner = row + 1 - 2 * core
    key_slot = lax.rem(col, owners)
    source_row = col * owners // col_devs
    first_source = lax.rem(col * owners, col_devs)
    direct = lax.rem(source_row, 2) == core

    key_col = (row * col_devs + col) // owners
    own_keys = key_col == col
    other_keys = jnp.logical_not(own_keys)

    def far_first(count):
        return sorted(range(1, count), key=lambda step: abs(step - count // 2))

    row_peers = [(row, lax.rem(col + step, col_devs)) for step in far_first(col_devs)]
    key_peers = [(lax.rem(row + step, row_devs), key_col) for step in far_first(row_devs)]
    barrier = pltpu.get_barrier_semaphore()

    def greet(peer):
        pl.semaphore_signal(barrier, inc=1, device_id=peer, device_id_type=MESH)

    for step in far_first(owners):
        greet((source_row, first_source + lax.rem(key_slot + step, owners)))

    @pl.when(other_keys)
    def _():
        greet((source_row, first_source + key_slot))

    for peer in row_peers + [(partner, col)]:
        greet(peer)

    moves = [
        (singles_hbm, singles_ref),
        (w_query_hbm, w_query_ref),
        (w_keyval_hbm, w_keyval_ref),
        (frames_hbm, frames_ref),
        (heads_hbm, heads_ref),
        (w_bias_hbm, w_bias_ref),
        (pair_hbm, pair_ref),
        (w_out_hbm, w_out_ref),
    ]
    loads = [
        pltpu.make_async_copy(src, dst, load_sem.at[n]) for n, (src, dst) in enumerate(moves)
    ]
    for load in loads:
        load.start()

    loads[0].wait()
    single = singles_ref[...]
    loads[1].wait()
    query_proj = dot(single, w_query_ref[...], NT)
    loads[2].wait()
    key_proj = dot(single, w_keyval_ref[...], NT)
    loads[3].wait()
    frame = frames_ref[...]

    lane = iota((1, FEAT), 1)
    lane_head = lane // GROUP
    within = lax.rem(lane, GROUP)
    is_scalar = within < CH
    axis = (within - CH) // PQ
    is_point = jnp.logical_and(within >= CH, within < CH + 3 * PQ)
    point = lax.rem(within - CH, PQ)
    targets = [jnp.where(is_scalar, lane_head * CH + within, -1)]
    for b in range(3):
        column = SCALAR + b * H * PQ + lane_head * PQ + point
        targets.append(jnp.where(is_point, column, -1))
    target = jnp.concatenate(targets, 1)
    width = SCALAR + 3 * H * PQ
    place = jnp.where(iota((width, 4 * FEAT), 0) == target, 1.0, 0.0).astype(BF16)
    key_part = jnp.concatenate(
        [key_proj[:, :SCALAR], key_proj[:, 2 * SCALAR : 2 * SCALAR + 3 * H * PQ]], 1
    )
    both = jnp.concatenate(
        [query_proj, key_part, jnp.zeros((8 - 2 * rows, width), F32)], 0
    )
    placed = dot(jnp.concatenate(pieces(both, 3), 0).astype(BF16), place, NN)
    placed = placed[0:8] + placed[8:16] + placed[16:24]
    frame8 = jnp.concatenate([frame, frame, jnp.zeros((8 - 2 * rows, 12), F32)], 0)

    def by_axis(first, stride):
        return jnp.where(
            axis == 0,
            frame8[:, first : first + 1],
            jnp.where(
                axis == 1,
                frame8[:, first + stride : first + stride + 1],
                frame8[:, first + 2 * stride : first + 2 * stride + 1],
            ),
        )

    moved = by_axis(9, 1)
    for b in range(3):
        moved = moved + by_axis(b, 3) * placed[:, (b + 1) * FEAT : (b + 2) * FEAT]
    moved = jnp.where(is_point, moved, 0.0)
    same_head = iota((FEAT, FEAT), 0) // GROUP == iota((FEAT, FEAT), 1) // GROUP
    same_head = jnp.where(same_head, 1.0, 0.0).astype(BF16)
    squares = jnp.concatenate(pieces(moved * moved, 3), 0).astype(BF16)
    squares = dot(squares, same_head, NN)
    squares = squares[0:8] + squares[8:16] + squares[16:24]

    loads[4].wait()
    raw = heads_ref[...]
    gamma = jnp.maximum(raw, 0.0) + jnp.log(1.0 + jnp.exp(-jnp.abs(raw)))
    weight = jnp.zeros((1, FEAT), F32)
    for h in range(H):
        weight = jnp.where(lane_head == h, gamma[:, h : h + 1], weight)
    weight = weight * (SCALE * math.sqrt(2.0 / (9.0 * PQ)) / 2.0)
    scalars = placed[:, :FEAT]
    first_extra = within == CH + 3 * PQ
    second_extra = within == CH + 3 * PQ + 1
    zero = jnp.zeros((8, FEAT), F32)
    q_feat = jnp.where(is_scalar, scalars * (SCALE / math.sqrt(CH)), moved * (2.0 * weight))
    q_feat = jnp.where(first_extra, -weight * squares, q_feat)
    q_feat = jnp.where(second_extra, weight + zero, q_feat)
    k_feat = jnp.where(is_scalar, scalars, moved)
    k_feat = jnp.where(first_extra, 1.0, k_feat)
    k_feat = jnp.where(second_extra, -squares, k_feat)
    v_points = moved_points(frame, key_proj[:, 2 * SCALAR + 3 * H * PQ :], H * PV)
    v_feat = jnp.concatenate(
        [key_proj[:, SCALAR : 2 * SCALAR]]
        + v_points
        + [jnp.zeros((rows, 4 * LANES - VALUE), F32)],
        1,
    )

    own_rows = pl.ds(col * rows, rows)
    for t in range(FEAT // LANES):
        part = slice(t * LANES, (t + 1) * LANES)
        q_all[own_rows, t, :] = q_feat[0:rows, part]
        k_own[:, t, :] = k_feat[rows : 2 * rows, part]
    for t in range(4):
        v_own[:, t, :] = v_feat[:, t * LANES : (t + 1) * LANES]

    key_rows = pl.ds(key_slot * rows, rows)

    @pl.when(own_keys)
    def _():
        for t in range(FEAT // LANES):
            k_all[key_rows, t, :] = k_feat[rows : 2 * rows, t * LANES : (t + 1) * LANES]
        for t in range(4):
            v_all[key_rows, t, :] = v_feat[:, t * LANES : (t + 1) * LANES]

    pl.semaphore_wait(barrier, owners + col_devs - own_keys.astype(jnp.int32))

    def remote(src, dst, peer, kind):
        return pltpu.make_async_remote_copy(
            src_ref=src,
            dst_ref=dst,
            send_sem=send_sem.at[kind],
            recv_sem=recv_sem.at[kind],
            device_id=peer,
            device_id_type=MESH,
        )

    def sent(ref, kind):
        remote(ref, ref, (partner, col), kind).wait_send()

    def received(ref, kind):
        remote(ref, ref, (partner, col), kind).wait_recv()

    K, Q, V, RELAY, LSE, POINT, PART = range(7)
    peers = col_devs - 1

    def of_others(act, ref, count, kind):
        @pl.when(own_keys)
        def _():
            act(ref.at[pl.ds(0, (count - 1) * rows)], kind)

        @pl.when(other_keys)
        def _():
            act(ref.at[pl.ds(0, count * rows)], kind)

    for peer in key_peers:
        remote(k_own, k_all.at[key_rows], peer, K).start()

    @pl.when(other_keys)
    def _():
        remote(k_own, k_all.at[key_rows], (row, key_col), K).start()

    for peer in row_peers:
        mine = q_all.at[own_rows]
        remote(mine, mine, peer, Q).start()

    loads[5].wait()
    bias_rows = jnp.concatenate([w_bias_ref[...] * SCALE, jnp.zeros((HP - H, CZ), F32)], 0)
    bias_pieces = jnp.concatenate(pieces(bias_rows, 3), 0).astype(BF16)
    loads[6].wait()

    def bias_block(block):
        for u in range(8):
            i = block * 8 + u
            high, middle, low = [piece.astype(BF16) for piece in pieces(pair_ref[i], 3)]
            pair_hi[i] = high
            pair_lo[i] = middle
            first = dot(bias_pieces, high, NT)
            second = dot(bias_pieces[0 : 2 * HP], middle, NT)
            third = dot(bias_pieces[0:HP], low, NT)
            small = first[2 * HP :] + second[HP:] + third
            bias_ref[i] = first[0:HP] + (first[HP : 2 * HP] + second[0:HP] + small)

    blocks = queries // 8
    pl.loop(0, blocks // 2)(bias_block)
    for step in range(2, row_devs, 2):
        peer = (lax.rem(row + step, row_devs), key_col)
        remote(v_own, v_all.at[key_rows], peer, V).start()

    @pl.when(other_keys)
    def _():
        remote(v_own, v_all.at[key_rows], (row, key_col), V).start()

    pl.loop(blocks // 2, blocks)(bias_block)
    of_others(received, k_all, owners, K)
    received(q_all.at[pl.ds(0, peers * rows)], Q)

    lse_lane = VALUE % LANES
    lane128 = iota((1, LANES), 1)
    lse = jnp.zeros((queries, LANES), F32)
    for t in range(FEAT // LANES):
        q1, q2, q3 = [piece.astype(BF16) for piece in pieces(q_all[:, t, :], 3)]
        k1, k2, k3 = [piece.astype(BF16) for piece in pieces(k_all[:, t, :], 3)]
        left = jnp.concatenate([q1, q1, q2, q1, q2, q3], 1)
        right = jnp.concatenate([k1, k2, k1, k3, k2, k1], 1)
        tile_head = lax.rem(iota((1, 6 * LANES), 1), LANES) // GROUP
        for g in range(LANES // GROUP):
            h = t * (LANES // GROUP) + g
            mask = jnp.where(tile_head == g, 1.0, 0.0).astype(BF16)
            logits = dot(left, right * mask, NT) + bias_ref[:, h, :]
            top = jnp.max(logits, axis=1, keepdims=True)
            exponent = jnp.exp(logits - top)
            total = jnp.sum(exponent, axis=1, keepdims=True)
            attn_ref[:, h, :] = exponent * (1.0 / total)
            lse = jnp.where(lane128 == lse_lane + h, top + jnp.log(total), lse)

    turned = jnp.concatenate([lse, jnp.zeros((LANES - queries, LANES), F32)], 0).T
    own_lse = turned[lse_lane : lse_lane + HP]
    lse_all[col] = own_lse
    for peer in row_peers:
        mine = lse_all.at[col, pl.ds(0, H)]
        remote(mine, mine, peer, LSE).start()

    @pl.when(direct)
    def _():
        of_others(received, v_all, owners, V)
        remote(v_all, v_all, (partner, col), RELAY).start()

    @pl.loop(0, queries // 8)
    def _(block):
        for u in range(8):
            i = block * 8 + u
            stacked = jnp.concatenate(pieces(attn_ref[i], 2), 0).astype(BF16)
            high = dot(stacked, pair_hi[i], NN)
            low = dot(stacked[0:HP], pair_lo[i], NN)
            pooled_ref[i] = high[0:HP] + (high[HP:] + low)

    @pl.when(jnp.logical_not(direct))
    def _():
        received(v_all, RELAY)

    values = jnp.concatenate([v_all[:, t, :] for t in range(4)], 1)
    v1, v2 = [piece.astype(BF16) for piece in pieces(values, 2)]
    lane_of = value_head(iota((1, 4 * LANES), 1))
    gathered = jnp.zeros((queries, 4 * LANES), F32)
    for h in range(H):
        mask = jnp.where(lane_of == h, 1.0, 0.0).astype(BF16)
        a1, a2 = [piece.astype(BF16) for piece in pieces(attn_ref[:, h, :], 2)]
        left = jnp.concatenate([a1, a2], 0)
        high = dot(left, v1 * mask, NN)
        low = dot(a1, v2 * mask, NN)
        gathered = gathered + (high[0:queries] + (high[queries:] + low))
    for t in range(4):
        tile = gathered[:, t * LANES : (t + 1) * LANES]
        if t == 3:
            tile = jnp.where(lane128 >= lse_lane, lse, tile)
        point_own[:, t, :] = tile
    for i in range(rows):
        point_all[col, i] = point_own[col * rows + i]
    for peer in row_peers:
        theirs = point_own.at[pl.ds(peer[1] * rows, rows)]
        remote(theirs, point_all.at[col], peer, POINT).start()

    loads[7].wait()
    received(lse_all.at[pl.ds(0, peers), pl.ds(0, H)], LSE)
    everyone = lse_all[...]
    top = jnp.max(everyone, axis=0)
    whole = top + jnp.log(jnp.sum(jnp.exp(everyone - top[None]), axis=0))
    factor = jnp.exp(own_lse - whole)
    factor = jnp.concatenate([factor, jnp.zeros((LANES - HP, LANES), F32)], 0).T
    projected = jnp.zeros((queries, CS), F32)
    for h in range(0, H, 2):
        scaled = jnp.concatenate(
            [pooled_ref[:, g, :] * factor[0:queries, g : g + 1] for g in (h, h + 1)], 1
        )
        stacked = jnp.concatenate(pieces(scaled, 2), 0).astype(BF16)
        share = dot(stacked, w_out_ref[SPLIT + h * CZ : SPLIT + (h + 2) * CZ, :], NN)
        projected = projected + (share[0:queries] + share[queries:])
    for t in range(CS // LANES):
        part_own[:, t, :] = projected[:, t * LANES : (t + 1) * LANES]
    for i in range(rows):
        part_all[col, i] = part_own[col * rows + i]
    for peer in row_peers:
        theirs = part_own.at[pl.ds(peer[1] * rows, rows)]
        remote(theirs, part_all.at[col], peer, PART).start()

    spread = iota((LANES, 4 * LANES), 0) - lse_lane == value_head(
        iota((LANES, 4 * LANES), 1)
    )
    spread = jnp.logical_and(spread, iota((LANES, 4 * LANES), 0) >= lse_lane)
    spread = jnp.where(spread, 1.0, 0.0).astype(BF16)
    received(point_all.at[pl.ds(0, peers)], POINT)
    shares = []
    for i in range(rows):
        sums = point_all[:, i, 3, :]
        share = jnp.exp(sums - jnp.max(sums, axis=0, keepdims=True))
        shares.append(share / jnp.sum(share, axis=0, keepdims=True))
    count = rows * col_devs
    shares = jnp.concatenate(pieces(jnp.concatenate(shares, 0), 2), 0).astype(BF16)
    wide = dot(shares, spread, NN)
    wide = wide[0:count] + wide[count:]

    def over_devices(tiles):
        return jnp.concatenate([jnp.sum(tile, axis=0, keepdims=True) for tile in tiles], 0)

    kept = jnp.concatenate(
        [
            over_devices(
                point_all[:, i, t, :]
                * wide[i * col_devs : (i + 1) * col_devs, t * LANES : (t + 1) * LANES]
                for i in range(rows)
            )
            for t in range(4)
        ],
        1,
    )
    wide = H * PV
    relative = [
        kept[:, SCALAR + b * wide : SCALAR + (b + 1) * wide] - frame[:, 9 + b : 10 + b]
        for b in range(3)
    ]
    local = [
        frame[:, a : a + 1] * relative[0]
        + frame[:, 3 + a : 4 + a] * relative[1]
        + frame[:, 6 + a : 7 + a] * relative[2]
        for a in range(3)
    ]
    length = jnp.sqrt(local[0] ** 2 + local[1] ** 2 + local[2] ** 2 + 1.0)
    features = jnp.concatenate([kept[:, :SCALAR]] + local + [length], 1).astype(BF16)
    update = dot(features, w_out_ref[0:SPLIT, :], NN)

    received(part_all.at[pl.ds(0, peers)], PART)
    for t in range(CS // LANES):
        part = slice(t * LANES, (t + 1) * LANES)
        terms = over_devices(part_all[:, i, t, :] for i in range(rows))
        out_ref[:, part] = update[:, part] + terms

    of_others(sent, k_all, row_devs, K)
    of_others(sent, v_all, row_devs // 2, V)
    sent(q_all.at[pl.ds(0, peers * rows)], Q)

    @pl.when(direct)
    def _():
        sent(v_all, RELAY)

    sent(lse_all.at[pl.ds(0, peers), pl.ds(0, H)], LSE)
    sent(point_all.at[pl.ds(0, peers)], POINT)
    sent(part_all.at[pl.ds(0, peers)], PART)


def solution(mesh):
    sizes = (mesh.shape["row"], mesh.shape["col"])

    def body(singles, pair, frames, w_query, w_keyval, w_bias, head_weights, w_out):
        rows = singles.shape[0]
        queries, keys = pair.shape[0], pair.shape[1]
        vmem = pl.BlockSpec(memory_space=pltpu.VMEM)
        hbm = pl.BlockSpec(memory_space=pl.ANY)
        dma = pltpu.SemaphoreType.DMA
        return pl.pallas_call(
            functools.partial(kernel, sizes),
            out_shape=jax.ShapeDtypeStruct((rows, w_out.shape[1]), F32),
            in_specs=[hbm] * 8,
            out_specs=vmem,
            scratch_shapes=[
                pltpu.VMEM(singles.shape, singles.dtype),
                pltpu.VMEM(frames.shape, F32),
                pltpu.VMEM(w_bias.shape[::-1], F32),
                pltpu.VMEM((1, H), F32),
                pltpu.VMEM(pair.shape, F32),
                pltpu.VMEM(pair.shape, BF16),
                pltpu.VMEM(pair.shape, BF16),
                pltpu.VMEM(w_query.shape[::-1], w_query.dtype),
                pltpu.VMEM(w_keyval.shape[::-1], w_keyval.dtype),
                pltpu.VMEM(w_out.shape, w_out.dtype),
                pltpu.VMEM((queries, FEAT // LANES, LANES), F32),
                pltpu.VMEM((rows, FEAT // LANES, LANES), F32),
                pltpu.VMEM((rows, 4, LANES), F32),
                pltpu.VMEM((keys, FEAT // LANES, LANES), F32),
                pltpu.VMEM((keys, 4, LANES), F32),
                pltpu.VMEM((queries, HP, keys), F32),
                pltpu.VMEM((queries, HP, keys), F32),
                pltpu.VMEM((queries, HP, CZ), F32),
                pltpu.VMEM((sizes[1], HP, LANES), F32),
                pltpu.VMEM((queries, 4, LANES), F32),
                pltpu.VMEM((sizes[1], rows, 4, LANES), F32),
                pltpu.VMEM((queries, CS // LANES, LANES), F32),
                pltpu.VMEM((sizes[1], rows, CS // LANES, LANES), F32),
                dma((8,)),
                dma((7,)),
                dma((7,)),
            ],
            compiler_params=pltpu.CompilerParams(
                collective_id=0, has_side_effects=True, vmem_limit_bytes=60 * 2**20
            ),
        )(
            singles,
            frames,
            w_bias.T,
            head_weights.reshape(1, H),
            pair,
            w_query.T,
            w_keyval.T,
            w_out,
        )

    return jax.shard_map(
        body,
        mesh=mesh,
        in_specs=(
            P(("row", "col"), None),
            P("row", "col", None),
            P(("row", "col"), None),
            P(),
            P(),
            P(),
            P(),
            P(),
        ),
        out_specs=P(("row", "col"), None),
        check_vma=False,
    )
```

```python
import functools
import math

import jax
import jax.numpy as jnp
from jax import lax
from jax.experimental import pallas as pl
from jax.experimental.pallas import tpu as pltpu
from jax.sharding import PartitionSpec as P

CS = 384
CZ = 128
H = 12
CH = 16
PQ = 4
PV = 8

HP = 16
LANES = 128
SCALAR = H * CH
VALUE = SCALAR + 3 * H * PV
SPLIT = H * (CH + 4 * PV)
GROUP = 32
INNER = 4
FEAT = H * GROUP
SCALE = math.sqrt(1.0 / 3.0)
MESH = pl.DeviceIdType.MESH
NT = (((1,), (1,)), ((), ()))
NN = (((1,), (0,)), ((), ()))
F32 = jnp.float32
BF16 = jnp.bfloat16


def dot(left, right, dims):
    return lax.dot_general(left, right, dims, preferred_element_type=F32)


def pieces(value, count):
    result = []
    for _ in range(count):
        piece = value.astype(BF16).astype(F32)
        result.append(piece)
        value = value - piece
    return result


def iota(shape, dim):
    return lax.broadcasted_iota(jnp.int32, shape, dim)


def moved_points(frame, local, width):
    parts = [local[:, b * width : (b + 1) * width] for b in range(3)]
    return [
        frame[:, 3 * a : 3 * a + 1] * parts[0]
        + frame[:, 3 * a + 1 : 3 * a + 2] * parts[1]
        + frame[:, 3 * a + 2 : 3 * a + 3] * parts[2]
        + frame[:, 9 + a : 10 + a]
        for a in range(3)
    ]


def value_head(lane):
    points = lax.rem(lane - SCALAR, H * PV) // PV
    head = jnp.where(lane < SCALAR, lane // CH, points)
    return jnp.where(lane < VALUE, head, -1)


def kernel(
    sizes,
    singles_hbm,
    frames_hbm,
    w_bias_hbm,
    heads_hbm,
    pair_hbm,
    w_query_hbm,
    w_keyval_hbm,
    w_out_hbm,
    out_ref,
    singles_ref,
    frames_ref,
    w_bias_ref,
    heads_ref,
    pair_ref,
    pair_hi,
    pair_lo,
    w_query_ref,
    w_keyval_ref,
    w_out_ref,
    q_all,
    k_own,
    v_own,
    k_all,
    v_all,
    bias_ref,
    attn_ref,
    pooled_ref,
    lse_all,
    point_own,
    point_inner,
    point_mid,
    point_outer,
    part_own,
    part_all,
    load_sem,
    send_sem,
    recv_sem,
):
    row_devs, col_devs = sizes
    rows = singles_ref.shape[0]
    queries, keys = pair_ref.shape[0], pair_ref.shape[1]
    owners = keys // rows
    row = lax.axis_index("row")
    col = lax.axis_index("col")

    core = lax.rem(row, 2)
    partner = row + 1 - 2 * core
    outer_devs = col_devs // INNER
    inner = lax.rem(col, INNER)
    outer = col // INNER
    key_slot = lax.rem(col, owners)
    source_row = col * owners // col_devs
    first_source = lax.rem(col * owners, col_devs)
    direct = lax.rem(source_row, 2) == core

    key_col = (row * col_devs + col) // owners
    own_keys = key_col == col
    other_keys = jnp.logical_not(own_keys)

    def far_first(count):
        return sorted(range(1, count), key=lambda step: abs(step - count // 2))

    row_peers = [(row, lax.rem(col + step, col_devs)) for step in far_first(col_devs)]
    inner_steps, outer_steps = far_first(INNER), far_first(outer_devs)
    key_peers = [(lax.rem(row + step, row_devs), key_col) for step in far_first(row_devs)]
    barrier = pltpu.get_barrier_semaphore()

    def greet(peer):
        pl.semaphore_signal(barrier, inc=1, device_id=peer, device_id_type=MESH)

    for step in far_first(owners):
        greet((source_row, first_source + lax.rem(key_slot + step, owners)))

    @pl.when(other_keys)
    def _():
        greet((source_row, first_source + key_slot))

    for peer in row_peers + [(partner, col)]:
        greet(peer)

    moves = [
        (singles_hbm, singles_ref),
        (w_query_hbm, w_query_ref),
        (w_keyval_hbm, w_keyval_ref),
        (frames_hbm, frames_ref),
        (heads_hbm, heads_ref),
        (w_bias_hbm, w_bias_ref),
        (pair_hbm, pair_ref),
        (w_out_hbm, w_out_ref),
    ]
    loads = [
        pltpu.make_async_copy(src, dst, load_sem.at[n]) for n, (src, dst) in enumerate(moves)
    ]
    for load in loads:
        load.start()

    loads[0].wait()
    single = singles_ref[...]
    loads[1].wait()
    query_proj = dot(single, w_query_ref[...], NT)
    loads[2].wait()
    key_proj = dot(single, w_keyval_ref[...], NT)
    loads[3].wait()
    frame = frames_ref[...]

    lane = iota((1, FEAT), 1)
    lane_head = lane // GROUP
    within = lax.rem(lane, GROUP)
    is_scalar = within < CH
    axis = (within - CH) // PQ
    is_point = jnp.logical_and(within >= CH, within < CH + 3 * PQ)
    point = lax.rem(within - CH, PQ)
    targets = [jnp.where(is_scalar, lane_head * CH + within, -1)]
    for b in range(3):
        column = SCALAR + b * H * PQ + lane_head * PQ + point
        targets.append(jnp.where(is_point, column, -1))
    target = jnp.concatenate(targets, 1)
    width = SCALAR + 3 * H * PQ
    place = jnp.where(iota((width, 4 * FEAT), 0) == target, 1.0, 0.0).astype(BF16)
    key_part = jnp.concatenate(
        [key_proj[:, :SCALAR], key_proj[:, 2 * SCALAR : 2 * SCALAR + 3 * H * PQ]], 1
    )
    both = jnp.concatenate(
        [query_proj, key_part, jnp.zeros((8 - 2 * rows, width), F32)], 0
    )
    placed = dot(jnp.concatenate(pieces(both, 3), 0).astype(BF16), place, NN)
    placed = placed[0:8] + placed[8:16] + placed[16:24]
    frame8 = jnp.concatenate([frame, frame, jnp.zeros((8 - 2 * rows, 12), F32)], 0)

    def by_axis(first, stride):
        return jnp.where(
            axis == 0,
            frame8[:, first : first + 1],
            jnp.where(
                axis == 1,
                frame8[:, first + stride : first + stride + 1],
                frame8[:, first + 2 * stride : first + 2 * stride + 1],
            ),
        )

    moved = by_axis(9, 1)
    for b in range(3):
        moved = moved + by_axis(b, 3) * placed[:, (b + 1) * FEAT : (b + 2) * FEAT]
    moved = jnp.where(is_point, moved, 0.0)
    same_head = iota((FEAT, FEAT), 0) // GROUP == iota((FEAT, FEAT), 1) // GROUP
    same_head = jnp.where(same_head, 1.0, 0.0).astype(BF16)
    squares = jnp.concatenate(pieces(moved * moved, 3), 0).astype(BF16)
    squares = dot(squares, same_head, NN)
    squares = squares[0:8] + squares[8:16] + squares[16:24]

    loads[4].wait()
    raw = heads_ref[...]
    gamma = jnp.maximum(raw, 0.0) + jnp.log(1.0 + jnp.exp(-jnp.abs(raw)))
    weight = jnp.zeros((1, FEAT), F32)
    for h in range(H):
        weight = jnp.where(lane_head == h, gamma[:, h : h + 1], weight)
    weight = weight * (SCALE * math.sqrt(2.0 / (9.0 * PQ)) / 2.0)
    scalars = placed[:, :FEAT]
    first_extra = within == CH + 3 * PQ
    second_extra = within == CH + 3 * PQ + 1
    zero = jnp.zeros((8, FEAT), F32)
    q_feat = jnp.where(is_scalar, scalars * (SCALE / math.sqrt(CH)), moved * (2.0 * weight))
    q_feat = jnp.where(first_extra, -weight * squares, q_feat)
    q_feat = jnp.where(second_extra, weight + zero, q_feat)
    k_feat = jnp.where(is_scalar, scalars, moved)
    k_feat = jnp.where(first_extra, 1.0, k_feat)
    k_feat = jnp.where(second_extra, -squares, k_feat)
    v_points = moved_points(frame, key_proj[:, 2 * SCALAR + 3 * H * PQ :], H * PV)
    v_feat = jnp.concatenate(
        [key_proj[:, SCALAR : 2 * SCALAR]]
        + v_points
        + [jnp.zeros((rows, 4 * LANES - VALUE), F32)],
        1,
    )

    own_rows = pl.ds(col * rows, rows)
    for t in range(FEAT // LANES):
        part = slice(t * LANES, (t + 1) * LANES)
        q_all[own_rows, t, :] = q_feat[0:rows, part]
        k_own[:, t, :] = k_feat[rows : 2 * rows, part]
    for t in range(4):
        v_own[:, t, :] = v_feat[:, t * LANES : (t + 1) * LANES]

    key_rows = pl.ds(key_slot * rows, rows)

    @pl.when(own_keys)
    def _():
        for t in range(FEAT // LANES):
            k_all[key_rows, t, :] = k_feat[rows : 2 * rows, t * LANES : (t + 1) * LANES]
        for t in range(4):
            v_all[key_rows, t, :] = v_feat[:, t * LANES : (t + 1) * LANES]

    pl.semaphore_wait(barrier, owners + col_devs - own_keys.astype(jnp.int32))

    def remote(src, dst, peer, kind):
        return pltpu.make_async_remote_copy(
            src_ref=src,
            dst_ref=dst,
            send_sem=send_sem.at[kind],
            recv_sem=recv_sem.at[kind],
            device_id=peer,
            device_id_type=MESH,
        )

    def sent(ref, kind):
        remote(ref, ref, (partner, col), kind).wait_send()

    def received(ref, kind):
        remote(ref, ref, (partner, col), kind).wait_recv()

    K, Q, V, RELAY, LSE, POINT_INNER, POINT_OUTER, PART = range(8)
    peers = col_devs - 1

    def of_others(act, ref, count, kind):
        @pl.when(own_keys)
        def _():
            act(ref.at[pl.ds(0, (count - 1) * rows)], kind)

        @pl.when(other_keys)
        def _():
            act(ref.at[pl.ds(0, count * rows)], kind)

    for peer in key_peers:
        remote(k_own, k_all.at[key_rows], peer, K).start()

    @pl.when(other_keys)
    def _():
        remote(k_own, k_all.at[key_rows], (row, key_col), K).start()

    for peer in row_peers:
        mine = q_all.at[own_rows]
        remote(mine, mine, peer, Q).start()

    loads[5].wait()
    bias_rows = jnp.concatenate([w_bias_ref[...] * SCALE, jnp.zeros((HP - H, CZ), F32)], 0)
    bias_pieces = jnp.concatenate(pieces(bias_rows, 3), 0).astype(BF16)
    loads[6].wait()

    def bias_block(block):
        for u in range(8):
            i = block * 8 + u
            high, middle, low = [piece.astype(BF16) for piece in pieces(pair_ref[i], 3)]
            pair_hi[i] = high
            pair_lo[i] = middle
            first = dot(bias_pieces, high, NT)
            second = dot(bias_pieces[0 : 2 * HP], middle, NT)
            third = dot(bias_pieces[0:HP], low, NT)
            small = first[2 * HP :] + second[HP:] + third
            bias_ref[i] = first[0:HP] + (first[HP : 2 * HP] + second[0:HP] + small)

    blocks = queries // 8
    pl.loop(0, blocks // 2)(bias_block)
    for step in range(2, row_devs, 2):
        peer = (lax.rem(row + step, row_devs), key_col)
        remote(v_own, v_all.at[key_rows], peer, V).start()

    @pl.when(other_keys)
    def _():
        remote(v_own, v_all.at[key_rows], (row, key_col), V).start()

    pl.loop(blocks // 2, blocks)(bias_block)
    of_others(received, k_all, owners, K)
    received(q_all.at[pl.ds(0, peers * rows)], Q)

    lse_lane = VALUE % LANES
    lane128 = iota((1, LANES), 1)
    lse = jnp.zeros((queries, LANES), F32)
    for t in range(FEAT // LANES):
        q1, q2, q3 = [piece.astype(BF16) for piece in pieces(q_all[:, t, :], 3)]
        k1, k2, k3 = [piece.astype(BF16) for piece in pieces(k_all[:, t, :], 3)]
        left = jnp.concatenate([q1, q1, q2, q1, q2, q3], 1)
        right = jnp.concatenate([k1, k2, k1, k3, k2, k1], 1)
        tile_head = lax.rem(iota((1, 6 * LANES), 1), LANES) // GROUP
        for g in range(LANES // GROUP):
            h = t * (LANES // GROUP) + g
            mask = jnp.where(tile_head == g, 1.0, 0.0).astype(BF16)
            logits = dot(left, right * mask, NT) + bias_ref[:, h, :]
            top = jnp.max(logits, axis=1, keepdims=True)
            exponent = jnp.exp(logits - top)
            total = jnp.sum(exponent, axis=1, keepdims=True)
            attn_ref[:, h, :] = exponent * (1.0 / total)
            lse = jnp.where(lane128 == lse_lane + h, top + jnp.log(total), lse)

    turned = jnp.concatenate([lse, jnp.zeros((LANES - queries, LANES), F32)], 0).T
    own_lse = turned[lse_lane : lse_lane + HP]
    lse_all[col] = own_lse
    for peer in row_peers:
        mine = lse_all.at[col, pl.ds(0, H)]
        remote(mine, mine, peer, LSE).start()

    @pl.when(direct)
    def _():
        of_others(received, v_all, owners, V)
        remote(v_all, v_all, (partner, col), RELAY).start()

    @pl.loop(0, queries // 8)
    def _(block):
        for u in range(8):
            i = block * 8 + u
            stacked = jnp.concatenate(pieces(attn_ref[i], 2), 0).astype(BF16)
            high = dot(stacked, pair_hi[i], NN)
            low = dot(stacked[0:HP], pair_lo[i], NN)
            pooled_ref[i] = high[0:HP] + (high[HP:] + low)

    @pl.when(jnp.logical_not(direct))
    def _():
        received(v_all, RELAY)

    values = jnp.concatenate([v_all[:, t, :] for t in range(4)], 1)
    v1, v2 = [piece.astype(BF16) for piece in pieces(values, 2)]
    lane_of = value_head(iota((1, 4 * LANES), 1))
    gathered = jnp.zeros((queries, 4 * LANES), F32)
    for h in range(H):
        mask = jnp.where(lane_of == h, 1.0, 0.0).astype(BF16)
        a1, a2 = [piece.astype(BF16) for piece in pieces(attn_ref[:, h, :], 2)]
        left = jnp.concatenate([a1, a2], 0)
        high = dot(left, v1 * mask, NN)
        low = dot(a1, v2 * mask, NN)
        gathered = gathered + (high[0:queries] + (high[queries:] + low))
    for t in range(4):
        tile = gathered[:, t * LANES : (t + 1) * LANES]
        if t == 3:
            tile = jnp.where(lane128 >= lse_lane, lse, tile)
        point_own[:, t, :] = tile
    for z in range(outer_devs):
        for i in range(rows):
            at = (z * INNER + inner) * rows + i
            point_inner[inner, z * rows + i] = point_own[at]
    for step in inner_steps:
        theirs = lax.rem(inner + step, INNER)
        for z in range(outer_devs):
            remote(
                point_own.at[pl.ds((z * INNER + theirs) * rows, rows)],
                point_inner.at[inner, pl.ds(z * rows, rows)],
                (row, outer * INNER + theirs),
                POINT_INNER,
            ).start()

    loads[7].wait()
    received(lse_all.at[pl.ds(0, peers), pl.ds(0, H)], LSE)
    everyone = lse_all[...]
    top = jnp.max(everyone, axis=0)
    whole = top + jnp.log(jnp.sum(jnp.exp(everyone - top[None]), axis=0))
    factor = jnp.exp(own_lse - whole)
    factor = jnp.concatenate([factor, jnp.zeros((LANES - HP, LANES), F32)], 0).T
    projected = jnp.zeros((queries, CS), F32)
    for h in range(0, H, 2):
        scaled = jnp.concatenate(
            [pooled_ref[:, g, :] * factor[0:queries, g : g + 1] for g in (h, h + 1)], 1
        )
        stacked = jnp.concatenate(pieces(scaled, 2), 0).astype(BF16)
        share = dot(stacked, w_out_ref[SPLIT + h * CZ : SPLIT + (h + 2) * CZ, :], NN)
        projected = projected + (share[0:queries] + share[queries:])
    for t in range(CS // LANES):
        part_own[:, t, :] = projected[:, t * LANES : (t + 1) * LANES]
    for i in range(rows):
        part_all[col, i] = part_own[col * rows + i]
    for peer in row_peers:
        theirs = part_own.at[pl.ds(peer[1] * rows, rows)]
        remote(theirs, part_all.at[col], peer, PART).start()

    spread = iota((LANES, 4 * LANES), 0) - lse_lane == value_head(
        iota((LANES, 4 * LANES), 1)
    )
    spread = jnp.logical_and(spread, iota((LANES, 4 * LANES), 0) >= lse_lane)
    spread = jnp.where(spread, 1.0, 0.0).astype(BF16)

    def spread_heads(shares):
        wide = dot(jnp.concatenate(pieces(shares, 2), 0).astype(BF16), spread, NN)
        return wide[0 : shares.shape[0]] + wide[shares.shape[0] :]

    received(point_inner.at[pl.ds(0, INNER - 1)], POINT_INNER)
    count = outer_devs * rows
    sums = [point_inner[d, :, 3, :] for d in range(INNER)]
    top = functools.reduce(jnp.maximum, sums)
    shares = [jnp.exp(value - top) for value in sums]
    total = sum(shares)
    wide = spread_heads(jnp.concatenate([share / total for share in shares], 0))
    for t in range(4):
        tile = sum(
            point_inner[d, :, t, :]
            * wide[d * count : (d + 1) * count, t * LANES : (t + 1) * LANES]
            for d in range(INNER)
        )
        if t == 3:
            tile = jnp.where(lane128 >= lse_lane, top + jnp.log(total), tile)
        point_mid[:, t, :] = tile
    for i in range(rows):
        point_outer[outer, i] = point_mid[outer * rows + i]
    for step in outer_steps:
        theirs = lax.rem(outer + step, outer_devs)
        remote(
            point_mid.at[pl.ds(theirs * rows, rows)],
            point_outer.at[outer],
            (row, theirs * INNER + inner),
            POINT_OUTER,
        ).start()

    def over_devices(tiles):
        return jnp.concatenate([jnp.sum(tile, axis=0, keepdims=True) for tile in tiles], 0)

    received(point_outer.at[pl.ds(0, outer_devs - 1)], POINT_OUTER)
    shares = []
    for i in range(rows):
        sums = point_outer[:, i, 3, :]
        share = jnp.exp(sums - jnp.max(sums, axis=0, keepdims=True))
        shares.append(share / jnp.sum(share, axis=0, keepdims=True))
    wide = spread_heads(jnp.concatenate(shares, 0))
    kept = jnp.concatenate(
        [
            over_devices(
                point_outer[:, i, t, :]
                * wide[i * outer_devs : (i + 1) * outer_devs, t * LANES : (t + 1) * LANES]
                for i in range(rows)
            )
            for t in range(4)
        ],
        1,
    )
    wide = H * PV
    relative = [
        kept[:, SCALAR + b * wide : SCALAR + (b + 1) * wide] - frame[:, 9 + b : 10 + b]
        for b in range(3)
    ]
    local = [
        frame[:, a : a + 1] * relative[0]
        + frame[:, 3 + a : 4 + a] * relative[1]
        + frame[:, 6 + a : 7 + a] * relative[2]
        for a in range(3)
    ]
    length = jnp.sqrt(local[0] ** 2 + local[1] ** 2 + local[2] ** 2 + 1.0)
    features = jnp.concatenate([kept[:, :SCALAR]] + local + [length], 1).astype(BF16)
    update = dot(features, w_out_ref[0:SPLIT, :], NN)

    received(part_all.at[pl.ds(0, peers)], PART)
    for t in range(CS // LANES):
        part = slice(t * LANES, (t + 1) * LANES)
        terms = over_devices(part_all[:, i, t, :] for i in range(rows))
        out_ref[:, part] = update[:, part] + terms

    of_others(sent, k_all, row_devs, K)
    of_others(sent, v_all, row_devs // 2, V)
    sent(q_all.at[pl.ds(0, peers * rows)], Q)

    @pl.when(direct)
    def _():
        sent(v_all, RELAY)

    sent(lse_all.at[pl.ds(0, peers), pl.ds(0, H)], LSE)
    sent(point_inner.at[pl.ds(0, INNER - 1)], POINT_INNER)
    sent(point_outer.at[pl.ds(0, outer_devs - 1)], POINT_OUTER)
    sent(part_all.at[pl.ds(0, peers)], PART)


def solution(mesh):
    sizes = (mesh.shape["row"], mesh.shape["col"])

    def body(singles, pair, frames, w_query, w_keyval, w_bias, head_weights, w_out):
        rows = singles.shape[0]
        queries, keys = pair.shape[0], pair.shape[1]
        vmem = pl.BlockSpec(memory_space=pltpu.VMEM)
        hbm = pl.BlockSpec(memory_space=pl.ANY)
        dma = pltpu.SemaphoreType.DMA
        return pl.pallas_call(
            functools.partial(kernel, sizes),
            out_shape=jax.ShapeDtypeStruct((rows, w_out.shape[1]), F32),
            in_specs=[hbm] * 8,
            out_specs=vmem,
            scratch_shapes=[
                pltpu.VMEM(singles.shape, singles.dtype),
                pltpu.VMEM(frames.shape, F32),
                pltpu.VMEM(w_bias.shape[::-1], F32),
                pltpu.VMEM((1, H), F32),
                pltpu.VMEM(pair.shape, F32),
                pltpu.VMEM(pair.shape, BF16),
                pltpu.VMEM(pair.shape, BF16),
                pltpu.VMEM(w_query.shape[::-1], w_query.dtype),
                pltpu.VMEM(w_keyval.shape[::-1], w_keyval.dtype),
                pltpu.VMEM(w_out.shape, w_out.dtype),
                pltpu.VMEM((queries, FEAT // LANES, LANES), F32),
                pltpu.VMEM((rows, FEAT // LANES, LANES), F32),
                pltpu.VMEM((rows, 4, LANES), F32),
                pltpu.VMEM((keys, FEAT // LANES, LANES), F32),
                pltpu.VMEM((keys, 4, LANES), F32),
                pltpu.VMEM((queries, HP, keys), F32),
                pltpu.VMEM((queries, HP, keys), F32),
                pltpu.VMEM((queries, HP, CZ), F32),
                pltpu.VMEM((sizes[1], HP, LANES), F32),
                pltpu.VMEM((queries, 4, LANES), F32),
                pltpu.VMEM((INNER, sizes[1] // INNER * rows, 4, LANES), F32),
                pltpu.VMEM((sizes[1] // INNER * rows, 4, LANES), F32),
                pltpu.VMEM((sizes[1] // INNER, rows, 4, LANES), F32),
                pltpu.VMEM((queries, CS // LANES, LANES), F32),
                pltpu.VMEM((sizes[1], rows, CS // LANES, LANES), F32),
                dma((8,)),
                dma((8,)),
                dma((8,)),
            ],
            compiler_params=pltpu.CompilerParams(
                collective_id=0, has_side_effects=True, vmem_limit_bytes=60 * 2**20
            ),
        )(
            singles,
            frames,
            w_bias.T,
            head_weights.reshape(1, H),
            pair,
            w_query.T,
            w_keyval.T,
            w_out,
        )

    return jax.shard_map(
        body,
        mesh=mesh,
        in_specs=(
            P(("row", "col"), None),
            P("row", "col", None),
            P(("row", "col"), None),
            P(),
            P(),
            P(),
            P(),
            P(),
        ),
        out_specs=P(("row", "col"), None),
        check_vma=False,
    )
```

```python
import functools
import math

import jax
import jax.numpy as jnp
from jax import lax
from jax.experimental import pallas as pl
from jax.experimental.pallas import tpu as pltpu
from jax.sharding import PartitionSpec as P

CS = 384
CZ = 128
H = 12
CH = 16
PQ = 4
PV = 8

HP = 16
LANES = 128
SCALAR = H * CH
VALUE = SCALAR + 3 * H * PV
SPLIT = H * (CH + 4 * PV)
GROUP = 32
INNER = 4
FEAT = H * GROUP
SCALE = math.sqrt(1.0 / 3.0)
MESH = pl.DeviceIdType.MESH
NT = (((1,), (1,)), ((), ()))
NN = (((1,), (0,)), ((), ()))
F32 = jnp.float32
BF16 = jnp.bfloat16


def dot(left, right, dims):
    return lax.dot_general(left, right, dims, preferred_element_type=F32)


def pieces(value, count):
    result = []
    for _ in range(count):
        piece = value.astype(BF16).astype(F32)
        result.append(piece)
        value = value - piece
    return result


def iota(shape, dim):
    return lax.broadcasted_iota(jnp.int32, shape, dim)


def moved_points(frame, local, width):
    parts = [local[:, b * width : (b + 1) * width] for b in range(3)]
    return [
        frame[:, 3 * a : 3 * a + 1] * parts[0]
        + frame[:, 3 * a + 1 : 3 * a + 2] * parts[1]
        + frame[:, 3 * a + 2 : 3 * a + 3] * parts[2]
        + frame[:, 9 + a : 10 + a]
        for a in range(3)
    ]


def value_head(lane):
    points = lax.rem(lane - SCALAR, H * PV) // PV
    head = jnp.where(lane < SCALAR, lane // CH, points)
    return jnp.where(lane < VALUE, head, -1)


def kernel(
    sizes,
    singles_hbm,
    frames_hbm,
    w_bias_hbm,
    heads_hbm,
    pair_hbm,
    w_query_hbm,
    w_keyval_hbm,
    w_out_hbm,
    out_ref,
    singles_ref,
    frames_ref,
    w_bias_ref,
    heads_ref,
    pair_ref,
    pair_hi,
    pair_lo,
    w_query_ref,
    w_keyval_ref,
    w_out_ref,
    q_all,
    k_own,
    v_own,
    k_all,
    v_all,
    bias_ref,
    attn_ref,
    pooled_ref,
    lse_all,
    point_own,
    point_inner,
    point_mid,
    point_outer,
    part_own,
    part_all,
    load_sem,
    send_sem,
    recv_sem,
):
    row_devs, col_devs = sizes
    rows = singles_ref.shape[0]
    queries, keys = pair_ref.shape[0], pair_ref.shape[1]
    owners = keys // rows
    row = lax.axis_index("row")
    col = lax.axis_index("col")

    core = lax.rem(row, 2)
    partner = row + 1 - 2 * core
    outer_devs = col_devs // INNER
    inner = lax.rem(col, INNER)
    outer = col // INNER
    key_slot = lax.rem(col, owners)
    source_row = col * owners // col_devs
    first_source = lax.rem(col * owners, col_devs)
    direct = lax.rem(source_row, 2) == core

    key_col = (row * col_devs + col) // owners
    own_keys = key_col == col
    other_keys = jnp.logical_not(own_keys)

    def far_first(count):
        return sorted(range(1, count), key=lambda step: abs(step - count // 2))

    row_peers = [(row, lax.rem(col + step, col_devs)) for step in far_first(col_devs)]
    inner_steps, outer_steps = far_first(INNER), far_first(outer_devs)
    key_peers = [(lax.rem(row + step, row_devs), key_col) for step in far_first(row_devs)]
    barrier = pltpu.get_barrier_semaphore()

    def greet(peer):
        pl.semaphore_signal(barrier, inc=1, device_id=peer, device_id_type=MESH)

    for step in far_first(owners):
        greet((source_row, first_source + lax.rem(key_slot + step, owners)))

    @pl.when(other_keys)
    def _():
        greet((source_row, first_source + key_slot))

    for peer in row_peers + [(partner, col)]:
        greet(peer)

    moves = [
        (singles_hbm, singles_ref),
        (w_query_hbm, w_query_ref),
        (w_keyval_hbm, w_keyval_ref),
        (frames_hbm, frames_ref),
        (heads_hbm, heads_ref),
        (w_bias_hbm, w_bias_ref),
        (pair_hbm, pair_ref),
        (w_out_hbm, w_out_ref),
    ]
    loads = [
        pltpu.make_async_copy(src, dst, load_sem.at[n]) for n, (src, dst) in enumerate(moves)
    ]
    for load in loads:
        load.start()

    loads[0].wait()
    single = singles_ref[...]
    loads[1].wait()
    query_proj = dot(single, w_query_ref[...], NT)
    loads[2].wait()
    key_proj = dot(single, w_keyval_ref[...], NT)
    loads[3].wait()
    frame = frames_ref[...]

    lane = iota((1, FEAT), 1)
    lane_head = lane // GROUP
    within = lax.rem(lane, GROUP)
    is_scalar = within < CH
    axis = (within - CH) // PQ
    is_point = jnp.logical_and(within >= CH, within < CH + 3 * PQ)
    point = lax.rem(within - CH, PQ)
    targets = [jnp.where(is_scalar, lane_head * CH + within, -1)]
    for b in range(3):
        column = SCALAR + b * H * PQ + lane_head * PQ + point
        targets.append(jnp.where(is_point, column, -1))
    target = jnp.concatenate(targets, 1)
    width = SCALAR + 3 * H * PQ
    place = jnp.where(iota((width, 4 * FEAT), 0) == target, 1.0, 0.0).astype(BF16)
    key_part = jnp.concatenate(
        [key_proj[:, :SCALAR], key_proj[:, 2 * SCALAR : 2 * SCALAR + 3 * H * PQ]], 1
    )
    both = jnp.concatenate(
        [query_proj, key_part, jnp.zeros((8 - 2 * rows, width), F32)], 0
    )
    placed = dot(jnp.concatenate(pieces(both, 3), 0).astype(BF16), place, NN)
    placed = placed[0:8] + placed[8:16] + placed[16:24]
    frame8 = jnp.concatenate([frame, frame, jnp.zeros((8 - 2 * rows, 12), F32)], 0)

    def by_axis(first, stride):
        return jnp.where(
            axis == 0,
            frame8[:, first : first + 1],
            jnp.where(
                axis == 1,
                frame8[:, first + stride : first + stride + 1],
                frame8[:, first + 2 * stride : first + 2 * stride + 1],
            ),
        )

    moved = by_axis(9, 1)
    for b in range(3):
        moved = moved + by_axis(b, 3) * placed[:, (b + 1) * FEAT : (b + 2) * FEAT]
    moved = jnp.where(is_point, moved, 0.0)
    same_head = iota((FEAT, FEAT), 0) // GROUP == iota((FEAT, FEAT), 1) // GROUP
    same_head = jnp.where(same_head, 1.0, 0.0).astype(BF16)
    squares = jnp.concatenate(pieces(moved * moved, 3), 0).astype(BF16)
    squares = dot(squares, same_head, NN)
    squares = squares[0:8] + squares[8:16] + squares[16:24]

    loads[4].wait()
    raw = heads_ref[...]
    gamma = jnp.maximum(raw, 0.0) + jnp.log(1.0 + jnp.exp(-jnp.abs(raw)))
    weight = jnp.zeros((1, FEAT), F32)
    for h in range(H):
        weight = jnp.where(lane_head == h, gamma[:, h : h + 1], weight)
    weight = weight * (SCALE * math.sqrt(2.0 / (9.0 * PQ)) / 2.0)
    scalars = placed[:, :FEAT]
    first_extra = within == CH + 3 * PQ
    second_extra = within == CH + 3 * PQ + 1
    zero = jnp.zeros((8, FEAT), F32)
    q_feat = jnp.where(is_scalar, scalars * (SCALE / math.sqrt(CH)), moved * (2.0 * weight))
    q_feat = jnp.where(first_extra, -weight * squares, q_feat)
    q_feat = jnp.where(second_extra, weight + zero, q_feat)
    k_feat = jnp.where(is_scalar, scalars, moved)
    k_feat = jnp.where(first_extra, 1.0, k_feat)
    k_feat = jnp.where(second_extra, -squares, k_feat)
    v_points = moved_points(frame, key_proj[:, 2 * SCALAR + 3 * H * PQ :], H * PV)
    v_feat = jnp.concatenate(
        [key_proj[:, SCALAR : 2 * SCALAR]]
        + v_points
        + [jnp.zeros((rows, 4 * LANES - VALUE), F32)],
        1,
    )

    own_rows = pl.ds(col * rows, rows)
    for t in range(FEAT // LANES):
        part = slice(t * LANES, (t + 1) * LANES)
        q_all[own_rows, t, :] = q_feat[0:rows, part]
        k_own[:, t, :] = k_feat[rows : 2 * rows, part]
    for t in range(4):
        v_own[:, t, :] = v_feat[:, t * LANES : (t + 1) * LANES]

    key_rows = pl.ds(key_slot * rows, rows)

    @pl.when(own_keys)
    def _():
        for t in range(FEAT // LANES):
            k_all[key_rows, t, :] = k_feat[rows : 2 * rows, t * LANES : (t + 1) * LANES]
        for t in range(4):
            v_all[key_rows, t, :] = v_feat[:, t * LANES : (t + 1) * LANES]

    pl.semaphore_wait(barrier, owners + col_devs - own_keys.astype(jnp.int32))

    def remote(src, dst, peer, kind):
        return pltpu.make_async_remote_copy(
            src_ref=src,
            dst_ref=dst,
            send_sem=send_sem.at[kind],
            recv_sem=recv_sem.at[kind],
            device_id=peer,
            device_id_type=MESH,
        )

    def sent(ref, kind):
        remote(ref, ref, (partner, col), kind).wait_send()

    def received(ref, kind):
        remote(ref, ref, (partner, col), kind).wait_recv()

    K, Q, V, RELAY, LSE, POINT_INNER, POINT_OUTER, PART = range(8)
    peers = col_devs - 1

    def of_others(act, ref, count, kind):
        @pl.when(own_keys)
        def _():
            act(ref.at[pl.ds(0, (count - 1) * rows)], kind)

        @pl.when(other_keys)
        def _():
            act(ref.at[pl.ds(0, count * rows)], kind)

    for peer in key_peers:
        remote(k_own, k_all.at[key_rows], peer, K).start()

    @pl.when(other_keys)
    def _():
        remote(k_own, k_all.at[key_rows], (row, key_col), K).start()

    for peer in row_peers:
        mine = q_all.at[own_rows]
        remote(mine, mine, peer, Q).start()

    loads[5].wait()
    bias_rows = jnp.concatenate([w_bias_ref[...] * SCALE, jnp.zeros((HP - H, CZ), F32)], 0)
    bias_pieces = jnp.concatenate(pieces(bias_rows, 3), 0).astype(BF16)
    loads[6].wait()

    def bias_block(block):
        for u in range(8):
            i = block * 8 + u
            high, middle, low = [piece.astype(BF16) for piece in pieces(pair_ref[i], 3)]
            pair_hi[i] = high
            pair_lo[i] = middle
            first = dot(bias_pieces, high, NT)
            second = dot(bias_pieces[0 : 2 * HP], middle, NT)
            third = dot(bias_pieces[0:HP], low, NT)
            small = first[2 * HP :] + second[HP:] + third
            bias_ref[i] = first[0:HP] + (first[HP : 2 * HP] + second[0:HP] + small)

    blocks = queries // 8
    pl.loop(0, blocks // 2)(bias_block)
    for step in range(2, row_devs, 2):
        peer = (lax.rem(row + step, row_devs), key_col)
        remote(v_own, v_all.at[key_rows], peer, V).start()

    @pl.when(other_keys)
    def _():
        remote(v_own, v_all.at[key_rows], (row, key_col), V).start()

    pl.loop(blocks // 2, blocks)(bias_block)
    of_others(received, k_all, owners, K)
    received(q_all.at[pl.ds(0, peers * rows)], Q)

    lse_lane = VALUE % LANES
    lane128 = iota((1, LANES), 1)
    lse = jnp.zeros((queries, LANES), F32)
    for t in range(FEAT // LANES):
        q1, q2, q3 = [piece.astype(BF16) for piece in pieces(q_all[:, t, :], 3)]
        k1, k2, k3 = [piece.astype(BF16) for piece in pieces(k_all[:, t, :], 3)]
        left = jnp.concatenate([q1, q1, q2, q1, q2, q3], 1)
        right = jnp.concatenate([k1, k2, k1, k3, k2, k1], 1)
        tile_head = lax.rem(iota((1, 6 * LANES), 1), LANES) // GROUP
        for g in range(LANES // GROUP):
            h = t * (LANES // GROUP) + g
            mask = jnp.where(tile_head == g, 1.0, 0.0).astype(BF16)
            logits = dot(left, right * mask, NT) + bias_ref[:, h, :]
            top = jnp.max(logits, axis=1, keepdims=True)
            exponent = jnp.exp(logits - top)
            total = jnp.sum(exponent, axis=1, keepdims=True)
            attn_ref[:, h, :] = exponent * (1.0 / total)
            lse = jnp.where(lane128 == lse_lane + h, top + jnp.log(total), lse)

    turned = jnp.concatenate([lse, jnp.zeros((LANES - queries, LANES), F32)], 0).T
    own_lse = turned[lse_lane : lse_lane + HP]
    lse_all[col] = own_lse
    for peer in row_peers:
        mine = lse_all.at[col, pl.ds(0, H)]
        remote(mine, mine, peer, LSE).start()

    @pl.when(direct)
    def _():
        of_others(received, v_all, owners, V)
        remote(v_all, v_all, (partner, col), RELAY).start()

    @pl.loop(0, queries // 24)
    def _(block):
        for u in range(24):
            i = block * 24 + u
            stacked = jnp.concatenate(pieces(attn_ref[i], 2), 0).astype(BF16)
            high = dot(stacked, pair_hi[i], NN)
            low = dot(stacked[0:HP], pair_lo[i], NN)
            pooled_ref[i] = high[0:HP] + (high[HP:] + low)

    @pl.when(jnp.logical_not(direct))
    def _():
        received(v_all, RELAY)

    values = jnp.concatenate([v_all[:, t, :] for t in range(4)], 1)
    v1, v2 = [piece.astype(BF16) for piece in pieces(values, 2)]
    lane_of = value_head(iota((1, 4 * LANES), 1))
    for t in range(0, 4, 2):
        part = slice(t * LANES, (t + 2) * LANES)
        gathered = jnp.zeros((queries, 2 * LANES), F32)
        for h in range(H):
            mask = jnp.where(lane_of[:, part] == h, 1.0, 0.0).astype(BF16)
            a1, a2 = [piece.astype(BF16) for piece in pieces(attn_ref[:, h, :], 2)]
            high = dot(jnp.concatenate([a1, a2], 0), v1[:, part] * mask, NN)
            low = dot(a1, v2[:, part] * mask, NN)
            gathered = gathered + (high[0:queries] + (high[queries:] + low))
        if t == 0:
            point_own[:, 0, :] = gathered[:, 0:LANES]
            point_own[:, 1, :] = gathered[:, LANES:]
        else:
            last = gathered[:, LANES:]
            point_own[:, 2, :] = gathered[:, 0:LANES]
            point_own[:, 3, :] = jnp.where(lane128 >= lse_lane, lse, last)
    for z in range(outer_devs):
        for i in range(rows):
            at = (z * INNER + inner) * rows + i
            point_inner[inner, z * rows + i] = point_own[at]
    for step in inner_steps:
        theirs = lax.rem(inner + step, INNER)
        for z in range(outer_devs):
            remote(
                point_own.at[pl.ds((z * INNER + theirs) * rows, rows)],
                point_inner.at[inner, pl.ds(z * rows, rows)],
                (row, outer * INNER + theirs),
                POINT_INNER,
            ).start()

    loads[7].wait()
    received(lse_all.at[pl.ds(0, peers), pl.ds(0, H)], LSE)
    everyone = lse_all[...]
    top = jnp.max(everyone, axis=0)
    whole = top + jnp.log(jnp.sum(jnp.exp(everyone - top[None]), axis=0))
    factor = jnp.exp(own_lse - whole)
    factor = jnp.concatenate([factor, jnp.zeros((LANES - HP, LANES), F32)], 0).T
    projected = jnp.zeros((queries, CS), F32)
    for h in range(0, H, 2):
        scaled = jnp.concatenate(
            [pooled_ref[:, g, :] * factor[0:queries, g : g + 1] for g in (h, h + 1)], 1
        )
        stacked = jnp.concatenate(pieces(scaled, 2), 0).astype(BF16)
        share = dot(stacked, w_out_ref[SPLIT + h * CZ : SPLIT + (h + 2) * CZ, :], NN)
        projected = projected + (share[0:queries] + share[queries:])
    for t in range(CS // LANES):
        part_own[:, t, :] = projected[:, t * LANES : (t + 1) * LANES]
    for i in range(rows):
        part_all[col, i] = part_own[col * rows + i]
    for peer in row_peers:
        theirs = part_own.at[pl.ds(peer[1] * rows, rows)]
        remote(theirs, part_all.at[col], peer, PART).start()

    spread = iota((LANES, 4 * LANES), 0) - lse_lane == value_head(
        iota((LANES, 4 * LANES), 1)
    )
    spread = jnp.logical_and(spread, iota((LANES, 4 * LANES), 0) >= lse_lane)
    spread = jnp.where(spread, 1.0, 0.0).astype(BF16)

    def spread_heads(shares):
        wide = dot(jnp.concatenate(pieces(shares, 2), 0).astype(BF16), spread, NN)
        return wide[0 : shares.shape[0]] + wide[shares.shape[0] :]

    received(point_inner.at[pl.ds(0, INNER - 1)], POINT_INNER)
    count = outer_devs * rows
    sums = [point_inner[d, :, 3, :] for d in range(INNER)]
    top = functools.reduce(jnp.maximum, sums)
    shares = [jnp.exp(value - top) for value in sums]
    total = sum(shares)
    wide = spread_heads(jnp.concatenate([share / total for share in shares], 0))
    for t in range(4):
        tile = sum(
            point_inner[d, :, t, :]
            * wide[d * count : (d + 1) * count, t * LANES : (t + 1) * LANES]
            for d in range(INNER)
        )
        if t == 3:
            tile = jnp.where(lane128 >= lse_lane, top + jnp.log(total), tile)
        point_mid[:, t, :] = tile
    for i in range(rows):
        point_outer[outer, i] = point_mid[outer * rows + i]
    for step in outer_steps:
        theirs = lax.rem(outer + step, outer_devs)
        remote(
            point_mid.at[pl.ds(theirs * rows, rows)],
            point_outer.at[outer],
            (row, theirs * INNER + inner),
            POINT_OUTER,
        ).start()

    def over_devices(tiles):
        return jnp.concatenate([jnp.sum(tile, axis=0, keepdims=True) for tile in tiles], 0)

    received(point_outer.at[pl.ds(0, outer_devs - 1)], POINT_OUTER)
    shares = []
    for i in range(rows):
        sums = point_outer[:, i, 3, :]
        share = jnp.exp(sums - jnp.max(sums, axis=0, keepdims=True))
        shares.append(share / jnp.sum(share, axis=0, keepdims=True))
    wide = spread_heads(jnp.concatenate(shares, 0))
    kept = jnp.concatenate(
        [
            over_devices(
                point_outer[:, i, t, :]
                * wide[i * outer_devs : (i + 1) * outer_devs, t * LANES : (t + 1) * LANES]
                for i in range(rows)
            )
            for t in range(4)
        ],
        1,
    )
    wide = H * PV
    relative = [
        kept[:, SCALAR + b * wide : SCALAR + (b + 1) * wide] - frame[:, 9 + b : 10 + b]
        for b in range(3)
    ]
    local = [
        frame[:, a : a + 1] * relative[0]
        + frame[:, 3 + a : 4 + a] * relative[1]
        + frame[:, 6 + a : 7 + a] * relative[2]
        for a in range(3)
    ]
    length = jnp.sqrt(local[0] ** 2 + local[1] ** 2 + local[2] ** 2 + 1.0)
    features = jnp.concatenate([kept[:, :SCALAR]] + local + [length], 1).astype(BF16)
    update = dot(features, w_out_ref[0:SPLIT, :], NN)

    received(part_all.at[pl.ds(0, peers)], PART)
    for t in range(CS // LANES):
        part = slice(t * LANES, (t + 1) * LANES)
        terms = over_devices(part_all[:, i, t, :] for i in range(rows))
        out_ref[:, part] = update[:, part] + terms

    of_others(sent, k_all, row_devs, K)
    of_others(sent, v_all, row_devs // 2, V)
    sent(q_all.at[pl.ds(0, peers * rows)], Q)

    @pl.when(direct)
    def _():
        sent(v_all, RELAY)

    sent(lse_all.at[pl.ds(0, peers), pl.ds(0, H)], LSE)
    sent(point_inner.at[pl.ds(0, INNER - 1)], POINT_INNER)
    sent(point_outer.at[pl.ds(0, outer_devs - 1)], POINT_OUTER)
    sent(part_all.at[pl.ds(0, peers)], PART)


def solution(mesh):
    sizes = (mesh.shape["row"], mesh.shape["col"])

    def body(singles, pair, frames, w_query, w_keyval, w_bias, head_weights, w_out):
        rows = singles.shape[0]
        queries, keys = pair.shape[0], pair.shape[1]
        vmem = pl.BlockSpec(memory_space=pltpu.VMEM)
        hbm = pl.BlockSpec(memory_space=pl.ANY)
        dma = pltpu.SemaphoreType.DMA
        return pl.pallas_call(
            functools.partial(kernel, sizes),
            out_shape=pltpu.VMEM((rows, w_out.shape[1]), F32),
            in_specs=[hbm] * 8,
            out_specs=vmem,
            scratch_shapes=[
                pltpu.VMEM(singles.shape, singles.dtype),
                pltpu.VMEM(frames.shape, F32),
                pltpu.VMEM(w_bias.shape[::-1], F32),
                pltpu.VMEM((1, H), F32),
                pltpu.VMEM(pair.shape, F32),
                pltpu.VMEM(pair.shape, BF16),
                pltpu.VMEM(pair.shape, BF16),
                pltpu.VMEM(w_query.shape[::-1], w_query.dtype),
                pltpu.VMEM(w_keyval.shape[::-1], w_keyval.dtype),
                pltpu.VMEM(w_out.shape, w_out.dtype),
                pltpu.VMEM((queries, FEAT // LANES, LANES), F32),
                pltpu.VMEM((rows, FEAT // LANES, LANES), F32),
                pltpu.VMEM((rows, 4, LANES), F32),
                pltpu.VMEM((keys, FEAT // LANES, LANES), F32),
                pltpu.VMEM((keys, 4, LANES), F32),
                pltpu.VMEM((queries, HP, keys), F32),
                pltpu.VMEM((queries, HP, keys), F32),
                pltpu.VMEM((queries, HP, CZ), F32),
                pltpu.VMEM((sizes[1], HP, LANES), F32),
                pltpu.VMEM((queries, 4, LANES), F32),
                pltpu.VMEM((INNER, sizes[1] // INNER * rows, 4, LANES), F32),
                pltpu.VMEM((sizes[1] // INNER * rows, 4, LANES), F32),
                pltpu.VMEM((sizes[1] // INNER, rows, 4, LANES), F32),
                pltpu.VMEM((queries, CS // LANES, LANES), F32),
                pltpu.VMEM((sizes[1], rows, CS // LANES, LANES), F32),
                dma((8,)),
                dma((8,)),
                dma((8,)),
            ],
            compiler_params=pltpu.CompilerParams(
                collective_id=0, has_side_effects=True, vmem_limit_bytes=60 * 2**20
            ),
        )(
            singles,
            frames,
            w_bias.T,
            head_weights.reshape(1, H),
            pair,
            w_query.T,
            w_keyval.T,
            w_out,
        )

    return jax.shard_map(
        body,
        mesh=mesh,
        in_specs=(
            P(("row", "col"), None),
            P("row", "col", None),
            P(("row", "col"), None),
            P(),
            P(),
            P(),
            P(),
            P(),
        ),
        out_specs=P(("row", "col"), None),
        check_vma=False,
    )
```

```python
import functools
import math

import jax
import jax.numpy as jnp
from jax import lax
from jax.experimental import pallas as pl
from jax.experimental.pallas import tpu as pltpu
from jax.sharding import PartitionSpec as P

CS = 384
CZ = 128
H = 12
CH = 16
PQ = 4
PV = 8

HP = 16
PITCH = 24
LANES = 128
SCALAR = H * CH
VALUE = SCALAR + 3 * H * PV
SPLIT = H * (CH + 4 * PV)
GROUP = 32
INNER = 4
FEAT = H * GROUP
SCALE = math.sqrt(1.0 / 3.0)
MESH = pl.DeviceIdType.MESH
NT = (((1,), (1,)), ((), ()))
NN = (((1,), (0,)), ((), ()))
F32 = jnp.float32
BF16 = jnp.bfloat16


def dot(left, right, dims):
    return lax.dot_general(left, right, dims, preferred_element_type=F32)


def pieces(value, count):
    result = []
    for _ in range(count):
        piece = value.astype(BF16).astype(F32)
        result.append(piece)
        value = value - piece
    return result


def iota(shape, dim):
    return lax.broadcasted_iota(jnp.int32, shape, dim)


def moved_points(frame, local, width):
    parts = [local[:, b * width : (b + 1) * width] for b in range(3)]
    return [
        frame[:, 3 * a : 3 * a + 1] * parts[0]
        + frame[:, 3 * a + 1 : 3 * a + 2] * parts[1]
        + frame[:, 3 * a + 2 : 3 * a + 3] * parts[2]
        + frame[:, 9 + a : 10 + a]
        for a in range(3)
    ]


def value_head(lane):
    points = lax.rem(lane - SCALAR, H * PV) // PV
    head = jnp.where(lane < SCALAR, lane // CH, points)
    return jnp.where(lane < VALUE, head, -1)


def kernel(
    sizes,
    singles_hbm,
    frames_hbm,
    w_bias_hbm,
    heads_hbm,
    pair_hbm,
    w_query_hbm,
    w_keyval_hbm,
    w_out_hbm,
    out_ref,
    singles_ref,
    frames_ref,
    w_bias_ref,
    heads_ref,
    pair_ref,
    pair_hi,
    pair_lo,
    w_query_ref,
    w_keyval_ref,
    w_out_ref,
    q_all,
    k_own,
    v_own,
    k_all,
    v_all,
    bias_ref,
    attn_ref,
    pooled_ref,
    lse_all,
    point_own,
    point_inner,
    point_mid,
    point_outer,
    part_own,
    part_all,
    load_sem,
    send_sem,
    recv_sem,
):
    row_devs, col_devs = sizes
    rows = singles_ref.shape[0]
    queries, keys = pair_ref.shape[0], pair_ref.shape[1]
    owners = keys // rows
    row = lax.axis_index("row")
    col = lax.axis_index("col")

    core = lax.rem(row, 2)
    partner = row + 1 - 2 * core
    outer_devs = col_devs // INNER
    inner = lax.rem(col, INNER)
    outer = col // INNER
    key_slot = lax.rem(col, owners)
    source_row = col * owners // col_devs
    first_source = lax.rem(col * owners, col_devs)
    direct = lax.rem(source_row, 2) == core

    key_col = (row * col_devs + col) // owners
    own_keys = key_col == col
    other_keys = jnp.logical_not(own_keys)

    def far_first(count):
        return sorted(range(1, count), key=lambda step: abs(step - count // 2))

    row_peers = [(row, lax.rem(col + step, col_devs)) for step in far_first(col_devs)]
    inner_steps, outer_steps = far_first(INNER), far_first(outer_devs)
    key_peers = [(lax.rem(row + step, row_devs), key_col) for step in far_first(row_devs)]
    barrier = pltpu.get_barrier_semaphore()

    def greet(peer):
        pl.semaphore_signal(barrier, inc=1, device_id=peer, device_id_type=MESH)

    for step in far_first(owners):
        greet((source_row, first_source + lax.rem(key_slot + step, owners)))

    @pl.when(other_keys)
    def _():
        greet((source_row, first_source + key_slot))

    for peer in row_peers + [(partner, col)]:
        greet(peer)

    moves = [
        (singles_hbm, singles_ref),
        (w_query_hbm, w_query_ref),
        (w_keyval_hbm, w_keyval_ref),
        (frames_hbm, frames_ref),
        (heads_hbm, heads_ref),
        (w_bias_hbm, w_bias_ref),
        (pair_hbm, pair_ref),
        (w_out_hbm, w_out_ref),
    ]
    loads = [
        pltpu.make_async_copy(src, dst, load_sem.at[n]) for n, (src, dst) in enumerate(moves)
    ]
    for load in loads:
        load.start()

    loads[0].wait()
    single = singles_ref[...]
    loads[1].wait()
    query_proj = dot(single, w_query_ref[...], NT)
    loads[2].wait()
    key_proj = dot(single, w_keyval_ref[...], NT)
    loads[3].wait()
    frame = frames_ref[...]

    lane = iota((1, FEAT), 1)
    lane_head = lane // GROUP
    within = lax.rem(lane, GROUP)
    is_scalar = within < CH
    axis = (within - CH) // PQ
    is_point = jnp.logical_and(within >= CH, within < CH + 3 * PQ)
    point = lax.rem(within - CH, PQ)
    targets = [jnp.where(is_scalar, lane_head * CH + within, -1)]
    for b in range(3):
        column = SCALAR + b * H * PQ + lane_head * PQ + point
        targets.append(jnp.where(is_point, column, -1))
    target = jnp.concatenate(targets, 1)
    width = SCALAR + 3 * H * PQ
    place = jnp.where(iota((width, 4 * FEAT), 0) == target, 1.0, 0.0).astype(BF16)
    key_part = jnp.concatenate(
        [key_proj[:, :SCALAR], key_proj[:, 2 * SCALAR : 2 * SCALAR + 3 * H * PQ]], 1
    )
    both = jnp.concatenate(
        [query_proj, key_part, jnp.zeros((8 - 2 * rows, width), F32)], 0
    )
    placed = dot(jnp.concatenate(pieces(both, 3), 0).astype(BF16), place, NN)
    placed = placed[0:8] + placed[8:16] + placed[16:24]
    frame8 = jnp.concatenate([frame, frame, jnp.zeros((8 - 2 * rows, 12), F32)], 0)

    def by_axis(first, stride):
        return jnp.where(
            axis == 0,
            frame8[:, first : first + 1],
            jnp.where(
                axis == 1,
                frame8[:, first + stride : first + stride + 1],
                frame8[:, first + 2 * stride : first + 2 * stride + 1],
            ),
        )

    moved = by_axis(9, 1)
    for b in range(3):
        moved = moved + by_axis(b, 3) * placed[:, (b + 1) * FEAT : (b + 2) * FEAT]
    moved = jnp.where(is_point, moved, 0.0)
    same_head = iota((FEAT, FEAT), 0) // GROUP == iota((FEAT, FEAT), 1) // GROUP
    same_head = jnp.where(same_head, 1.0, 0.0).astype(BF16)
    squares = jnp.concatenate(pieces(moved * moved, 3), 0).astype(BF16)
    squares = dot(squares, same_head, NN)
    squares = squares[0:8] + squares[8:16] + squares[16:24]

    loads[4].wait()
    raw = heads_ref[...]
    gamma = jnp.maximum(raw, 0.0) + jnp.log(1.0 + jnp.exp(-jnp.abs(raw)))
    weight = jnp.zeros((1, FEAT), F32)
    for h in range(H):
        weight = jnp.where(lane_head == h, gamma[:, h : h + 1], weight)
    weight = weight * (SCALE * math.sqrt(2.0 / (9.0 * PQ)) / 2.0)
    scalars = placed[:, :FEAT]
    first_extra = within == CH + 3 * PQ
    second_extra = within == CH + 3 * PQ + 1
    zero = jnp.zeros((8, FEAT), F32)
    q_feat = jnp.where(is_scalar, scalars * (SCALE / math.sqrt(CH)), moved * (2.0 * weight))
    q_feat = jnp.where(first_extra, -weight * squares, q_feat)
    q_feat = jnp.where(second_extra, weight + zero, q_feat)
    k_feat = jnp.where(is_scalar, scalars, moved)
    k_feat = jnp.where(first_extra, 1.0, k_feat)
    k_feat = jnp.where(second_extra, -squares, k_feat)
    v_points = moved_points(frame, key_proj[:, 2 * SCALAR + 3 * H * PQ :], H * PV)
    v_feat = jnp.concatenate(
        [key_proj[:, SCALAR : 2 * SCALAR]]
        + v_points
        + [jnp.zeros((rows, 4 * LANES - VALUE), F32)],
        1,
    )

    own_rows = pl.ds(col * rows, rows)
    for t in range(FEAT // LANES):
        part = slice(t * LANES, (t + 1) * LANES)
        q_all[own_rows, t, :] = q_feat[0:rows, part]
        k_own[:, t, :] = k_feat[rows : 2 * rows, part]
    for t in range(4):
        v_own[:, t, :] = v_feat[:, t * LANES : (t + 1) * LANES]

    key_rows = pl.ds(key_slot * rows, rows)

    @pl.when(own_keys)
    def _():
        for t in range(FEAT // LANES):
            k_all[key_rows, t, :] = k_feat[rows : 2 * rows, t * LANES : (t + 1) * LANES]
        for t in range(4):
            v_all[key_rows, t, :] = v_feat[:, t * LANES : (t + 1) * LANES]

    pl.semaphore_wait(barrier, owners + col_devs - own_keys.astype(jnp.int32))

    def remote(src, dst, peer, kind):
        return pltpu.make_async_remote_copy(
            src_ref=src,
            dst_ref=dst,
            send_sem=send_sem.at[kind],
            recv_sem=recv_sem.at[kind],
            device_id=peer,
            device_id_type=MESH,
        )

    def sent(ref, kind):
        remote(ref, ref, (partner, col), kind).wait_send()

    def received(ref, kind):
        remote(ref, ref, (partner, col), kind).wait_recv()

    K, Q, V, RELAY, LSE, POINT_INNER, POINT_OUTER, PART = range(8)
    peers = col_devs - 1

    def of_others(act, ref, count, kind):
        @pl.when(own_keys)
        def _():
            act(ref.at[pl.ds(0, (count - 1) * rows)], kind)

        @pl.when(other_keys)
        def _():
            act(ref.at[pl.ds(0, count * rows)], kind)

    for peer in key_peers:
        remote(k_own, k_all.at[key_rows], peer, K).start()

    @pl.when(other_keys)
    def _():
        remote(k_own, k_all.at[key_rows], (row, key_col), K).start()

    for peer in row_peers:
        mine = q_all.at[own_rows]
        remote(mine, mine, peer, Q).start()

    loads[5].wait()
    bias_rows = jnp.concatenate([w_bias_ref[...] * SCALE, jnp.zeros((HP - H, CZ), F32)], 0)
    bias_pieces = jnp.concatenate(pieces(bias_rows, 3), 0).astype(BF16)
    loads[6].wait()

    def bias_block(block):
        for u in range(8):
            i = block * 8 + u
            high, middle, low = [piece.astype(BF16) for piece in pieces(pair_ref[i], 3)]
            pair_hi[i] = high
            pair_lo[i] = middle
            first = dot(bias_pieces, high, NT)
            second = dot(bias_pieces[0 : 2 * HP], middle, NT)
            third = dot(bias_pieces[0:HP], low, NT)
            small = first[2 * HP :] + second[HP:] + third
            bias_ref[i, 0:HP, :] = first[0:HP] + (first[HP : 2 * HP] + second[0:HP] + small)

    blocks = queries // 8
    pl.loop(0, blocks // 2)(bias_block)
    for step in range(2, row_devs, 2):
        peer = (lax.rem(row + step, row_devs), key_col)
        remote(v_own, v_all.at[key_rows], peer, V).start()

    @pl.when(other_keys)
    def _():
        remote(v_own, v_all.at[key_rows], (row, key_col), V).start()

    pl.loop(blocks // 2, blocks)(bias_block)
    of_others(received, k_all, owners, K)
    received(q_all.at[pl.ds(0, peers * rows)], Q)

    lse_lane = VALUE % LANES
    lane128 = iota((1, LANES), 1)
    lse = jnp.zeros((queries, LANES), F32)
    per_tile = LANES // GROUP
    tile_head = lax.rem(iota((6 * LANES, keys), 0), LANES) // GROUP

    def inner_products(t):
        q1, q2, q3 = [piece.astype(BF16) for piece in pieces(q_all[:, t, :], 3)]
        k1, k2, k3 = [piece.astype(BF16) for piece in pieces(k_all[:, t, :].T, 3)]
        left = jnp.concatenate([q1, q1, q2, q1, q2, q3], 1)
        right = jnp.concatenate([k1, k2, k1, k3, k2, k1], 0)
        masks = [jnp.where(tile_head == g, 1.0, 0.0).astype(BF16) for g in range(per_tile)]
        return [dot(left, right * mask, NN) for mask in masks]

    coming = inner_products(0)
    for t in range(FEAT // LANES):
        products = coming
        if (t + 1) * LANES < FEAT:
            coming = inner_products(t + 1)
        for g in range(per_tile):
            h = t * per_tile + g
            logits = products[g] + bias_ref[:, h, :]
            top = jnp.max(logits, axis=1, keepdims=True)
            exponent = jnp.exp(logits - top)
            total = jnp.sum(exponent, axis=1, keepdims=True)
            attn_ref[:, h, :] = exponent * (1.0 / total)
            lse = jnp.where(lane128 == lse_lane + h, top + jnp.log(total), lse)

    turned = jnp.concatenate([lse, jnp.zeros((LANES - queries, LANES), F32)], 0).T
    own_lse = turned[lse_lane : lse_lane + HP]
    lse_all[col] = own_lse
    for peer in row_peers:
        mine = lse_all.at[col, pl.ds(0, H)]
        remote(mine, mine, peer, LSE).start()

    @pl.when(direct)
    def _():
        of_others(received, v_all, owners, V)
        remote(v_all, v_all, (partner, col), RELAY).start()

    @pl.loop(0, queries // 24)
    def _(block):
        for u in range(24):
            i = block * 24 + u
            stacked = jnp.concatenate(pieces(attn_ref[i, 0:HP, :], 2), 0).astype(BF16)
            high = dot(stacked, pair_hi[i], NN)
            low = dot(stacked[0:HP], pair_lo[i], NN)
            pooled_ref[i, 0:HP, :] = high[0:HP] + (high[HP:] + low)

    @pl.when(jnp.logical_not(direct))
    def _():
        received(v_all, RELAY)

    values = jnp.concatenate([v_all[:, t, :] for t in range(4)], 1)
    v1, v2 = [piece.astype(BF16) for piece in pieces(values, 2)]
    lane_of = value_head(iota((1, 4 * LANES), 1))
    for t in range(0, 4, 2):
        part = slice(t * LANES, (t + 2) * LANES)
        gathered = jnp.zeros((queries, 2 * LANES), F32)
        for h in range(H):
            mask = jnp.where(lane_of[:, part] == h, 1.0, 0.0).astype(BF16)
            a1, a2 = [piece.astype(BF16) for piece in pieces(attn_ref[:, h, :], 2)]
            high = dot(jnp.concatenate([a1, a2], 0), v1[:, part] * mask, NN)
            low = dot(a1, v2[:, part] * mask, NN)
            gathered = gathered + (high[0:queries] + (high[queries:] + low))
        if t == 0:
            point_own[:, 0, :] = gathered[:, 0:LANES]
            point_own[:, 1, :] = gathered[:, LANES:]
        else:
            last = gathered[:, LANES:]
            point_own[:, 2, :] = gathered[:, 0:LANES]
            point_own[:, 3, :] = jnp.where(lane128 >= lse_lane, lse, last)
    for z in range(outer_devs):
        for i in range(rows):
            at = (z * INNER + inner) * rows + i
            point_inner[inner, z * rows + i] = point_own[at]
    for step in inner_steps:
        theirs = lax.rem(inner + step, INNER)
        for z in range(outer_devs):
            remote(
                point_own.at[pl.ds((z * INNER + theirs) * rows, rows)],
                point_inner.at[inner, pl.ds(z * rows, rows)],
                (row, outer * INNER + theirs),
                POINT_INNER,
            ).start()

    loads[7].wait()
    received(lse_all.at[pl.ds(0, peers), pl.ds(0, H)], LSE)
    everyone = lse_all[...]
    top = jnp.max(everyone, axis=0)
    whole = top + jnp.log(jnp.sum(jnp.exp(everyone - top[None]), axis=0))
    factor = jnp.exp(own_lse - whole)
    factor = jnp.concatenate([factor, jnp.zeros((LANES - HP, LANES), F32)], 0).T
    projected = jnp.zeros((queries, CS), F32)
    for h in range(0, H, 2):
        scaled = jnp.concatenate(
            [pooled_ref[:, g, :] * factor[0:queries, g : g + 1] for g in (h, h + 1)], 1
        )
        stacked = jnp.concatenate(pieces(scaled, 2), 0).astype(BF16)
        share = dot(stacked, w_out_ref[SPLIT + h * CZ : SPLIT + (h + 2) * CZ, :], NN)
        projected = projected + (share[0:queries] + share[queries:])
    for t in range(CS // LANES):
        part_own[:, t, :] = projected[:, t * LANES : (t + 1) * LANES]
    for i in range(rows):
        part_all[col, i] = part_own[col * rows + i]
    for peer in row_peers:
        theirs = part_own.at[pl.ds(peer[1] * rows, rows)]
        remote(theirs, part_all.at[col], peer, PART).start()

    spread = iota((LANES, 4 * LANES), 0) - lse_lane == value_head(
        iota((LANES, 4 * LANES), 1)
    )
    spread = jnp.logical_and(spread, iota((LANES, 4 * LANES), 0) >= lse_lane)
    spread = jnp.where(spread, 1.0, 0.0).astype(BF16)

    def spread_heads(shares):
        wide = dot(jnp.concatenate(pieces(shares, 2), 0).astype(BF16), spread, NN)
        return wide[0 : shares.shape[0]] + wide[shares.shape[0] :]

    received(point_inner.at[pl.ds(0, INNER - 1)], POINT_INNER)
    count = outer_devs * rows
    sums = [point_inner[d, :, 3, :] for d in range(INNER)]
    top = functools.reduce(jnp.maximum, sums)
    shares = [jnp.exp(value - top) for value in sums]
    total = sum(shares)
    wide = spread_heads(jnp.concatenate([share / total for share in shares], 0))
    for t in range(4):
        tile = sum(
            point_inner[d, :, t, :]
            * wide[d * count : (d + 1) * count, t * LANES : (t + 1) * LANES]
            for d in range(INNER)
        )
        if t == 3:
            tile = jnp.where(lane128 >= lse_lane, top + jnp.log(total), tile)
        point_mid[:, t, :] = tile
    for i in range(rows):
        point_outer[outer, i] = point_mid[outer * rows + i]
    for step in outer_steps:
        theirs = lax.rem(outer + step, outer_devs)
        remote(
            point_mid.at[pl.ds(theirs * rows, rows)],
            point_outer.at[outer],
            (row, theirs * INNER + inner),
            POINT_OUTER,
        ).start()

    def over_devices(tiles):
        return jnp.concatenate([jnp.sum(tile, axis=0, keepdims=True) for tile in tiles], 0)

    received(point_outer.at[pl.ds(0, outer_devs - 1)], POINT_OUTER)
    shares = []
    for i in range(rows):
        sums = point_outer[:, i, 3, :]
        share = jnp.exp(sums - jnp.max(sums, axis=0, keepdims=True))
        shares.append(share / jnp.sum(share, axis=0, keepdims=True))
    wide = spread_heads(jnp.concatenate(shares, 0))
    kept = jnp.concatenate(
        [
            over_devices(
                point_outer[:, i, t, :]
                * wide[i * outer_devs : (i + 1) * outer_devs, t * LANES : (t + 1) * LANES]
                for i in range(rows)
            )
            for t in range(4)
        ],
        1,
    )
    wide = H * PV
    relative = [
        kept[:, SCALAR + b * wide : SCALAR + (b + 1) * wide] - frame[:, 9 + b : 10 + b]
        for b in range(3)
    ]
    local = [
        frame[:, a : a + 1] * relative[0]
        + frame[:, 3 + a : 4 + a] * relative[1]
        + frame[:, 6 + a : 7 + a] * relative[2]
        for a in range(3)
    ]
    length = jnp.sqrt(local[0] ** 2 + local[1] ** 2 + local[2] ** 2 + 1.0)
    features = jnp.concatenate([kept[:, :SCALAR]] + local + [length], 1).astype(BF16)
    update = dot(features, w_out_ref[0:SPLIT, :], NN)

    received(part_all.at[pl.ds(0, peers)], PART)
    for t in range(CS // LANES):
        part = slice(t * LANES, (t + 1) * LANES)
        terms = over_devices(part_all[:, i, t, :] for i in range(rows))
        out_ref[:, part] = update[:, part] + terms

    of_others(sent, k_all, row_devs, K)
    of_others(sent, v_all, row_devs // 2, V)
    sent(q_all.at[pl.ds(0, peers * rows)], Q)

    @pl.when(direct)
    def _():
        sent(v_all, RELAY)

    sent(lse_all.at[pl.ds(0, peers), pl.ds(0, H)], LSE)
    sent(point_inner.at[pl.ds(0, INNER - 1)], POINT_INNER)
    sent(point_outer.at[pl.ds(0, outer_devs - 1)], POINT_OUTER)
    sent(part_all.at[pl.ds(0, peers)], PART)


def solution(mesh):
    sizes = (mesh.shape["row"], mesh.shape["col"])

    def body(singles, pair, frames, w_query, w_keyval, w_bias, head_weights, w_out):
        rows = singles.shape[0]
        queries, keys = pair.shape[0], pair.shape[1]
        vmem = pl.BlockSpec(memory_space=pltpu.VMEM)
        hbm = pl.BlockSpec(memory_space=pl.ANY)
        dma = pltpu.SemaphoreType.DMA
        return pl.pallas_call(
            functools.partial(kernel, sizes),
            out_shape=pltpu.VMEM((rows, w_out.shape[1]), F32),
            in_specs=[hbm] * 8,
            out_specs=vmem,
            scratch_shapes=[
                pltpu.VMEM(singles.shape, singles.dtype),
                pltpu.VMEM(frames.shape, F32),
                pltpu.VMEM(w_bias.shape[::-1], F32),
                pltpu.VMEM((1, H), F32),
                pltpu.VMEM(pair.shape, F32),
                pltpu.VMEM(pair.shape, BF16),
                pltpu.VMEM(pair.shape, BF16),
                pltpu.VMEM(w_query.shape[::-1], w_query.dtype),
                pltpu.VMEM(w_keyval.shape[::-1], w_keyval.dtype),
                pltpu.VMEM(w_out.shape, w_out.dtype),
                pltpu.VMEM((queries, FEAT // LANES, LANES), F32),
                pltpu.VMEM((rows, FEAT // LANES, LANES), F32),
                pltpu.VMEM((rows, 4, LANES), F32),
                pltpu.VMEM((keys, FEAT // LANES, LANES), F32),
                pltpu.VMEM((keys, 4, LANES), F32),
                pltpu.VMEM((queries, PITCH, keys), F32),
                pltpu.VMEM((queries, PITCH, keys), F32),
                pltpu.VMEM((queries, PITCH, CZ), F32),
                pltpu.VMEM((sizes[1], HP, LANES), F32),
                pltpu.VMEM((queries, 4, LANES), F32),
                pltpu.VMEM((INNER, sizes[1] // INNER * rows, 4, LANES), F32),
                pltpu.VMEM((sizes[1] // INNER * rows, 4, LANES), F32),
                pltpu.VMEM((sizes[1] // INNER, rows, 4, LANES), F32),
                pltpu.VMEM((queries, CS // LANES, LANES), F32),
                pltpu.VMEM((sizes[1], rows, CS // LANES, LANES), F32),
                dma((8,)),
                dma((8,)),
                dma((8,)),
            ],
            compiler_params=pltpu.CompilerParams(
                collective_id=0, has_side_effects=True, vmem_limit_bytes=60 * 2**20
            ),
        )(
            singles,
            frames,
            w_bias.T,
            head_weights.reshape(1, H),
            pair,
            w_query.T,
            w_keyval.T,
            w_out,
        )

    return jax.shard_map(
        body,
        mesh=mesh,
        in_specs=(
            P(("row", "col"), None),
            P("row", "col", None),
            P(("row", "col"), None),
            P(),
            P(),
            P(),
            P(),
            P(),
        ),
        out_specs=P(("row", "col"), None),
        check_vma=False,
    )
```
